8 devices in a mesh: dp: 2 (over z, y), cp: 4 (over x, core).
Axes of the slice: x: 2, y: 2, z: 1, core: 2. Of those that a mesh axis runs over, the one named last changes fastest.
Arguments:
- queries: bfloat16 [64, 512, 10, 256], P('dp', 'cp'), parts along dimension 0
- key_states: bfloat16 [64, 512, 256], P('dp', 'cp'), parts along dimension 0
- value_states: bfloat16 [64, 512, 256], P('dp', 'cp'), parts along dimension 0
- segment_ids: int32 [64, 512], P('dp', 'cp'), parts along dimension 0
Outputs:
- output 1: bfloat16 [64, 512, 10, 256], P('dp', 'cp'), parts along dimension 0
- output 2: float32 [64, 512, 10], P('dp', 'cp'), parts along dimension 0
There are 2 independent parts. The reference program is written for one: setup_inputs(seed, part) draws one part's arguments, and reference() takes and returns one part's arrays. A program takes and returns all parts, laid end to end along the dimension named above; each array names one.
All inputs are finite; a program needn't handle non-finite values.
Results may differ from the reference program's by a relative error of at most 0.00326493.
Values are sent between devices in bfloat16 or wider.
A program may use at most 1 GiB of HBM per device.

```python
import jax
import jax.numpy as jnp
from jax import lax

BATCH = 32
SEQ = 512
HEADS = 10
HEAD = 256
CUTS = 1
QUERY_BLOCK = 64


def setup_inputs(seed: int = 0, part: int = 0) -> dict:
    base_key = jax.random.fold_in(jax.random.key(seed), part)
    sub_keys = jax.random.split(base_key, 5)
    queries = jax.random.normal(sub_keys[0], (BATCH, SEQ, HEADS, HEAD), jnp.float32)
    key_states = jax.random.normal(sub_keys[1], (BATCH, SEQ, HEAD), jnp.float32)
    value_noise = jax.random.normal(sub_keys[2], (BATCH, SEQ, HEAD), jnp.float32)
    drift = jnp.cumsum(jax.random.normal(sub_keys[3], (BATCH, SEQ, HEAD), jnp.float32), axis=1) * (2.0 / SEQ) ** 0.5
    value_states = 0.5 * value_noise + drift
    cut_points = jax.random.randint(sub_keys[4], (BATCH, CUTS), 1, SEQ)
    positions = jnp.arange(SEQ)
    segment_ids = jnp.sum((positions[None, :, None] >= cut_points[:, None, :]).astype(jnp.int32), axis=-1)
    return {
        "queries": queries.astype(jnp.bfloat16),
        "key_states": key_states.astype(jnp.bfloat16),
        "value_states": value_states.astype(jnp.bfloat16),
        "segment_ids": segment_ids.astype(jnp.int32),
    }


def reference(queries, key_states, value_states, segment_ids):
    score_scale = HEAD ** -0.5
    num_blocks = SEQ // QUERY_BLOCK
    key_pos = jnp.arange(SEQ)

    def one_row(row_inputs):
        q_row, k_row, v_row, seg_row = row_inputs
        k_wide = k_row.astype(jnp.float32)
        v_wide = v_row.astype(jnp.float32)

        def one_block(blk_idx):
            row_start = blk_idx * QUERY_BLOCK
            q_blk = lax.dynamic_slice_in_dim(q_row, row_start, QUERY_BLOCK, 0).astype(jnp.float32)
            seg_blk = lax.dynamic_slice_in_dim(seg_row, row_start, QUERY_BLOCK, 0)
            q_pos = row_start + jnp.arange(QUERY_BLOCK)
            visible = (key_pos[None, :] <= q_pos[:, None]) & (seg_row[None, :] == seg_blk[:, None])
            scores = jnp.einsum("qhd,kd->qhk", q_blk, k_wide) * score_scale
            scores = jnp.where(visible[:, None, :], scores, -jnp.inf)
            row_max = jnp.max(scores, axis=-1)
            weights = jnp.exp(scores - row_max[..., None])
            weight_sum = jnp.sum(weights, axis=-1)
            weighted = jnp.einsum("qhk,kd->qhd", weights, v_wide) / weight_sum[..., None]
            return weighted.astype(jnp.bfloat16), row_max + jnp.log(weight_sum)

        out_blocks, lse_blocks = lax.map(one_block, jnp.arange(num_blocks))
        return out_blocks.reshape(SEQ, HEADS, HEAD), lse_blocks.reshape(SEQ, HEADS)

    attn_out, log_sum_exp = lax.map(one_row, (queries, key_states, value_states, segment_ids))
    return attn_out, log_sum_exp
```

```python
import functools

import jax
import jax.numpy as jnp
from jax import lax
from jax.experimental import pallas as pl
from jax.experimental.pallas import tpu as pltpu
from jax.sharding import PartitionSpec as P


CHUNKS = (8, 8, 8, 4, 4)
LOG2E = 1.4426950408889634


def attend_kernel(first, heads, s_ref, q_ref, own_ref, near_ref, fara_ref, farb_ref, *rest):
    if first:
        o_ref, lse_ref, key_scr, val_scr = rest
    else:
        _, lse_in, o_ref, lse_ref, key_scr, val_scr = rest
    base = s_ref[0]
    step = pl.program_id(0)
    piece = own_ref.shape[1] // 2
    head = q_ref.shape[3]
    group = 2
    scale = head ** -0.5
    cut = s_ref[6 + base + step]
    me = s_ref[1]

    if not first:
        @pl.when(step == 0)
        def _():
            lse_ref[...] = lse_in[...]

    blocks = (own_ref, near_ref, fara_ref, farb_ref)

    def run(count):
        keys = count * piece
        for n in range(count):
            key_scr[n * piece:(n + 1) * piece] = blocks[n][0, :piece]
            val_scr[n * piece:(n + 1) * piece] = blocks[n][0, piece:]
        lane = lax.broadcasted_iota(jnp.int32, (piece, keys), 1)
        k_pos = lane + me * piece
        for n in range(1, count):
            k_pos = jnp.where(lane >= n * piece, lane + s_ref[2 + n] - n * piece, k_pos)
        q_pos = lax.broadcasted_iota(jnp.int32, (piece, keys), 0) + me * piece
        low = jnp.where(q_pos >= cut, cut, 0)
        visible = (k_pos <= q_pos) & (k_pos >= low)
        cap = jnp.where(visible, jnp.inf, -jnp.inf)
        cap = jnp.concatenate([cap] * group, axis=0)
        cols = []
        for g in range(heads // group):
            q = q_ref[0, g * group:(g + 1) * group].reshape(group * piece, head)
            s = lax.dot_general(q, key_scr[:keys], (((1,), (1,)), ((), ())), preferred_element_type=jnp.float32)
            s = jnp.minimum(s, cap)
            m = jnp.max(s, axis=1, keepdims=True)
            p = jnp.exp2((s - m) * (scale * LOG2E))
            l = jnp.sum(p, axis=1, keepdims=True)
            o = jnp.dot(p.astype(jnp.bfloat16), val_scr[:keys], preferred_element_type=jnp.float32)
            o = o * (1.0 / l)
            o_ref[0, g * group:(g + 1) * group] = o.astype(jnp.bfloat16).reshape(group, piece, head)
            e = m * scale + jnp.log(l)
            for j in range(group):
                cols.append(e[j * piece:(j + 1) * piece])
        rows = jnp.concatenate(cols, axis=1).T
        lse_ref[:, pl.ds(base + step, 1), :] = rows[:, None, :]

    @pl.when(me < 2)
    def _():
        run(2)

    @pl.when(me >= 2)
    def _():
        run(4)


def attend(base, size, batch, scalars, q, own, near, fara, farb, prev):
    _, heads, piece, head = q.shape
    first = prev is None
    kv = pl.BlockSpec((1, 2 * piece, head), lambda i, s: (i, 0, 0))
    qspec = pl.BlockSpec((1, heads, piece, head), lambda i, s: (base + i, 0, 0, 0))
    lse = pl.BlockSpec((heads, batch, piece), lambda i, s: (0, 0, 0))
    in_specs = [qspec, kv, kv, kv, kv]
    args = [q, own, near, fara, farb]
    aliases = {}
    if not first:
        in_specs += [pl.BlockSpec(memory_space=pl.ANY), lse]
        args += list(prev)
        aliases = {6: 0}
    return pl.pallas_call(
        functools.partial(attend_kernel, first, heads),
        grid_spec=pltpu.PrefetchScalarGridSpec(
            num_scalar_prefetch=1,
            grid=(size,),
            in_specs=in_specs,
            out_specs=[qspec, lse],
            scratch_shapes=[pltpu.VMEM((4 * piece, head), jnp.bfloat16)] * 2,
        ),
        out_shape=[
            jax.ShapeDtypeStruct(q.shape, jnp.bfloat16),
            jax.ShapeDtypeStruct((heads, batch, piece), jnp.float32),
        ],
        input_output_aliases=aliases,
        compiler_params=pltpu.CompilerParams(dimension_semantics=("arbitrary",)),
        cost_estimate=pl.CostEstimate(
            flops=size * heads * piece * 4 * piece * head * 4,
            bytes_accessed=size * heads * piece * head * 4,
            transcendentals=0,
        ),
    )(scalars.at[0].set(base), *args)


def shift(x, pairs):
    return lax.ppermute(x, "cp", pairs)


def solution(mesh):
    def local(q_loc, k_loc, v_loc, seg_loc):
        batch, piece, _, _ = q_loc.shape
        me = lax.axis_index("cp")
        q = jnp.transpose(q_loc, (0, 2, 1, 3))
        kv = jnp.concatenate([k_loc, v_loc], axis=1)
        bounds = [sum(CHUNKS[:n]) for n in range(len(CHUNKS) + 1)]
        owns = [kv[a:b] for a, b in zip(bounds[:-1], bounds[1:])]
        fara = [shift(x, [(0, 2), (1, 3)]) for x in owns]
        near = [shift(x, [(0, 1), (2, 3)]) for x in owns]
        farb = [shift(x, [(2, 3), (3, 2)]) for x in fara]
        cuts = lax.psum(jnp.sum((seg_loc == 0).astype(jnp.int32), axis=1), "cp")
        head_scalars = jnp.stack([
            jnp.int32(0),
            me,
            jnp.int32(0),
            jnp.where(me % 2 == 1, (me - 1) * piece, 1 << 20),
            jnp.where(me >= 2, (me - 2) * piece, 1 << 20),
            jnp.where(me >= 2, (3 - me) * piece, 1 << 20),
        ]).astype(jnp.int32)
        scalars = jnp.concatenate([head_scalars, cuts])
        state = None
        for n, size in enumerate(CHUNKS):
            state = attend(bounds[n], size, batch, scalars, q, owns[n], near[n], fara[n], farb[n], state)
        out, lse = state
        return jnp.transpose(out, (0, 2, 1, 3)), jnp.transpose(lse, (1, 2, 0))

    return jax.shard_map(
        local,
        mesh=mesh,
        in_specs=(P("dp", "cp", None, None), P("dp", "cp", None), P("dp", "cp", None), P("dp", "cp")),
        out_specs=(P("dp", "cp", None, None), P("dp", "cp", None)),
        check_vma=False,
    )
```

```python
import functools

import jax
import jax.numpy as jnp
from jax import lax
from jax.experimental import pallas as pl
from jax.experimental.pallas import tpu as pltpu
from jax.sharding import PartitionSpec as P


CHUNKS = (2, 5, 6, 6, 6, 4, 2, 1)
GROUP = 2
LOG2E = 1.4426950408889634


def attend_kernel(first, base, s_ref, q_ref, kv_ref, near_k_ref, near_v_ref, fara_ref, farb_ref, *rest):
    if first:
        o_ref, lse_ref, vt_scr = rest
    else:
        _, lse_in, o_ref, lse_ref, vt_scr = rest
    step = pl.program_id(0)
    heads, piece, head = q_ref.shape[1:]
    width = GROUP * piece
    scale = head ** -0.5
    cut = s_ref[5 + base + step]
    me = s_ref[0]

    if not first:
        @pl.when(step == 0)
        def _():
            lse_ref[...] = lse_in[...]

    def run(count):
        keys = [kv_ref[0, :piece], near_k_ref[0], fara_ref[0, :piece], farb_ref[0, :piece]][:count]
        vals = [kv_ref[0, piece:], near_v_ref[0], fara_ref[0, piece:], farb_ref[0, piece:]][:count]
        caps = []
        for n in range(count):
            k_pos = lax.broadcasted_iota(jnp.int32, (piece, piece), 0) + s_ref[1 + n]
            q_pos = lax.broadcasted_iota(jnp.int32, (piece, piece), 1) + me * piece
            low = jnp.where(q_pos >= cut, cut, 0)
            caps.append(jnp.where((k_pos <= q_pos) & (k_pos >= low), jnp.inf, -jnp.inf))
            vt_scr[:, n * piece:(n + 1) * piece] = vals[n].T
        cap = jnp.concatenate(caps, axis=0)
        cap = jnp.concatenate([cap] * GROUP, axis=1)
        key = jnp.concatenate(keys, axis=0)
        for g in range(heads // GROUP):
            q = q_ref[0, g * GROUP:(g + 1) * GROUP].reshape(width, head)
            s = lax.dot_general(key, q, (((1,), (1,)), ((), ())), preferred_element_type=jnp.float32)
            s = jnp.minimum(s, cap)
            m = jnp.max(s, axis=0, keepdims=True)
            p = jnp.exp2((s - m) * (scale * LOG2E))
            l = jnp.sum(p, axis=0, keepdims=True)
            o = jnp.dot(vt_scr[:, :count * piece], p.astype(jnp.bfloat16), preferred_element_type=jnp.float32)
            o = o * (1.0 / l)
            o_ref[0, g * GROUP:(g + 1) * GROUP] = o.astype(jnp.bfloat16).T.reshape(GROUP, piece, head)
            e = m * scale + jnp.log(l)
            for j in range(GROUP):
                lse_ref[g * GROUP + j, pl.ds(base + step, 1), :] = e[:, j * piece:(j + 1) * piece]

    @pl.when(me < 2)
    def _():
        run(2)

    @pl.when(me >= 2)
    def _():
        run(4)


def attend(base, size, scalars, q, own, near, fara, farb, prev):
    batch, heads, piece, head = q.shape
    first = prev is None
    kv = pl.BlockSpec((1, 2 * piece, head), lambda i, s: (i, 0, 0))
    half = pl.BlockSpec((1, piece, head), lambda i, s: (base + i, 0, 0))
    qspec = pl.BlockSpec((1, heads, piece, head), lambda i, s: (base + i, 0, 0, 0))
    lse = pl.BlockSpec((heads, batch, piece), lambda i, s: (0, 0, 0))
    in_specs = [qspec, kv, half, half, kv, kv]
    args = [q, own, *near, fara, farb]
    aliases = {}
    if not first:
        in_specs += [pl.BlockSpec(memory_space=pl.ANY), lse]
        args += list(prev)
        aliases = {7: 0}
    return pl.pallas_call(
        functools.partial(attend_kernel, first, base),
        grid_spec=pltpu.PrefetchScalarGridSpec(
            num_scalar_prefetch=1,
            grid=(size,),
            in_specs=in_specs,
            out_specs=[qspec, lse],
            scratch_shapes=[pltpu.VMEM((head, 4 * piece), jnp.bfloat16)],
        ),
        out_shape=[
            jax.ShapeDtypeStruct(q.shape, jnp.bfloat16),
            jax.ShapeDtypeStruct((heads, batch, piece), jnp.float32),
        ],
        input_output_aliases=aliases,
        compiler_params=pltpu.CompilerParams(dimension_semantics=("arbitrary",)),
        cost_estimate=pl.CostEstimate(
            flops=size * heads * piece * 4 * piece * head * 4,
            bytes_accessed=size * heads * piece * head * 4,
            transcendentals=0,
        ),
    )(scalars, *args)


def shift(x, pairs):
    return lax.ppermute(x, "cp", pairs)


ACROSS = [(0, 2), (1, 3)]
BESIDE = [(0, 1), (2, 3)]
SWAP = [(2, 3), (3, 2)]


def solution(mesh):
    def local(q_loc, k_loc, v_loc, seg_loc):
        _, piece, _, _ = q_loc.shape
        me = lax.axis_index("cp")
        q = jnp.transpose(q_loc, (0, 2, 1, 3))
        bounds = [sum(CHUNKS[:n]) for n in range(len(CHUNKS) + 1)]
        owns = [jnp.concatenate([k_loc[a:b], v_loc[a:b]], axis=1) for a, b in zip(bounds[:-1], bounds[1:])]
        seg_a = shift(seg_loc, ACROSS)
        fara = [shift(x, ACROSS) for x in owns]
        seg_n = shift(seg_loc, BESIDE)
        near = [shift(k_loc, BESIDE), shift(v_loc, BESIDE)]
        seg_b = shift(seg_a, SWAP)
        farb = [shift(x, SWAP) for x in fara]

        def zeros(seg, there):
            return jnp.where(there, jnp.sum((seg == 0).astype(jnp.int32), axis=1), 0)

        odd, upper = me % 2 == 1, me >= 2
        cuts = zeros(seg_loc, True) + zeros(seg_n, odd) + zeros(seg_a, upper) + zeros(seg_b, upper)
        head_scalars = jnp.stack([
            me,
            me * piece,
            jnp.where(odd, (me - 1) * piece, 1 << 20),
            jnp.where(upper, (me - 2) * piece, 1 << 20),
            jnp.where(upper, (3 - me) * piece, 1 << 20),
        ]).astype(jnp.int32)
        scalars = jnp.concatenate([head_scalars, cuts])
        state = None
        for n, size in enumerate(CHUNKS):
            state = attend(bounds[n], size, scalars, q, owns[n], near, fara[n], farb[n], state)
        out, lse = state
        return jnp.transpose(out, (0, 2, 1, 3)), jnp.transpose(lse, (1, 2, 0))

    return jax.shard_map(
        local,
        mesh=mesh,
        in_specs=(P("dp", "cp", None, None), P("dp", "cp", None), P("dp", "cp", None), P("dp", "cp")),
        out_specs=(P("dp", "cp", None, None), P("dp", "cp", None)),
        check_vma=False,
    )
```

```python
import functools

import jax
import jax.numpy as jnp
from jax import lax
from jax.experimental import pallas as pl
from jax.experimental.pallas import tpu as pltpu
from jax.sharding import PartitionSpec as P


CHUNKS = (4, 8, 8, 7, 5)
BOUNDS = tuple(sum(CHUNKS[:n]) for n in range(len(CHUNKS) + 1))
GROUP = 2
LOG2E = 1.4426950408889634

ACROSS = [(0, 2), (1, 3)]
BESIDE = [(0, 1), (2, 3)]
SWAP = [(2, 3), (3, 2)]


def pack_kernel(ranges, tails, seg_ref, k_ref, v_ref, *rest):
    count = len(ranges)
    outs, (k_scr, v_scr, z_scr, in_sem, out_sem) = rest[:count], rest[count:]
    piece = k_ref.shape[1]
    first = min(a for a, _ in ranges)
    last = max(b for _, b in ranges)
    loads = [
        pltpu.make_async_copy(src.at[pl.ds(first, last - first)], dst.at[pl.ds(first, last - first)], in_sem.at[i])
        for i, (src, dst) in enumerate(((k_ref, k_scr), (v_ref, v_scr)))
    ]
    for load in loads:
        load.start()
    here = jnp.sum((seg_ref[...] == 0).astype(jnp.float32), axis=1, keepdims=True)
    z_scr[...] = jnp.broadcast_to(here, z_scr.shape).astype(jnp.bfloat16)
    for load in loads:
        load.wait()
    for out, (a, b), tail in zip(outs, ranges, tails):
        @pl.loop(0, b - a)
        def _(i):
            for half, src in enumerate((k_scr, v_scr)):
                pltpu.make_async_copy(
                    src.at[a + i], out.at[pl.ds(pl.multiple_of((2 * i + half) * piece, piece), piece)], out_sem
                ).start()

        if tail:
            pltpu.make_async_copy(z_scr, out.at[pl.ds((b - a) * 2 * piece, z_scr.shape[0])], out_sem).start()
    for out in outs:
        pltpu.make_async_copy(out, out, out_sem).wait()


def pack(ranges, tails, seg, k, v):
    batch, piece, head = k.shape
    return pl.pallas_call(
        functools.partial(pack_kernel, ranges, tails),
        in_specs=[pl.BlockSpec(memory_space=pltpu.VMEM)] + [pl.BlockSpec(memory_space=pl.ANY)] * 2,
        out_specs=[pl.BlockSpec(memory_space=pl.ANY)] * len(ranges),
        out_shape=[
            jax.ShapeDtypeStruct(((b - a) * 2 * piece + (batch if tail else 0), head), jnp.bfloat16)
            for (a, b), tail in zip(ranges, tails)
        ],
        scratch_shapes=[
            pltpu.VMEM(k.shape, jnp.bfloat16),
            pltpu.VMEM(k.shape, jnp.bfloat16),
            pltpu.VMEM((batch, head), jnp.bfloat16),
            pltpu.SemaphoreType.DMA((2,)),
            pltpu.SemaphoreType.DMA,
        ],
        cost_estimate=pl.CostEstimate(flops=1 << 20, bytes_accessed=4 * k.size, transcendentals=0),
    )(seg, k, v)


def attend_kernel(first, base, s_ref, q_ref, k_ref, v_ref, near_ref, fara_ref, farb_ref, *rest):
    if first:
        o_ref, lse_ref, k_scr, v_scr = rest
    else:
        _, lse_in, o_ref, lse_ref, k_scr, v_scr = rest
    step = pl.program_id(0)
    seq = base + step
    heads, piece, head = q_ref.shape[1:]
    batch = lse_ref.shape[1]
    width = GROUP * piece
    scale = head ** -0.5
    me, odd = s_ref[0], s_ref[1]
    cut, need = s_ref[2 + seq], s_ref[2 + batch + seq]

    if not first:
        @pl.when(step == 0)
        def _():
            lse_ref[...] = lse_in[...]

    def put(slot, k, v):
        k_scr[slot * piece:(slot + 1) * piece] = k
        v_scr[slot * piece:(slot + 1) * piece] = v

    put(0, k_ref[0], v_ref[0])

    @pl.when(odd == 1)
    def _():
        for slot, ref in enumerate((near_ref, fara_ref, farb_ref)):
            put(slot + 1, ref[:piece], ref[piece:])

    @pl.when(odd == 0)
    def _():
        for slot, ref in enumerate((farb_ref, fara_ref)):
            put(slot + 1, ref[:piece], ref[piece:])

    def run(count):
        keys = count * piece
        lane = lax.broadcasted_iota(jnp.int32, (piece, piece), 1)
        row = lax.broadcasted_iota(jnp.int32, (piece, piece), 0)
        low = jnp.maximum(jnp.where(row >= cut, cut, -keys), -me * piece)
        caps = [
            jnp.where((lane - n * piece <= row) & (lane - n * piece >= low), jnp.inf, -jnp.inf) for n in range(count)
        ]
        cap = jnp.concatenate([jnp.concatenate(caps, axis=1)] * GROUP, axis=0)
        logs = jnp.zeros((piece, piece), jnp.float32)

        def scores(g):
            q = q_ref[0, g * GROUP:(g + 1) * GROUP].reshape(width, head)
            s = lax.dot_general(q, k_scr[:keys], (((1,), (1,)), ((), ())), preferred_element_type=jnp.float32)
            s = jnp.minimum(s, cap)
            return s, jnp.max(s, axis=1, keepdims=True)

        def weigh(s, m):
            p = jnp.exp2((s - m) * (scale * LOG2E))
            return p.astype(jnp.bfloat16), m, jnp.sum(p, axis=1, keepdims=True)

        def finish(g, logs, p, m, l):
            o = jnp.dot(p, v_scr[:keys], preferred_element_type=jnp.float32) * (1.0 / l)
            o_ref[0, g * GROUP:(g + 1) * GROUP] = o.astype(jnp.bfloat16).reshape(GROUP, piece, head)
            e = m * scale + jnp.log(l)
            for j in range(GROUP):
                logs = jnp.where(lane == g * GROUP + j, e[j * piece:(j + 1) * piece], logs)
            return logs

        groups = heads // GROUP
        now, before = scores(0), None
        for g in range(groups):
            later = scores(g + 1) if g + 1 < groups else None
            if before is not None:
                logs = finish(g - 1, logs, *before)
            before, now = weigh(*now), later
        logs = finish(groups - 1, logs, *before)
        lse_ref[:, pl.ds(seq, 1), :] = logs.T[:heads][:, None, :]

    for count in (2, 3, 4):
        @pl.when((need == count) | (count == 2 and need == 1))
        def _():
            run(count)


def attend(n, scalars, q, k, v, near, fara, farb, prev):
    batch, heads, piece, head = q.shape
    base, size = BOUNDS[n], CHUNKS[n]
    first = prev is None
    own = pl.BlockSpec((1, piece, head), lambda i: (base + i, 0, 0))
    whole = pl.BlockSpec((2 * piece, head), lambda i: (base + i, 0))
    chunk = pl.BlockSpec((2 * piece, head), lambda i: (i, 0))
    qspec = pl.BlockSpec((1, heads, piece, head), lambda i: (base + i, 0, 0, 0))
    lse = pl.BlockSpec((heads, batch, piece), lambda i: (0, 0, 0))
    in_specs = [pl.BlockSpec(memory_space=pltpu.SMEM), qspec, own, own, whole, chunk, chunk]
    args = [scalars, q, k, v, near, fara, farb]
    aliases = {}
    if not first:
        in_specs += [pl.BlockSpec(memory_space=pl.ANY), lse]
        args += list(prev)
        aliases = {7: 0}
    return pl.pallas_call(
        functools.partial(attend_kernel, first, base),
        grid=(size,),
        in_specs=in_specs,
        out_specs=[qspec, lse],
        scratch_shapes=[pltpu.VMEM((4 * piece, head), jnp.bfloat16)] * 2,
        out_shape=[
            jax.ShapeDtypeStruct(q.shape, jnp.bfloat16),
            jax.ShapeDtypeStruct((heads, batch, piece), jnp.float32),
        ],
        input_output_aliases=aliases,
        compiler_params=pltpu.CompilerParams(dimension_semantics=("arbitrary",)),
        cost_estimate=pl.CostEstimate(
            flops=size * heads * piece * 4 * piece * head * 4,
            bytes_accessed=size * heads * piece * head * 4,
            transcendentals=0,
        ),
    )(*args)


def shift(x, pairs):
    return lax.ppermute(x, "cp", pairs)


def solution(mesh):
    def local(q_loc, k_loc, v_loc, seg_loc):
        batch, piece, _, _ = q_loc.shape
        me = lax.axis_index("cp")
        q = jnp.transpose(q_loc, (0, 2, 1, 3))
        ranges = tuple(zip(BOUNDS[:-1], BOUNDS[1:]))
        sends = pack(ranges[:1], (True,), seg_loc, k_loc, v_loc)
        *more, whole = pack(ranges[1:] + ((0, batch),), (False,) * len(ranges[1:]) + (True,), seg_loc, k_loc, v_loc)
        sends = list(sends) + more
        fara = [shift(x, ACROSS) for x in sends]
        near = shift(whole, BESIDE)
        farb = [shift(x, SWAP) for x in fara]

        def zeros(packed, there):
            return jnp.where(there, packed[-batch:, 0].astype(jnp.int32), 0)

        odd, upper = me % 2 == 1, me >= 2
        cuts = zeros(whole, True) + zeros(near, odd) + zeros(fara[0], upper) + zeros(farb[0], upper)
        need = jnp.where(cuts <= me * piece, me - cuts // piece, me) + 1
        scalars = jnp.concatenate([
            jnp.stack([me, me % 2]).astype(jnp.int32), cuts - me * piece, need.astype(jnp.int32)
        ])
        state = None
        for n in range(len(CHUNKS)):
            state = attend(n, scalars, q, k_loc, v_loc, near, fara[n], farb[n], state)
        out, lse = state
        return jnp.transpose(out, (0, 2, 1, 3)), jnp.transpose(lse, (1, 2, 0))

    return jax.shard_map(
        local,
        mesh=mesh,
        in_specs=(P("dp", "cp", None, None), P("dp", "cp", None), P("dp", "cp", None), P("dp", "cp")),
        out_specs=(P("dp", "cp", None, None), P("dp", "cp", None)),
        check_vma=False,
    )
```

```python
import functools

import jax
import jax.numpy as jnp
from jax import lax
from jax.experimental import pallas as pl
from jax.experimental.pallas import tpu as pltpu
from jax.sharding import PartitionSpec as P


CHUNKS = (4, 8, 8, 7, 3, 2)
BOUNDS = tuple(sum(CHUNKS[:n]) for n in range(len(CHUNKS) + 1))
GROUP = 2
DEPTH = 4
LOG2E = 1.4426950408889634

ACROSS = [(0, 2), (1, 3)]
BESIDE = [(0, 1), (2, 3)]
SWAP = [(2, 3), (3, 2)]


def pack_kernel(ranges, tails, seg_ref, k_ref, v_ref, *rest):
    count = len(ranges)
    outs, (k_scr, v_scr, z_scr, in_sem, out_sem) = rest[:count], rest[count:]
    piece = k_ref.shape[1]
    first = min(a for a, _ in ranges)
    last = max(b for _, b in ranges)
    loads = [
        pltpu.make_async_copy(src.at[pl.ds(first, last - first)], dst.at[pl.ds(first, last - first)], in_sem.at[i])
        for i, (src, dst) in enumerate(((k_ref, k_scr), (v_ref, v_scr)))
    ]
    for load in loads:
        load.start()
    here = jnp.sum((seg_ref[...] == 0).astype(jnp.float32), axis=1, keepdims=True)
    z_scr[...] = jnp.broadcast_to(here, z_scr.shape).astype(jnp.bfloat16)
    for load in loads:
        load.wait()
    for out, (a, b), tail in zip(outs, ranges, tails):
        @pl.loop(0, b - a)
        def _(i):
            for half, src in enumerate((k_scr, v_scr)):
                pltpu.make_async_copy(
                    src.at[a + i], out.at[pl.ds(pl.multiple_of((2 * i + half) * piece, piece), piece)], out_sem
                ).start()

        if tail:
            pltpu.make_async_copy(z_scr, out.at[pl.ds((b - a) * 2 * piece, z_scr.shape[0])], out_sem).start()
    for out in outs:
        pltpu.make_async_copy(out, out, out_sem).wait()


def pack(ranges, tails, seg, k, v):
    batch, piece, head = k.shape
    return pl.pallas_call(
        functools.partial(pack_kernel, ranges, tails),
        in_specs=[pl.BlockSpec(memory_space=pltpu.VMEM)] + [pl.BlockSpec(memory_space=pl.ANY)] * 2,
        out_specs=[pl.BlockSpec(memory_space=pl.ANY)] * len(ranges),
        out_shape=[
            jax.ShapeDtypeStruct(((b - a) * 2 * piece + (batch if tail else 0), head), jnp.bfloat16)
            for (a, b), tail in zip(ranges, tails)
        ],
        scratch_shapes=[
            pltpu.VMEM(k.shape, jnp.bfloat16),
            pltpu.VMEM(k.shape, jnp.bfloat16),
            pltpu.VMEM((batch, head), jnp.bfloat16),
            pltpu.SemaphoreType.DMA((2,)),
            pltpu.SemaphoreType.DMA,
        ],
        cost_estimate=pl.CostEstimate(flops=1 << 20, bytes_accessed=4 * k.size, transcendentals=0),
    )(seg, k, v)


def attend_kernel(first, base, size, s_ref, q_ref, k_ref, v_ref, near_ref, fara_ref, farb_ref, *rest):
    if first:
        o_ref, lse_ref, q_buf, k_buf, v_buf, o_buf, in_sem, out_sem = rest
    else:
        _, lse_in, o_ref, lse_ref, q_buf, k_buf, v_buf, o_buf, in_sem, out_sem = rest
        lse_ref[...] = lse_in[...]
    depth, heads, piece, head = q_buf.shape
    batch = lse_ref.shape[1]
    width = GROUP * piece
    scale = head ** -0.5
    me, odd = s_ref[0], s_ref[1]

    def loads(step):
        slot = lax.rem(step, depth)
        seq = base + step
        out = [
            pltpu.make_async_copy(q_ref.at[seq], q_buf.at[slot], in_sem.at[slot]),
            pltpu.make_async_copy(k_ref.at[seq], k_buf.at[slot, pl.ds(0, piece)], in_sem.at[slot]),
            pltpu.make_async_copy(v_ref.at[seq], v_buf.at[slot, pl.ds(0, piece)], in_sem.at[slot]),
        ]
        there = pl.ds(pl.multiple_of(jnp.where(odd == 1, 1, 3) * piece, piece), piece)
        for half, buf in enumerate((k_buf, v_buf)):
            rows = pl.ds(pl.multiple_of((2 * seq + half) * piece, piece), piece)
            out.append(pltpu.make_async_copy(near_ref.at[rows], buf.at[slot, there], in_sem.at[slot]))
        return out

    def place(step):
        slot = lax.rem(step, depth)
        for ref, block in ((fara_ref, 2), (farb_ref, jnp.where(odd == 1, 3, 1))):
            there = pl.ds(pl.multiple_of(block * piece, piece), piece)
            for half, buf in enumerate((k_buf, v_buf)):
                buf[slot, there] = ref[pl.ds(pl.multiple_of((2 * step + half) * piece, piece), piece)]

    def store(step):
        slot = lax.rem(step, 2)
        return pltpu.make_async_copy(o_buf.at[slot], o_ref.at[base + step], out_sem.at[slot])

    def run(count, seq, slot, out, cut):
        keys = count * piece
        lane = lax.broadcasted_iota(jnp.int32, (piece, piece), 1)
        row = lax.broadcasted_iota(jnp.int32, (piece, piece), 0)
        low = jnp.maximum(jnp.where(row >= cut, cut, -keys), -me * piece)
        caps = [
            jnp.where((lane - n * piece <= row) & (lane - n * piece >= low), jnp.inf, -jnp.inf) for n in range(count)
        ]
        cap = jnp.concatenate([jnp.concatenate(caps, axis=1)] * GROUP, axis=0)
        logs = jnp.zeros((piece, piece), jnp.float32)

        def scores(g):
            q = q_buf[slot, g * GROUP:(g + 1) * GROUP].reshape(width, head)
            s = lax.dot_general(q, k_buf[slot, :keys], (((1,), (1,)), ((), ())), preferred_element_type=jnp.float32)
            s = jnp.minimum(s, cap)
            return s, jnp.max(s, axis=1, keepdims=True)

        def weigh(s, m):
            p = jnp.exp2((s - m) * (scale * LOG2E))
            return p.astype(jnp.bfloat16), m, jnp.sum(p, axis=1, keepdims=True)

        def finish(g, logs, p, m, l):
            o = jnp.dot(p, v_buf[slot, :keys], preferred_element_type=jnp.float32) * (1.0 / l)
            o_buf[out, g * GROUP:(g + 1) * GROUP] = o.astype(jnp.bfloat16).reshape(GROUP, piece, head)
            e = m * scale + jnp.log(l)
            for j in range(GROUP):
                logs = jnp.where(lane == g * GROUP + j, e[j * piece:(j + 1) * piece], logs)
            return logs

        groups = heads // GROUP
        now, before = scores(0), None
        for g in range(groups):
            later = scores(g + 1) if g + 1 < groups else None
            if before is not None:
                logs = finish(g - 1, logs, *before)
            before, now = weigh(*now), later
        logs = finish(groups - 1, logs, *before)
        lse_ref[:, pl.ds(seq, 1), :] = logs.T[:heads][:, None, :]

    for step in range(min(depth - 1, size)):
        for load in loads(step):
            load.start()

    @pl.loop(0, size)
    def _(step):
        seq = base + step

        @pl.when(step + depth - 1 < size)
        def _():
            for load in loads(step + depth - 1):
                load.start()

        @pl.when(step >= 2)
        def _():
            store(step - 2).wait()

        for load in loads(step):
            load.wait()
        place(step)
        cut, need = s_ref[2 + seq], s_ref[2 + batch + seq]
        for count in (2, 3, 4):
            @pl.when((need == count) | (count == 2 and need == 1))
            def _():
                run(count, seq, lax.rem(step, depth), lax.rem(step, 2), cut)
        store(step).start()

    for step in range(max(size - 2, 0), size):
        store(step).wait()


def attend(n, scalars, q, k, v, near, fara, farb, prev):
    batch, heads, piece, head = q.shape
    base, size = BOUNDS[n], CHUNKS[n]
    first = prev is None
    hbm = pl.BlockSpec(memory_space=pltpu.HBM)
    vmem = pl.BlockSpec(memory_space=pltpu.VMEM)
    in_specs = [pl.BlockSpec(memory_space=pltpu.SMEM)] + [hbm] * 4 + [vmem] * 2
    q, k, v, near = (pltpu.with_memory_space_constraint(x, pltpu.HBM) for x in (q, k, v, near))
    args = [scalars, q, k, v, near, fara, farb]
    aliases = {}
    if not first:
        in_specs += [hbm, vmem]
        args += list(prev)
        aliases = {7: 0}
    return pl.pallas_call(
        functools.partial(attend_kernel, first, base, size),
        in_specs=in_specs,
        out_specs=[hbm, vmem],
        scratch_shapes=[
            pltpu.VMEM((DEPTH, heads, piece, head), jnp.bfloat16),
            pltpu.VMEM((DEPTH, 4 * piece, head), jnp.bfloat16),
            pltpu.VMEM((DEPTH, 4 * piece, head), jnp.bfloat16),
            pltpu.VMEM((2, heads, piece, head), jnp.bfloat16),
            pltpu.SemaphoreType.DMA((DEPTH,)),
            pltpu.SemaphoreType.DMA((2,)),
        ],
        out_shape=[
            jax.ShapeDtypeStruct(q.shape, jnp.bfloat16),
            jax.ShapeDtypeStruct((heads, batch, piece), jnp.float32),
        ],
        input_output_aliases=aliases,
        compiler_params=pltpu.CompilerParams(vmem_limit_bytes=32 << 20),
        cost_estimate=pl.CostEstimate(
            flops=size * heads * piece * 4 * piece * head * 4,
            bytes_accessed=size * heads * piece * head * 4,
            transcendentals=0,
        ),
    )(*args)


def shift(x, pairs):
    return lax.ppermute(x, "cp", pairs)


def solution(mesh):
    def local(q_loc, k_loc, v_loc, seg_loc):
        batch, piece, _, _ = q_loc.shape
        me = lax.axis_index("cp")
        q = jnp.transpose(q_loc, (0, 2, 1, 3))
        ranges = tuple(zip(BOUNDS[:-1], BOUNDS[1:]))
        sends = pack(ranges[:1], (True,), seg_loc, k_loc, v_loc)
        *more, whole = pack(ranges[1:] + ((0, batch),), (False,) * len(ranges[1:]) + (True,), seg_loc, k_loc, v_loc)
        sends = list(sends) + more
        fara = [shift(x, ACROSS) for x in sends]
        near = shift(whole, BESIDE)
        farb = [shift(x, SWAP) for x in fara]

        def zeros(packed, there):
            return jnp.where(there, packed[-batch:, 0].astype(jnp.int32), 0)

        odd, upper = me % 2 == 1, me >= 2
        cuts = zeros(whole, True) + zeros(near, odd) + zeros(fara[0], upper) + zeros(farb[0], upper)
        need = jnp.where(cuts <= me * piece, me - cuts // piece, me) + 1
        scalars = jnp.concatenate([
            jnp.stack([me, me % 2]).astype(jnp.int32), cuts - me * piece, need.astype(jnp.int32)
        ])
        state = None
        for n in range(len(CHUNKS)):
            state = attend(n, scalars, q, k_loc, v_loc, near, fara[n], farb[n], state)
        out, lse = state
        return jnp.transpose(out, (0, 2, 1, 3)), jnp.transpose(lse, (1, 2, 0))

    return jax.shard_map(
        local,
        mesh=mesh,
        in_specs=(P("dp", "cp", None, None), P("dp", "cp", None), P("dp", "cp", None), P("dp", "cp")),
        out_specs=(P("dp", "cp", None, None), P("dp", "cp", None)),
        check_vma=False,
    )
```

```python
import functools

import jax
import jax.numpy as jnp
from jax import lax
from jax.experimental import pallas as pl
from jax.experimental.pallas import tpu as pltpu
from jax.sharding import PartitionSpec as P


CHUNKS = (6, 10, 9, 5, 2)
BOUNDS = tuple(sum(CHUNKS[:n]) for n in range(len(CHUNKS) + 1))
GROUP = 2
DEPTH = 3
LOG2E = 1.4426950408889634

ACROSS = [(0, 2), (1, 3)]
BESIDE = [(0, 1), (2, 3)]
SWAP = [(2, 3), (3, 2)]


def pack_kernel(ranges, tails, seg_ref, k_ref, v_ref, *rest):
    count = len(ranges)
    outs, (k_scr, v_scr, z_scr, in_sem, out_sem) = rest[:count], rest[count:]
    piece = k_ref.shape[1]
    first = min(a for a, _ in ranges)
    last = max(b for _, b in ranges)
    loads = [
        pltpu.make_async_copy(src.at[pl.ds(first, last - first)], dst.at[pl.ds(first, last - first)], in_sem.at[i])
        for i, (src, dst) in enumerate(((k_ref, k_scr), (v_ref, v_scr)))
    ]
    for load in loads:
        load.start()
    here = jnp.sum((seg_ref[...] == 0).astype(jnp.float32), axis=1, keepdims=True)
    z_scr[...] = jnp.broadcast_to(here, z_scr.shape).astype(jnp.bfloat16)
    for load in loads:
        load.wait()
    for out, (a, b), tail in zip(outs, ranges, tails):
        @pl.loop(0, b - a)
        def _(i):
            for half, src in enumerate((k_scr, v_scr)):
                pltpu.make_async_copy(
                    src.at[a + i], out.at[pl.ds(pl.multiple_of((2 * i + half) * piece, piece), piece)], out_sem
                ).start()

        if tail:
            pltpu.make_async_copy(z_scr, out.at[pl.ds((b - a) * 2 * piece, z_scr.shape[0])], out_sem).start()
    for out in outs:
        pltpu.make_async_copy(out, out, out_sem).wait()


def pack(ranges, tails, seg, k, v):
    batch, piece, head = k.shape
    return pl.pallas_call(
        functools.partial(pack_kernel, ranges, tails),
        in_specs=[pl.BlockSpec(memory_space=pltpu.VMEM)] + [pl.BlockSpec(memory_space=pl.ANY)] * 2,
        out_specs=[pl.BlockSpec(memory_space=pl.ANY)] * len(ranges),
        out_shape=[
            jax.ShapeDtypeStruct(((b - a) * 2 * piece + (batch if tail else 0), head), jnp.bfloat16)
            for (a, b), tail in zip(ranges, tails)
        ],
        scratch_shapes=[
            pltpu.VMEM(k.shape, jnp.bfloat16),
            pltpu.VMEM(k.shape, jnp.bfloat16),
            pltpu.VMEM((batch, head), jnp.bfloat16),
            pltpu.SemaphoreType.DMA((2,)),
            pltpu.SemaphoreType.DMA,
        ],
        cost_estimate=pl.CostEstimate(flops=1 << 20, bytes_accessed=4 * k.size, transcendentals=0),
    )(seg, k, v)


def attend_kernel(first, base, size, s_hbm, q_ref, k_ref, v_ref, near_ref, fara_ref, farb_ref, *rest):
    if first:
        o_ref, lse_ref, *scratch = rest
    else:
        _, lse_in, o_ref, lse_ref, *scratch = rest
    s_ref, q_buf, k_buf, v_buf, o_buf, s_sem, kv_sem, q_sem, o_sem = scratch
    depth, heads, piece, head = q_buf.shape
    groups = heads // GROUP
    width = GROUP * piece
    scale = head ** -0.5
    me = lax.axis_index("cp")
    odd = lax.rem(me, 2)
    scalars = pltpu.make_async_copy(s_hbm, s_ref, s_sem)
    scalars.start()

    def kv_loads(step):
        slot = lax.rem(step, depth)
        seq = base + step
        there = pl.ds(pl.multiple_of(jnp.where(odd == 1, 1, 3) * piece, piece), piece)
        out = []
        for half, (ref, buf) in enumerate(((k_ref, k_buf), (v_ref, v_buf))):
            rows = pl.ds(pl.multiple_of((2 * seq + half) * piece, piece), piece)
            out.append(pltpu.make_async_copy(ref.at[seq], buf.at[slot, pl.ds(0, piece)], kv_sem.at[slot]))
            out.append(pltpu.make_async_copy(near_ref.at[rows], buf.at[slot, there], kv_sem.at[slot]))
        return out

    def part(g):
        return pl.ds(g * GROUP, GROUP)

    def q_load(step, g):
        slot = lax.rem(step, depth)
        return pltpu.make_async_copy(q_ref.at[base + step, part(g)], q_buf.at[slot, part(g)], q_sem.at[slot, g])

    def o_store(step, g):
        slot = lax.rem(step, 2)
        return pltpu.make_async_copy(o_buf.at[slot, part(g)], o_ref.at[base + step, part(g)], o_sem.at[slot, g])

    def load(step):
        for copy in kv_loads(step):
            copy.start()
        for g in range(groups):
            q_load(step, g).start()

    def place(step):
        slot = lax.rem(step, depth)
        for ref, block in ((fara_ref, 2), (farb_ref, jnp.where(odd == 1, 3, 1))):
            there = pl.ds(pl.multiple_of(block * piece, piece), piece)
            for half, buf in enumerate((k_buf, v_buf)):
                buf[slot, there] = ref[pl.ds(pl.multiple_of((2 * step + half) * piece, piece), piece)]

    def run(count, step, cut):
        seq = base + step
        slot, out = lax.rem(step, depth), lax.rem(step, 2)
        keys = count * piece
        lane = lax.broadcasted_iota(jnp.int32, (piece, piece), 1)
        row = lax.broadcasted_iota(jnp.int32, (piece, piece), 0)
        low = jnp.maximum(jnp.where(row >= cut, cut, -keys), -me * piece)
        caps = [
            jnp.where((lane - n * piece <= row) & (lane - n * piece >= low), jnp.inf, -jnp.inf) for n in range(count)
        ]
        cap = jnp.concatenate([jnp.concatenate(caps, axis=1)] * GROUP, axis=0)
        logs = jnp.zeros((piece, piece), jnp.float32)

        def scores(g):
            q = q_buf[slot, g * GROUP:(g + 1) * GROUP].reshape(width, head)
            s = lax.dot_general(q, k_buf[slot, :keys], (((1,), (1,)), ((), ())), preferred_element_type=jnp.float32)
            s = jnp.minimum(s, cap)
            return s, jnp.max(s, axis=1, keepdims=True)

        def weigh(s, m):
            p = jnp.exp2((s - m) * (scale * LOG2E))
            return p.astype(jnp.bfloat16), m, jnp.sum(p, axis=1, keepdims=True)

        def finish(g, logs, p, m, l):
            o = jnp.dot(p, v_buf[slot, :keys], preferred_element_type=jnp.float32) * (1.0 / l)
            o_buf[out, g * GROUP:(g + 1) * GROUP] = o.astype(jnp.bfloat16).reshape(GROUP, piece, head)
            e = m * scale + jnp.log(l)
            for j in range(GROUP):
                logs = jnp.where(lane == g * GROUP + j, e[j * piece:(j + 1) * piece], logs)
            return logs

        now, before = scores(0), None
        for g in range(groups):
            later = scores(g + 1) if g + 1 < groups else None
            if before is not None:
                logs = finish(g - 1, logs, *before)
            before, now = weigh(*now), later
        logs = finish(groups - 1, logs, *before)
        lse_ref[:, pl.ds(seq, 1), :] = logs.T[:heads][:, None, :]

    load(0)
    if size > 1:
        load(1)
    if not first:
        lse_ref[...] = lse_in[...]
    scalars.wait()

    @pl.loop(0, size)
    def _(step):
        for copy in kv_loads(step):
            copy.wait()
        for g in range(groups):
            q_load(step, g).wait()

        @pl.when(step + 2 < size)
        def _():
            load(step + 2)

        @pl.when(step >= 2)
        def _():
            for g in range(groups):
                o_store(step - 2, g).wait()

        place(step)
        run(4, step, s_ref[base + step])
        for g in range(groups):
            o_store(step, g).start()

    for step in range(max(size - 2, 0), size):
        for g in range(groups):
            o_store(step, g).wait()


def attend(n, scalars, q, k, v, near, fara, farb, prev):
    batch, heads, piece, head = q.shape
    base, size = BOUNDS[n], CHUNKS[n]
    first = prev is None
    hbm = pl.BlockSpec(memory_space=pltpu.HBM)
    vmem = pl.BlockSpec(memory_space=pltpu.VMEM)
    in_specs = [hbm] * 5 + [vmem] * 2
    scalars, q, k, v, near = (pltpu.with_memory_space_constraint(x, pltpu.HBM) for x in (scalars, q, k, v, near))
    args = [scalars, q, k, v, near, fara, farb]
    aliases = {}
    if not first:
        in_specs += [hbm, vmem]
        args += list(prev)
        aliases = {7: 0}
    return pl.pallas_call(
        functools.partial(attend_kernel, first, base, size),
        in_specs=in_specs,
        out_specs=[hbm, vmem],
        scratch_shapes=[
            pltpu.SMEM(scalars.shape, jnp.int32),
            pltpu.VMEM((DEPTH, heads, piece, head), jnp.bfloat16),
            pltpu.VMEM((DEPTH, 4 * piece, head), jnp.bfloat16),
            pltpu.VMEM((DEPTH, 4 * piece, head), jnp.bfloat16),
            pltpu.VMEM((2, heads, piece, head), jnp.bfloat16),
            pltpu.SemaphoreType.DMA,
            pltpu.SemaphoreType.DMA((DEPTH,)),
            pltpu.SemaphoreType.DMA((DEPTH, heads // GROUP)),
            pltpu.SemaphoreType.DMA((2, heads // GROUP)),
        ],
        out_shape=[
            jax.ShapeDtypeStruct(q.shape, jnp.bfloat16),
            jax.ShapeDtypeStruct((heads, batch, piece), jnp.float32),
        ],
        input_output_aliases=aliases,
        compiler_params=pltpu.CompilerParams(vmem_limit_bytes=32 << 20),
        cost_estimate=pl.CostEstimate(
            flops=size * heads * piece * 4 * piece * head * 4,
            bytes_accessed=size * heads * piece * head * 4,
            transcendentals=0,
        ),
    )(*args)


def shift(x, pairs):
    return lax.ppermute(x, "cp", pairs)


def solution(mesh):
    def local(q_loc, k_loc, v_loc, seg_loc):
        batch, piece, _, _ = q_loc.shape
        me = lax.axis_index("cp")
        q = jnp.transpose(q_loc, (0, 2, 1, 3))
        ranges = tuple(zip(BOUNDS[:-1], BOUNDS[1:]))
        sends = pack(ranges[:1], (True,), seg_loc, k_loc, v_loc)
        *more, whole = pack(ranges[1:] + ((0, batch),), (False,) * len(ranges[1:]) + (True,), seg_loc, k_loc, v_loc)
        sends = list(sends) + more
        fara = [shift(x, ACROSS) for x in sends]
        near = shift(whole, BESIDE)
        farb = [shift(x, SWAP) for x in fara]

        def zeros(packed, there):
            return jnp.where(there, packed[-batch:, 0].astype(jnp.int32), 0)

        odd, upper = me % 2 == 1, me >= 2
        cuts = zeros(whole, True) + zeros(near, odd) + zeros(fara[0], upper) + zeros(farb[0], upper)
        need = jnp.where(cuts <= me * piece, me - cuts // piece, me) + 1
        scalars = jnp.concatenate([cuts - me * piece, need.astype(jnp.int32)])
        state = None
        for n in range(len(CHUNKS)):
            state = attend(n, scalars, q, k_loc, v_loc, near, fara[n], farb[n], state)
        out, lse = state
        return jnp.transpose(out, (0, 2, 1, 3)), jnp.transpose(lse, (1, 2, 0))

    return jax.shard_map(
        local,
        mesh=mesh,
        in_specs=(P("dp", "cp", None, None), P("dp", "cp", None), P("dp", "cp", None), P("dp", "cp")),
        out_specs=(P("dp", "cp", None, None), P("dp", "cp", None)),
        check_vma=False,
    )
```

```python
import functools

import jax
import jax.numpy as jnp
from jax import lax
from jax.experimental import pallas as pl
from jax.experimental.pallas import tpu as pltpu
from jax.sharding import PartitionSpec as P


CHUNKS = (6, 6, 5, 5, 5, 5)
BOUNDS = tuple(sum(CHUNKS[:n]) for n in range(len(CHUNKS) + 1))
GROUP = 2
DEPTH = 3
LOG2E = 1.4426950408889634

ACROSS = [(0, 2), (1, 3)]
BESIDE = [(0, 1), (2, 3)]
SWAP = [(2, 3), (3, 2)]


def pack_kernel(ranges, tails, seg_ref, k_ref, v_ref, *rest):
    count = len(ranges)
    outs, (k_scr, v_scr, z_scr, in_sem, out_sem) = rest[:count], rest[count:]
    piece = k_ref.shape[1]
    first = min(a for a, _ in ranges)
    last = max(b for _, b in ranges)
    loads = [
        pltpu.make_async_copy(src.at[pl.ds(first, last - first)], dst.at[pl.ds(first, last - first)], in_sem.at[i])
        for i, (src, dst) in enumerate(((k_ref, k_scr), (v_ref, v_scr)))
    ]
    for load in loads:
        load.start()
    here = jnp.sum((seg_ref[...] == 0).astype(jnp.float32), axis=1, keepdims=True)
    z_scr[...] = jnp.broadcast_to(here, z_scr.shape).astype(jnp.bfloat16)
    for load in loads:
        load.wait()
    for out, (a, b), tail in zip(outs, ranges, tails):
        @pl.loop(0, b - a)
        def _(i):
            for half, src in enumerate((k_scr, v_scr)):
                pltpu.make_async_copy(
                    src.at[a + i], out.at[pl.ds(pl.multiple_of((2 * i + half) * piece, piece), piece)], out_sem
                ).start()

        if tail:
            pltpu.make_async_copy(z_scr, out.at[pl.ds((b - a) * 2 * piece, z_scr.shape[0])], out_sem).start()
    for out in outs:
        pltpu.make_async_copy(out, out, out_sem).wait()


def pack(ranges, tails, seg, k, v):
    batch, piece, head = k.shape
    return pl.pallas_call(
        functools.partial(pack_kernel, ranges, tails),
        in_specs=[pl.BlockSpec(memory_space=pltpu.VMEM)] + [pl.BlockSpec(memory_space=pl.ANY)] * 2,
        out_specs=[pl.BlockSpec(memory_space=pl.ANY)] * len(ranges),
        out_shape=[
            jax.ShapeDtypeStruct(((b - a) * 2 * piece + (batch if tail else 0), head), jnp.bfloat16)
            for (a, b), tail in zip(ranges, tails)
        ],
        scratch_shapes=[
            pltpu.VMEM(k.shape, jnp.bfloat16),
            pltpu.VMEM(k.shape, jnp.bfloat16),
            pltpu.VMEM((batch, head), jnp.bfloat16),
            pltpu.SemaphoreType.DMA((2,)),
            pltpu.SemaphoreType.DMA,
        ],
        cost_estimate=pl.CostEstimate(flops=1 << 20, bytes_accessed=4 * k.size, transcendentals=0),
    )(seg, k, v)


def attend_kernel(first, base, size, s_hbm, q_ref, k_ref, v_ref, near_ref, fara_ref, farb_ref, *rest):
    if first:
        o_ref, lse_ref, *scratch = rest
    else:
        _, lse_in, o_ref, lse_ref, *scratch = rest
    s_ref, q_buf, k_buf, v_buf, o_buf, s_sem, kv_sem, q_sem, o_sem = scratch
    depth, heads, piece, head = q_buf.shape
    batch = lse_ref.shape[1]
    groups = heads // GROUP
    width = GROUP * piece
    scale = head ** -0.5
    me = lax.axis_index("cp")
    odd = lax.rem(me, 2)
    scalars = pltpu.make_async_copy(s_hbm, s_ref, s_sem)
    scalars.start()

    def kv_loads(step):
        slot = lax.rem(step, depth)
        seq = base + step
        there = pl.ds(pl.multiple_of(jnp.where(odd == 1, 1, 3) * piece, piece), piece)
        out = []
        for half, (ref, buf) in enumerate(((k_ref, k_buf), (v_ref, v_buf))):
            rows = pl.ds(pl.multiple_of((2 * seq + half) * piece, piece), piece)
            out.append(pltpu.make_async_copy(ref.at[seq], buf.at[slot, pl.ds(0, piece)], kv_sem.at[slot]))
            out.append(pltpu.make_async_copy(near_ref.at[rows], buf.at[slot, there], kv_sem.at[slot]))
        return out

    def part(g):
        return pl.ds(g * GROUP, GROUP)

    def q_load(step, g):
        slot = lax.rem(step, depth)
        return pltpu.make_async_copy(q_ref.at[base + step, part(g)], q_buf.at[slot, part(g)], q_sem.at[slot, g])

    def o_store(step, g):
        slot = lax.rem(step, 2)
        return pltpu.make_async_copy(o_buf.at[slot, part(g)], o_ref.at[base + step, part(g)], o_sem.at[slot, g])

    def load(step):
        for copy in kv_loads(step):
            copy.start()
        for g in range(groups):
            q_load(step, g).start()

    def place(step):
        slot = lax.rem(step, depth)
        for ref, block in ((fara_ref, 2), (farb_ref, jnp.where(odd == 1, 3, 1))):
            there = pl.ds(pl.multiple_of(block * piece, piece), piece)
            for half, buf in enumerate((k_buf, v_buf)):
                buf[slot, there] = ref[pl.ds(pl.multiple_of((2 * step + half) * piece, piece), piece)]

    def run(count, step, cut):
        seq = base + step
        slot, out = lax.rem(step, depth), lax.rem(step, 2)
        keys = count * piece
        lane = lax.broadcasted_iota(jnp.int32, (piece, piece), 1)
        row = lax.broadcasted_iota(jnp.int32, (piece, piece), 0)
        low = jnp.maximum(jnp.where(row >= cut, cut, -keys), -me * piece)
        caps = [
            jnp.where((lane - n * piece <= row) & (lane - n * piece >= low), jnp.inf, -jnp.inf) for n in range(count)
        ]
        cap = jnp.concatenate([jnp.concatenate(caps, axis=1)] * GROUP, axis=0)
        logs = jnp.zeros((piece, piece), jnp.float32)

        def scores(g):
            q = q_buf[slot, g * GROUP:(g + 1) * GROUP].reshape(width, head)
            s = lax.dot_general(q, k_buf[slot, :keys], (((1,), (1,)), ((), ())), preferred_element_type=jnp.float32)
            s = jnp.minimum(s, cap)
            return s, jnp.max(s, axis=1, keepdims=True)

        def weigh(s, m):
            p = jnp.exp2((s - m) * (scale * LOG2E))
            return p.astype(jnp.bfloat16), m, jnp.sum(p, axis=1, keepdims=True)

        def finish(g, logs, p, m, l):
            o = jnp.dot(p, v_buf[slot, :keys], preferred_element_type=jnp.float32) * (1.0 / l)
            o_buf[out, g * GROUP:(g + 1) * GROUP] = o.astype(jnp.bfloat16).reshape(GROUP, piece, head)
            e = m * scale + jnp.log(l)
            for j in range(GROUP):
                logs = jnp.where(lane == g * GROUP + j, e[j * piece:(j + 1) * piece], logs)
            return logs

        now, before = scores(0), None
        for g in range(groups):
            later = scores(g + 1) if g + 1 < groups else None
            if before is not None:
                logs = finish(g - 1, logs, *before)
            before, now = weigh(*now), later
        logs = finish(groups - 1, logs, *before)
        lse_ref[:, pl.ds(seq, 1), :] = logs.T[:heads][:, None, :]

    load(0)
    if size > 1:
        load(1)
    if not first:
        lse_ref[...] = lse_in[...]
    scalars.wait()

    @pl.loop(0, size)
    def _(step):
        for copy in kv_loads(step):
            copy.wait()
        for g in range(groups):
            q_load(step, g).wait()

        @pl.when(step + 2 < size)
        def _():
            load(step + 2)

        @pl.when(step >= 2)
        def _():
            for g in range(groups):
                o_store(step - 2, g).wait()

        place(step)
        cut, need = s_ref[base + step], s_ref[batch + base + step]
        for count in (2, 3, 4):
            @pl.when((need == count) | (count == 2 and need == 1))
            def _():
                run(count, step, cut)
        for g in range(groups):
            o_store(step, g).start()

    for step in range(max(size - 2, 0), size):
        for g in range(groups):
            o_store(step, g).wait()


def attend(n, scalars, q, k, v, near, fara, farb, prev):
    batch, heads, piece, head = q.shape
    base, size = BOUNDS[n], CHUNKS[n]
    first = prev is None
    hbm = pl.BlockSpec(memory_space=pltpu.HBM)
    vmem = pl.BlockSpec(memory_space=pltpu.VMEM)
    in_specs = [hbm] * 5 + [vmem] * 2
    scalars, q, k, v, near = (pltpu.with_memory_space_constraint(x, pltpu.HBM) for x in (scalars, q, k, v, near))
    args = [scalars, q, k, v, near, fara, farb]
    aliases = {}
    if not first:
        in_specs += [hbm, vmem]
        args += list(prev)
        aliases = {7: 0}
    return pl.pallas_call(
        functools.partial(attend_kernel, first, base, size),
        in_specs=in_specs,
        out_specs=[hbm, vmem],
        scratch_shapes=[
            pltpu.SMEM(scalars.shape, jnp.int32),
            pltpu.VMEM((DEPTH, heads, piece, head), jnp.bfloat16),
            pltpu.VMEM((DEPTH, 4 * piece, head), jnp.bfloat16),
            pltpu.VMEM((DEPTH, 4 * piece, head), jnp.bfloat16),
            pltpu.VMEM((2, heads, piece, head), jnp.bfloat16),
            pltpu.SemaphoreType.DMA,
            pltpu.SemaphoreType.DMA((DEPTH,)),
            pltpu.SemaphoreType.DMA((DEPTH, heads // GROUP)),
            pltpu.SemaphoreType.DMA((2, heads // GROUP)),
        ],
        out_shape=[
            jax.ShapeDtypeStruct(q.shape, jnp.bfloat16),
            jax.ShapeDtypeStruct((heads, batch, piece), jnp.float32),
        ],
        input_output_aliases=aliases,
        compiler_params=pltpu.CompilerParams(vmem_limit_bytes=32 << 20),
        cost_estimate=pl.CostEstimate(
            flops=size * heads * piece * 4 * piece * head * 4,
            bytes_accessed=size * heads * piece * head * 4,
            transcendentals=0,
        ),
    )(*args)


def shift(x, pairs):
    return lax.ppermute(x, "cp", pairs)


def solution(mesh):
    def local(q_loc, k_loc, v_loc, seg_loc):
        batch, piece, _, _ = q_loc.shape
        me = lax.axis_index("cp")
        q = jnp.transpose(q_loc, (0, 2, 1, 3))
        ranges = tuple(zip(BOUNDS[:-1], BOUNDS[1:]))
        sends = pack(ranges[:1], (True,), seg_loc, k_loc, v_loc)
        *more, whole = pack(ranges[1:] + ((0, batch),), (False,) * len(ranges[1:]) + (True,), seg_loc, k_loc, v_loc)
        sends = list(sends) + more
        fara = [shift(x, ACROSS) for x in sends]
        near = shift(whole, BESIDE)
        farb = [shift(x, SWAP) for x in fara]

        def zeros(packed, there):
            return jnp.where(there, packed[-batch:, 0].astype(jnp.int32), 0)

        odd, upper = me % 2 == 1, me >= 2
        cuts = zeros(whole, True) + zeros(near, odd) + zeros(fara[0], upper) + zeros(farb[0], upper)
        need = jnp.where(cuts <= me * piece, me - cuts // piece, me) + 1
        scalars = jnp.concatenate([cuts - me * piece, need.astype(jnp.int32)])
        state = None
        for n in range(len(CHUNKS)):
            state = attend(n, scalars, q, k_loc, v_loc, near, fara[n], farb[n], state)
        out, lse = state
        return jnp.transpose(out, (0, 2, 1, 3)), jnp.transpose(lse, (1, 2, 0))

    return jax.shard_map(
        local,
        mesh=mesh,
        in_specs=(P("dp", "cp", None, None), P("dp", "cp", None), P("dp", "cp", None), P("dp", "cp")),
        out_specs=(P("dp", "cp", None, None), P("dp", "cp", None)),
        check_vma=False,
    )
```

```python
import functools

import jax
import jax.numpy as jnp
from jax import lax
from jax.experimental import pallas as pl
from jax.experimental.pallas import tpu as pltpu
from jax.sharding import PartitionSpec as P


CHUNKS = (6, 6, 5, 5, 5, 5)
BOUNDS = tuple(sum(CHUNKS[:n]) for n in range(len(CHUNKS) + 1))
GROUP = 2
DEPTH = 3
LOG2E = 1.4426950408889634

ACROSS = [(0, 2), (1, 3)]
BESIDE = [(0, 1), (2, 3)]
SWAP = [(2, 3), (3, 2)]


def pack_kernel(ranges, tails, seg_ref, k_ref, v_ref, *rest):
    count = len(ranges)
    outs, (k_scr, v_scr, z_scr, in_sem, out_sem) = rest[:count], rest[count:]
    piece = k_ref.shape[1]
    first = min(a for a, _ in ranges)
    last = max(b for _, b in ranges)
    loads = [
        pltpu.make_async_copy(src.at[pl.ds(first, last - first)], dst.at[pl.ds(first, last - first)], in_sem.at[i])
        for i, (src, dst) in enumerate(((k_ref, k_scr), (v_ref, v_scr)))
    ]
    for load in loads:
        load.start()
    here = jnp.sum((seg_ref[...] == 0).astype(jnp.float32), axis=1, keepdims=True)
    z_scr[...] = jnp.broadcast_to(here, z_scr.shape).astype(jnp.bfloat16)
    for load in loads:
        load.wait()
    for out, (a, b), tail in zip(outs, ranges, tails):
        @pl.loop(0, b - a)
        def _(i):
            for half, src in enumerate((k_scr, v_scr)):
                pltpu.make_async_copy(
                    src.at[a + i], out.at[pl.ds(pl.multiple_of((2 * i + half) * piece, piece), piece)], out_sem
                ).start()

        if tail:
            pltpu.make_async_copy(z_scr, out.at[pl.ds((b - a) * 2 * piece, z_scr.shape[0])], out_sem).start()
    for out in outs:
        pltpu.make_async_copy(out, out, out_sem).wait()


def pack(ranges, tails, seg, k, v):
    batch, piece, head = k.shape
    return pl.pallas_call(
        functools.partial(pack_kernel, ranges, tails),
        in_specs=[pl.BlockSpec(memory_space=pltpu.VMEM)] + [pl.BlockSpec(memory_space=pl.ANY)] * 2,
        out_specs=[pl.BlockSpec(memory_space=pl.ANY)] * len(ranges),
        out_shape=[
            jax.ShapeDtypeStruct(((b - a) * 2 * piece + (batch if tail else 0), head), jnp.bfloat16)
            for (a, b), tail in zip(ranges, tails)
        ],
        scratch_shapes=[
            pltpu.VMEM(k.shape, jnp.bfloat16),
            pltpu.VMEM(k.shape, jnp.bfloat16),
            pltpu.VMEM((batch, head), jnp.bfloat16),
            pltpu.SemaphoreType.DMA((2,)),
            pltpu.SemaphoreType.DMA,
        ],
        cost_estimate=pl.CostEstimate(flops=1 << 20, bytes_accessed=4 * k.size, transcendentals=0),
    )(seg, k, v)


def attend_kernel(first, last, base, size, s_hbm, cut_ref, q_ref, k_ref, v_ref, near_ref, fara_ref, farb_ref, *rest):
    if not first:
        _, lse_in, q_in, kv_in, *rest = rest
    o_ref, lse_ref, *rest = rest
    if not last:
        q_out, kv_out, *rest = rest
    s_ref, n_ref, q_buf, k_buf, v_buf, o_buf, s_sem, kv_sem, q_sem, o_sem, ahead_sem = rest
    depth, heads, piece, head = q_buf.shape
    batch = lse_ref.shape[1]
    groups = heads // GROUP
    width = GROUP * piece
    scale = head ** -0.5
    me = lax.axis_index("cp")
    odd = lax.rem(me, 2)
    scalars = pltpu.make_async_copy(s_hbm, s_ref, s_sem)
    scalars.start()

    def kv_loads(step):
        slot = lax.rem(step, depth)
        seq = base + step
        there = pl.ds(pl.multiple_of(jnp.where(odd == 1, 1, 3) * piece, piece), piece)
        out = []
        for half, (ref, buf) in enumerate(((k_ref, k_buf), (v_ref, v_buf))):
            rows = pl.ds(pl.multiple_of((2 * seq + half) * piece, piece), piece)
            out.append(pltpu.make_async_copy(ref.at[seq], buf.at[slot, pl.ds(0, piece)], kv_sem.at[slot]))
            out.append(pltpu.make_async_copy(near_ref.at[rows], buf.at[slot, there], kv_sem.at[slot]))
        return out

    def aheads():
        at = base + size
        out = [pltpu.make_async_copy(q_ref.at[at], q_out, ahead_sem)]
        for half, ref in enumerate((k_ref, v_ref)):
            near_rows = pl.ds((2 * at + half) * piece, piece)
            out.append(pltpu.make_async_copy(ref.at[at], kv_out.at[2 * half], ahead_sem))
            out.append(pltpu.make_async_copy(near_ref.at[near_rows], kv_out.at[2 * half + 1], ahead_sem))
        return out

    def part(g):
        return pl.ds(g * GROUP, GROUP)

    def q_load(step, g):
        slot = lax.rem(step, depth)
        return pltpu.make_async_copy(q_ref.at[base + step, part(g)], q_buf.at[slot, part(g)], q_sem.at[slot, g])

    def o_store(step, g):
        slot = lax.rem(step, 2)
        return pltpu.make_async_copy(o_buf.at[slot, part(g)], o_ref.at[base + step, part(g)], o_sem.at[slot, g])

    def load(step):
        for copy in kv_loads(step):
            copy.start()
        for g in range(groups):
            q_load(step, g).start()

    def place(step):
        slot = lax.rem(step, depth)
        for ref, block in ((fara_ref, 2), (farb_ref, jnp.where(odd == 1, 3, 1))):
            there = pl.ds(pl.multiple_of(block * piece, piece), piece)
            for half, buf in enumerate((k_buf, v_buf)):
                buf[slot, there] = ref[pl.ds(pl.multiple_of((2 * step + half) * piece, piece), piece)]

    def run(count, step, cut):
        seq = base + step
        slot, out = lax.rem(step, depth), lax.rem(step, 2)
        keys = count * piece
        lane = lax.broadcasted_iota(jnp.int32, (piece, piece), 1)
        row = lax.broadcasted_iota(jnp.int32, (piece, piece), 0)
        low = jnp.maximum(jnp.where(row >= cut, cut, -keys), -me * piece)
        caps = [
            jnp.where((lane - n * piece <= row) & (lane - n * piece >= low), jnp.inf, -jnp.inf) for n in range(count)
        ]
        cap = jnp.concatenate([jnp.concatenate(caps, axis=1)] * GROUP, axis=0)
        logs = jnp.zeros((piece, piece), jnp.float32)

        def scores(g):
            q = q_buf[slot, g * GROUP:(g + 1) * GROUP].reshape(width, head)
            s = lax.dot_general(q, k_buf[slot, :keys], (((1,), (1,)), ((), ())), preferred_element_type=jnp.float32)
            s = jnp.minimum(s, cap)
            return s, jnp.max(s, axis=1, keepdims=True)

        def weigh(s, m):
            p = jnp.exp2((s - m) * (scale * LOG2E))
            return p.astype(jnp.bfloat16), m, jnp.sum(p, axis=1, keepdims=True)

        def finish(g, logs, p, m, l):
            o = jnp.dot(p, v_buf[slot, :keys], preferred_element_type=jnp.float32) * (1.0 / l)
            o_buf[out, g * GROUP:(g + 1) * GROUP] = o.astype(jnp.bfloat16).reshape(GROUP, piece, head)
            o_store(step, g).start()
            e = m * scale + jnp.log(l)
            for j in range(GROUP):
                logs = jnp.where(lane == g * GROUP + j, e[j * piece:(j + 1) * piece], logs)
            return logs

        now, before = scores(0), None
        for g in range(groups):
            later = scores(g + 1) if g + 1 < groups else None
            if before is not None:
                logs = finish(g - 1, logs, *before)
            before, now = weigh(*now), later
        logs = finish(groups - 1, logs, *before)
        lse_ref[:, pl.ds(seq, 1), :] = logs.T[:heads][:, None, :]

    n_ref[0] = jnp.where(me >= 2, 4, 2)
    if first:
        load(0)
    else:
        q_buf[0] = q_in[...]
        there = pl.ds(pl.multiple_of(jnp.where(odd == 1, 1, 3) * piece, piece), piece)
        for half, buf in enumerate((k_buf, v_buf)):
            buf[0, :piece] = kv_in[2 * half]
            buf[0, there] = kv_in[2 * half + 1]
        lse_ref[...] = lse_in[...]

    @pl.loop(0, size)
    def _(step):
        @pl.when((step > 0) | first)
        def _():
            for copy in kv_loads(step):
                copy.wait()
            for g in range(groups):
                q_load(step, g).wait()

        @pl.when((step == 0) & (size > 1))
        def _():
            load(1)

        @pl.when(step + 2 < size)
        def _():
            load(step + 2)

        if not last:
            @pl.when(step == max(size - 2, 0))
            def _():
                for copy in aheads():
                    copy.start()

        @pl.when(step >= 2)
        def _():
            for g in range(groups):
                o_store(step - 2, g).wait()

        place(step)
        need = n_ref[0]
        for count in (2, 3, 4):
            @pl.when((need == count) | (count == 2 and need == 1))
            def _():
                run(count, step, cut_ref[pl.ds(base + step, 1), :])

        @pl.when(step == 0)
        def _():
            scalars.wait()

        n_ref[0] = s_ref[jnp.minimum(base + step + 1, batch - 1)]

    if not last:
        for copy in aheads():
            copy.wait()
    for step in range(max(size - 2, 0), size):
        for g in range(groups):
            o_store(step, g).wait()


def attend(n, needs, cuts, q, k, v, near, fara, farb, prev):
    batch, heads, piece, head = q.shape
    base, size = BOUNDS[n], CHUNKS[n]
    first, last = prev is None, n == len(CHUNKS) - 1
    hbm = pl.BlockSpec(memory_space=pltpu.HBM)
    vmem = pl.BlockSpec(memory_space=pltpu.VMEM)
    in_specs = [hbm, vmem] + [hbm] * 4 + [vmem] * 2
    needs, q, k, v, near = (pltpu.with_memory_space_constraint(x, pltpu.HBM) for x in (needs, q, k, v, near))
    args = [needs, cuts, q, k, v, near, fara, farb]
    aliases = {}
    if not first:
        in_specs += [hbm, vmem, vmem, vmem]
        args += list(prev)
        aliases = {8: 0}
    out_shape = [
        jax.ShapeDtypeStruct(q.shape, jnp.bfloat16),
        jax.ShapeDtypeStruct((heads, batch, piece), jnp.float32),
    ]
    if not last:
        out_shape += [
            jax.ShapeDtypeStruct(q.shape[1:], jnp.bfloat16),
            jax.ShapeDtypeStruct((4, piece, head), jnp.bfloat16),
        ]
    return pl.pallas_call(
        functools.partial(attend_kernel, first, last, base, size),
        in_specs=in_specs,
        out_specs=[hbm] + [vmem] * (len(out_shape) - 1),
        scratch_shapes=[
            pltpu.SMEM(needs.shape, jnp.int32),
            pltpu.SMEM((1,), jnp.int32),
            pltpu.VMEM((DEPTH, heads, piece, head), jnp.bfloat16),
            pltpu.VMEM((DEPTH, 4 * piece, head), jnp.bfloat16),
            pltpu.VMEM((DEPTH, 4 * piece, head), jnp.bfloat16),
            pltpu.VMEM((2, heads, piece, head), jnp.bfloat16),
            pltpu.SemaphoreType.DMA,
            pltpu.SemaphoreType.DMA((DEPTH,)),
            pltpu.SemaphoreType.DMA((DEPTH, heads // GROUP)),
            pltpu.SemaphoreType.DMA((2, heads // GROUP)),
            pltpu.SemaphoreType.DMA,
        ],
        out_shape=out_shape,
        input_output_aliases=aliases,
        compiler_params=pltpu.CompilerParams(vmem_limit_bytes=32 << 20),
        cost_estimate=pl.CostEstimate(
            flops=size * heads * piece * 4 * piece * head * 4,
            bytes_accessed=size * heads * piece * head * 4,
            transcendentals=0,
        ),
    )(*args)


def shift(x, pairs):
    return lax.ppermute(x, "cp", pairs)


def solution(mesh):
    def local(q_loc, k_loc, v_loc, seg_loc):
        batch, piece, _, _ = q_loc.shape
        me = lax.axis_index("cp")
        q = jnp.transpose(q_loc, (0, 2, 1, 3))
        ranges = tuple(zip(BOUNDS[:-1], BOUNDS[1:]))
        sends = pack(ranges[:1], (True,), seg_loc, k_loc, v_loc)
        *more, whole = pack(ranges[1:] + ((0, batch),), (False,) * len(ranges[1:]) + (True,), seg_loc, k_loc, v_loc)
        sends = list(sends) + more
        fara = [shift(x, ACROSS) for x in sends]
        near = shift(whole, BESIDE)
        farb = [shift(x, SWAP) for x in fara]

        def zeros(packed, there):
            return jnp.where(there, packed[-batch:, 0].astype(jnp.int32), 0)

        odd, upper = me % 2 == 1, me >= 2
        cuts = zeros(whole, True) + zeros(near, odd) + zeros(fara[0], upper) + zeros(farb[0], upper)
        need = jnp.where(cuts <= me * piece, me - cuts // piece, me) + 1
        table = jnp.broadcast_to((cuts - me * piece)[:, None], (batch, piece))
        state = None
        for n in range(len(CHUNKS)):
            state = attend(n, need.astype(jnp.int32), table, q, k_loc, v_loc, near, fara[n], farb[n], state)
        out, lse = state[:2]
        return jnp.transpose(out, (0, 2, 1, 3)), jnp.transpose(lse, (1, 2, 0))

    return jax.shard_map(
        local,
        mesh=mesh,
        in_specs=(P("dp", "cp", None, None), P("dp", "cp", None), P("dp", "cp", None), P("dp", "cp")),
        out_specs=(P("dp", "cp", None, None), P("dp", "cp", None)),
        check_vma=False,
    )
```

```python
import functools

import jax
import jax.numpy as jnp
from jax import lax
from jax.experimental import pallas as pl
from jax.experimental.pallas import tpu as pltpu
from jax.sharding import PartitionSpec as P


CHUNKS = (6, 6, 5, 5, 5, 5)
BOUNDS = tuple(sum(CHUNKS[:n]) for n in range(len(CHUNKS) + 1))
GROUP = 2
DEPTH = 3
LOG2E = 1.4426950408889634

ACROSS = [(0, 2), (1, 3)]
BESIDE = [(0, 1), (2, 3)]
SWAP = [(2, 3), (3, 2)]


def pack_kernel(ranges, tails, seg_ref, k_ref, v_ref, *rest):
    outs, (seg_scr, seg_sem, sem) = rest[:-3], rest[-3:]
    batch, piece, head = k_ref.shape
    segments = pltpu.make_async_copy(seg_ref, seg_scr, seg_sem)
    segments.start()

    def copies(i, out, at):
        for half, ref in enumerate((k_ref, v_ref)):
            rows = pl.ds(pl.multiple_of((2 * i + half) * piece, piece), piece)
            yield pltpu.make_async_copy(ref.at[at + i], out.at[rows], sem)

    for out, (a, b) in zip(outs, ranges):
        @pl.loop(0, b - a)
        def _(i):
            for copy in copies(i, out, a):
                copy.start()
    segments.wait()
    here = jnp.sum((seg_scr[...] == 0).astype(jnp.float32), axis=1, keepdims=True)
    rows = jnp.broadcast_to(here, (batch, head)).astype(jnp.bfloat16)
    for out, (a, b), tail in zip(outs, ranges, tails):
        if tail:
            out[(b - a) * 2 * piece:] = rows
    for out, (a, b) in zip(outs, ranges):
        @pl.loop(0, b - a)
        def _(i):
            for copy in copies(i, out, a):
                copy.wait()


def pack(ranges, tails, seg, k, v):
    batch, piece, head = k.shape
    vmem, hbm = pl.BlockSpec(memory_space=pltpu.VMEM), pl.BlockSpec(memory_space=pltpu.HBM)
    seg, k, v = (pltpu.with_memory_space_constraint(x, pltpu.HBM) for x in (seg, k, v))
    return pl.pallas_call(
        functools.partial(pack_kernel, ranges, tails),
        in_specs=[hbm] * 3,
        out_specs=[vmem] * len(ranges),
        out_shape=[
            jax.ShapeDtypeStruct(((b - a) * 2 * piece + (batch if tail else 0), head), jnp.bfloat16)
            for (a, b), tail in zip(ranges, tails)
        ],
        scratch_shapes=[pltpu.VMEM(seg.shape, jnp.int32), pltpu.SemaphoreType.DMA, pltpu.SemaphoreType.DMA],
        compiler_params=pltpu.CompilerParams(vmem_limit_bytes=16 << 20),
        cost_estimate=pl.CostEstimate(flops=1 << 20, bytes_accessed=4 * k.size, transcendentals=0),
    )(seg, k, v)


def attend_kernel(first, last, base, size, s_hbm, cut_ref, q_ref, k_ref, v_ref, near_ref, fara_ref, farb_ref, *rest):
    if not first:
        _, lse_in, q_in, kv_in, *rest = rest
    o_ref, lse_ref, *rest = rest
    if not last:
        q_out, kv_out, *rest = rest
    s_ref, n_ref, q_buf, k_buf, v_buf, o_buf, s_sem, kv_sem, q_sem, o_sem, ahead_sem = rest
    depth, heads, piece, head = q_buf.shape
    batch = lse_ref.shape[1]
    groups = heads // GROUP
    width = GROUP * piece
    scale = head ** -0.5
    me = lax.axis_index("cp")
    odd = lax.rem(me, 2)
    scalars = pltpu.make_async_copy(s_hbm, s_ref, s_sem)
    scalars.start()

    def kv_loads(step):
        slot = lax.rem(step, depth)
        seq = base + step
        there = pl.ds(pl.multiple_of(jnp.where(odd == 1, 1, 3) * piece, piece), piece)
        out = []
        for half, (ref, buf) in enumerate(((k_ref, k_buf), (v_ref, v_buf))):
            rows = pl.ds(pl.multiple_of((2 * seq + half) * piece, piece), piece)
            out.append(pltpu.make_async_copy(ref.at[seq], buf.at[slot, pl.ds(0, piece)], kv_sem.at[slot]))
            out.append(pltpu.make_async_copy(near_ref.at[rows], buf.at[slot, there], kv_sem.at[slot]))
        return out

    def aheads():
        at = base + size
        out = [pltpu.make_async_copy(q_ref.at[at], q_out, ahead_sem)]
        for half, ref in enumerate((k_ref, v_ref)):
            near_rows = pl.ds((2 * at + half) * piece, piece)
            out.append(pltpu.make_async_copy(ref.at[at], kv_out.at[2 * half], ahead_sem))
            out.append(pltpu.make_async_copy(near_ref.at[near_rows], kv_out.at[2 * half + 1], ahead_sem))
        return out

    def part(g):
        return pl.ds(g * GROUP, GROUP)

    def q_load(step, g):
        slot = lax.rem(step, depth)
        return pltpu.make_async_copy(q_ref.at[base + step, part(g)], q_buf.at[slot, part(g)], q_sem.at[slot, g])

    def o_store(step, g):
        slot = lax.rem(step, 2)
        return pltpu.make_async_copy(o_buf.at[slot, part(g)], o_ref.at[base + step, part(g)], o_sem.at[slot, g])

    def load(step):
        for copy in kv_loads(step):
            copy.start()
        for g in range(groups):
            q_load(step, g).start()

    def place(step):
        slot = lax.rem(step, depth)
        for ref, block in ((fara_ref, 2), (farb_ref, jnp.where(odd == 1, 3, 1))):
            there = pl.ds(pl.multiple_of(block * piece, piece), piece)
            for half, buf in enumerate((k_buf, v_buf)):
                buf[slot, there] = ref[pl.ds(pl.multiple_of((2 * step + half) * piece, piece), piece)]

    def run(count, step, cut):
        seq = base + step
        slot, out = lax.rem(step, depth), lax.rem(step, 2)
        keys = count * piece
        lane = lax.broadcasted_iota(jnp.int32, (piece, piece), 1)
        row = lax.broadcasted_iota(jnp.int32, (piece, piece), 0)
        low = jnp.maximum(jnp.where(row >= cut, cut, -keys), -me * piece)
        caps = [
            jnp.where((lane - n * piece <= row) & (lane - n * piece >= low), jnp.inf, -jnp.inf) for n in range(count)
        ]
        cap = jnp.concatenate([jnp.concatenate(caps, axis=1)] * GROUP, axis=0)
        logs = jnp.zeros((piece, piece), jnp.float32)

        def scores(g):
            q = q_buf[slot, g * GROUP:(g + 1) * GROUP].reshape(width, head)
            s = lax.dot_general(q, k_buf[slot, :keys], (((1,), (1,)), ((), ())), preferred_element_type=jnp.float32)
            s = jnp.minimum(s, cap)
            return s, jnp.max(s, axis=1, keepdims=True)

        def weigh(s, m):
            p = jnp.exp2((s - m) * (scale * LOG2E))
            return p.astype(jnp.bfloat16), m, jnp.sum(p, axis=1, keepdims=True)

        def finish(g, logs, p, m, l):
            o = jnp.dot(p, v_buf[slot, :keys], preferred_element_type=jnp.float32) * (1.0 / l)
            o_buf[out, g * GROUP:(g + 1) * GROUP] = o.astype(jnp.bfloat16).reshape(GROUP, piece, head)
            o_store(step, g).start()
            e = m * scale + jnp.log(l)
            for j in range(GROUP):
                logs = jnp.where(lane == g * GROUP + j, e[j * piece:(j + 1) * piece], logs)
            return logs

        now, before = scores(0), None
        for g in range(groups):
            later = scores(g + 1) if g + 1 < groups else None
            if before is not None:
                logs = finish(g - 1, logs, *before)
            before, now = weigh(*now), later
        logs = finish(groups - 1, logs, *before)
        lse_ref[:, pl.ds(seq, 1), :] = logs.T[:heads][:, None, :]

    n_ref[0] = jnp.where(me >= 2, 4, 2)
    if first:
        load(0)
    else:
        q_buf[0] = q_in[...]
        there = pl.ds(pl.multiple_of(jnp.where(odd == 1, 1, 3) * piece, piece), piece)
        for half, buf in enumerate((k_buf, v_buf)):
            buf[0, :piece] = kv_in[2 * half]
            buf[0, there] = kv_in[2 * half + 1]
        lse_ref[...] = lse_in[...]

    @pl.loop(0, size)
    def _(step):
        @pl.when((step > 0) | first)
        def _():
            for copy in kv_loads(step):
                copy.wait()
            for g in range(groups):
                q_load(step, g).wait()

        @pl.when((step == 0) & (size > 1))
        def _():
            load(1)

        @pl.when(step + 2 < size)
        def _():
            load(step + 2)

        if not last:
            @pl.when(step == max(size - 2, 0))
            def _():
                for copy in aheads():
                    copy.start()

        @pl.when(step >= 2)
        def _():
            for g in range(groups):
                o_store(step - 2, g).wait()

        place(step)
        need = n_ref[0]
        for count in (2, 3, 4):
            @pl.when((need == count) | (count == 2 and need == 1))
            def _():
                run(count, step, cut_ref[pl.ds(base + step, 1), :])

        @pl.when(step == 0)
        def _():
            scalars.wait()

        n_ref[0] = s_ref[jnp.minimum(base + step + 1, batch - 1)]

    if not last:
        for copy in aheads():
            copy.wait()
    for step in range(max(size - 2, 0), size):
        for g in range(groups):
            o_store(step, g).wait()


def attend(n, needs, cuts, q, k, v, near, fara, farb, prev):
    batch, heads, piece, head = q.shape
    base, size = BOUNDS[n], CHUNKS[n]
    first, last = prev is None, n == len(CHUNKS) - 1
    hbm = pl.BlockSpec(memory_space=pltpu.HBM)
    vmem = pl.BlockSpec(memory_space=pltpu.VMEM)
    in_specs = [hbm, vmem] + [hbm] * 4 + [vmem] * 2
    needs, q, k, v, near = (pltpu.with_memory_space_constraint(x, pltpu.HBM) for x in (needs, q, k, v, near))
    args = [needs, cuts, q, k, v, near, fara, farb]
    aliases = {}
    if not first:
        in_specs += [hbm, vmem, vmem, vmem]
        args += list(prev)
        aliases = {8: 0}
    out_shape = [
        jax.ShapeDtypeStruct(q.shape, jnp.bfloat16),
        jax.ShapeDtypeStruct((heads, batch, piece), jnp.float32),
    ]
    if not last:
        out_shape += [
            jax.ShapeDtypeStruct(q.shape[1:], jnp.bfloat16),
            jax.ShapeDtypeStruct((4, piece, head), jnp.bfloat16),
        ]
    return pl.pallas_call(
        functools.partial(attend_kernel, first, last, base, size),
        in_specs=in_specs,
        out_specs=[hbm] + [vmem] * (len(out_shape) - 1),
        scratch_shapes=[
            pltpu.SMEM(needs.shape, jnp.int32),
            pltpu.SMEM((1,), jnp.int32),
            pltpu.VMEM((DEPTH, heads, piece, head), jnp.bfloat16),
            pltpu.VMEM((DEPTH, 4 * piece, head), jnp.bfloat16),
            pltpu.VMEM((DEPTH, 4 * piece, head), jnp.bfloat16),
            pltpu.VMEM((2, heads, piece, head), jnp.bfloat16),
            pltpu.SemaphoreType.DMA,
            pltpu.SemaphoreType.DMA((DEPTH,)),
            pltpu.SemaphoreType.DMA((DEPTH, heads // GROUP)),
            pltpu.SemaphoreType.DMA((2, heads // GROUP)),
            pltpu.SemaphoreType.DMA,
        ],
        out_shape=out_shape,
        input_output_aliases=aliases,
        compiler_params=pltpu.CompilerParams(vmem_limit_bytes=32 << 20),
        cost_estimate=pl.CostEstimate(
            flops=size * heads * piece * 4 * piece * head * 4,
            bytes_accessed=size * heads * piece * head * 4,
            transcendentals=0,
        ),
    )(*args)


def shift(x, pairs):
    return lax.ppermute(x, "cp", pairs)


def solution(mesh):
    def local(q_loc, k_loc, v_loc, seg_loc):
        batch, piece, _, _ = q_loc.shape
        me = lax.axis_index("cp")
        q = jnp.transpose(q_loc, (0, 2, 1, 3))
        ranges = tuple(zip(BOUNDS[:-1], BOUNDS[1:]))
        sends = pack(ranges[:1], (True,), seg_loc, k_loc, v_loc)
        *more, whole = pack(ranges[1:] + ((0, batch),), (False,) * len(ranges[1:]) + (True,), seg_loc, k_loc, v_loc)
        sends = list(sends) + more
        fara = [shift(x, ACROSS) for x in sends]
        near = shift(whole, BESIDE)
        farb = [shift(x, SWAP) for x in fara]

        def zeros(packed, there):
            return jnp.where(there, packed[-batch:, 0].astype(jnp.int32), 0)

        odd, upper = me % 2 == 1, me >= 2
        cuts = zeros(whole, True) + zeros(near, odd) + zeros(fara[0], upper) + zeros(farb[0], upper)
        need = jnp.where(cuts <= me * piece, me - cuts // piece, me) + 1
        table = jnp.broadcast_to((cuts - me * piece)[:, None], (batch, piece))
        state = None
        for n in range(len(CHUNKS)):
            state = attend(n, need.astype(jnp.int32), table, q, k_loc, v_loc, near, fara[n], farb[n], state)
        out, lse = state[:2]
        return jnp.transpose(out, (0, 2, 1, 3)), jnp.transpose(lse, (1, 2, 0))

    return jax.shard_map(
        local,
        mesh=mesh,
        in_specs=(P("dp", "cp", None, None), P("dp", "cp", None), P("dp", "cp", None), P("dp", "cp")),
        out_specs=(P("dp", "cp", None, None), P("dp", "cp", None)),
        check_vma=False,
    )
```

```python
import functools

import jax
import jax.numpy as jnp
from jax import lax
from jax.experimental import pallas as pl
from jax.experimental.pallas import tpu as pltpu
from jax.sharding import PartitionSpec as P


CHUNKS = (6, 6, 6, 6, 5, 3)
BOUNDS = tuple(sum(CHUNKS[:n]) for n in range(len(CHUNKS) + 1))
GROUP = 2
DEPTH = 3
LOG2E = 1.4426950408889634

ACROSS = [(0, 2), (1, 3)]
BESIDE = [(0, 1), (2, 3)]


def pack_kernel(ranges, tails, seg_ref, k_ref, v_ref, *rest):
    outs, (seg_scr, seg_sem, sem) = rest[:-3], rest[-3:]
    batch, piece, head = k_ref.shape
    segments = pltpu.make_async_copy(seg_ref, seg_scr, seg_sem)
    segments.start()

    def copies(i, out, at):
        for half, ref in enumerate((k_ref, v_ref)):
            rows = pl.ds(pl.multiple_of((2 * i + half) * piece, piece), piece)
            yield pltpu.make_async_copy(ref.at[at + i], out.at[rows], sem)

    for out, (a, b) in zip(outs, ranges):
        @pl.loop(0, b - a)
        def _(i):
            for copy in copies(i, out, a):
                copy.start()
    segments.wait()
    here = jnp.sum((seg_scr[...] == 0).astype(jnp.float32), axis=1, keepdims=True)
    rows = jnp.broadcast_to(here, (batch, head)).astype(jnp.bfloat16)
    for out, (a, b), tail in zip(outs, ranges, tails):
        if tail:
            out[(b - a) * 2 * piece:] = rows
    for out, (a, b) in zip(outs, ranges):
        @pl.loop(0, b - a)
        def _(i):
            for copy in copies(i, out, a):
                copy.wait()


def pack(ranges, tails, seg, k, v):
    batch, piece, head = k.shape
    vmem, hbm = pl.BlockSpec(memory_space=pltpu.VMEM), pl.BlockSpec(memory_space=pltpu.HBM)
    seg, k, v = (pltpu.with_memory_space_constraint(x, pltpu.HBM) for x in (seg, k, v))
    return pl.pallas_call(
        functools.partial(pack_kernel, ranges, tails),
        in_specs=[hbm] * 3,
        out_specs=[vmem] * len(ranges),
        out_shape=[
            jax.ShapeDtypeStruct(((b - a) * 2 * piece + (batch if tail else 0), head), jnp.bfloat16)
            for (a, b), tail in zip(ranges, tails)
        ],
        scratch_shapes=[pltpu.VMEM(seg.shape, jnp.int32), pltpu.SemaphoreType.DMA, pltpu.SemaphoreType.DMA],
        compiler_params=pltpu.CompilerParams(vmem_limit_bytes=16 << 20),
        cost_estimate=pl.CostEstimate(flops=1 << 20, bytes_accessed=4 * k.size, transcendentals=0),
    )(seg, k, v)


def attend_kernel(first, last, base, size, s_hbm, cut_ref, q_ref, k_ref, v_ref, near_ref, fara_ref, farb_ref, *rest):
    if not first:
        _, lse_in, q_in, kv_in, *rest = rest
    o_ref, lse_ref, *rest = rest
    if not last:
        q_out, kv_out, *rest = rest
    s_ref, n_ref, q_buf, k_buf, v_buf, o_buf, s_sem, kv_sem, q_sem, o_sem, ahead_sem = rest
    depth, heads, piece, head = q_buf.shape
    batch = lse_ref.shape[1]
    groups = heads // GROUP
    width = GROUP * piece
    scale = head ** -0.5
    me = lax.axis_index("cp")
    odd = lax.rem(me, 2)
    scalars = pltpu.make_async_copy(s_hbm, s_ref, s_sem)
    scalars.start()

    def kv_loads(step):
        slot = lax.rem(step, depth)
        seq = base + step
        there = pl.ds(pl.multiple_of(jnp.where(odd == 1, 1, 3) * piece, piece), piece)
        out = []
        for half, (ref, buf) in enumerate(((k_ref, k_buf), (v_ref, v_buf))):
            rows = pl.ds(pl.multiple_of((2 * seq + half) * piece, piece), piece)
            out.append(pltpu.make_async_copy(ref.at[seq], buf.at[slot, pl.ds(0, piece)], kv_sem.at[slot]))
            out.append(pltpu.make_async_copy(near_ref.at[rows], buf.at[slot, there], kv_sem.at[slot]))
        return out

    def aheads():
        at = base + size
        out = [pltpu.make_async_copy(q_ref.at[at], q_out, ahead_sem)]
        for half, ref in enumerate((k_ref, v_ref)):
            near_rows = pl.ds((2 * at + half) * piece, piece)
            out.append(pltpu.make_async_copy(ref.at[at], kv_out.at[2 * half], ahead_sem))
            out.append(pltpu.make_async_copy(near_ref.at[near_rows], kv_out.at[2 * half + 1], ahead_sem))
        return out

    def part(g):
        return pl.ds(g * GROUP, GROUP)

    def q_load(step, g):
        slot = lax.rem(step, depth)
        return pltpu.make_async_copy(q_ref.at[base + step, part(g)], q_buf.at[slot, part(g)], q_sem.at[slot, g])

    def o_store(step, g):
        slot = lax.rem(step, 2)
        return pltpu.make_async_copy(o_buf.at[slot, part(g)], o_ref.at[base + step, part(g)], o_sem.at[slot, g])

    def load(step):
        for copy in kv_loads(step):
            copy.start()
        for g in range(groups):
            q_load(step, g).start()

    def place(step):
        slot = lax.rem(step, depth)
        for ref, block in ((fara_ref, 2), (farb_ref, jnp.where(odd == 1, 3, 1))):
            there = pl.ds(pl.multiple_of(block * piece, piece), piece)
            for half, buf in enumerate((k_buf, v_buf)):
                buf[slot, there] = ref[pl.ds(pl.multiple_of((2 * step + half) * piece, piece), piece)]

    def run(count, step, cut):
        seq = base + step
        slot, out = lax.rem(step, depth), lax.rem(step, 2)
        keys = count * piece
        lane = lax.broadcasted_iota(jnp.int32, (piece, piece), 1)
        row = lax.broadcasted_iota(jnp.int32, (piece, piece), 0)
        low = jnp.maximum(jnp.where(row >= cut, cut, -keys), -me * piece)
        caps = [
            jnp.where((lane - n * piece <= row) & (lane - n * piece >= low), jnp.inf, -jnp.inf) for n in range(count)
        ]
        cap = jnp.concatenate([jnp.concatenate(caps, axis=1)] * GROUP, axis=0)
        logs = jnp.zeros((piece, piece), jnp.float32)

        def scores(g):
            q = q_buf[slot, g * GROUP:(g + 1) * GROUP].reshape(width, head)
            s = lax.dot_general(q, k_buf[slot, :keys], (((1,), (1,)), ((), ())), preferred_element_type=jnp.float32)
            s = jnp.minimum(s, cap)
            return s, jnp.max(s, axis=1, keepdims=True)

        def weigh(s, m):
            p = jnp.exp2((s - m) * (scale * LOG2E))
            return p.astype(jnp.bfloat16), m, jnp.sum(p, axis=1, keepdims=True)

        def finish(g, logs, p, m, l):
            o = jnp.dot(p, v_buf[slot, :keys], preferred_element_type=jnp.float32) * (1.0 / l)
            o_buf[out, g * GROUP:(g + 1) * GROUP] = o.astype(jnp.bfloat16).reshape(GROUP, piece, head)
            o_store(step, g).start()
            e = m * scale + jnp.log(l)
            for j in range(GROUP):
                logs = jnp.where(lane == g * GROUP + j, e[j * piece:(j + 1) * piece], logs)
            return logs

        now, before = scores(0), None
        for g in range(groups):
            later = scores(g + 1) if g + 1 < groups else None
            if before is not None:
                logs = finish(g - 1, logs, *before)
            before, now = weigh(*now), later
        logs = finish(groups - 1, logs, *before)
        lse_ref[:, pl.ds(seq, 1), :] = logs.T[:heads][:, None, :]

    n_ref[0] = jnp.where(me >= 2, 4, 2)
    if first:
        load(0)
    else:
        q_buf[0] = q_in[...]
        there = pl.ds(pl.multiple_of(jnp.where(odd == 1, 1, 3) * piece, piece), piece)
        for half, buf in enumerate((k_buf, v_buf)):
            buf[0, :piece] = kv_in[2 * half]
            buf[0, there] = kv_in[2 * half + 1]
        lse_ref[...] = lse_in[...]

    @pl.loop(0, size)
    def _(step):
        @pl.when((step > 0) | first)
        def _():
            for copy in kv_loads(step):
                copy.wait()
            for g in range(groups):
                q_load(step, g).wait()

        @pl.when((step == 0) & (size > 1))
        def _():
            load(1)

        @pl.when(step + 2 < size)
        def _():
            load(step + 2)

        if not last:
            @pl.when(step == max(size - 2, 0))
            def _():
                for copy in aheads():
                    copy.start()

        @pl.when(step >= 2)
        def _():
            for g in range(groups):
                o_store(step - 2, g).wait()

        place(step)
        need = n_ref[0]
        for count in (2, 3, 4):
            @pl.when((need == count) | (count == 2 and need == 1))
            def _():
                run(count, step, cut_ref[pl.ds(base + step, 1), :])

        @pl.when(step == 0)
        def _():
            scalars.wait()

        n_ref[0] = s_ref[jnp.minimum(base + step + 1, batch - 1)]

    if not last:
        for copy in aheads():
            copy.wait()
    for step in range(max(size - 2, 0), size):
        for g in range(groups):
            o_store(step, g).wait()


def attend(n, needs, cuts, q, k, v, near, fara, farb, prev):
    batch, heads, piece, head = q.shape
    base, size = BOUNDS[n], CHUNKS[n]
    first, last = prev is None, n == len(CHUNKS) - 1
    hbm = pl.BlockSpec(memory_space=pltpu.HBM)
    vmem = pl.BlockSpec(memory_space=pltpu.VMEM)
    in_specs = [hbm, vmem] + [hbm] * 4 + [vmem] * 2
    needs, q, k, v, near = (pltpu.with_memory_space_constraint(x, pltpu.HBM) for x in (needs, q, k, v, near))
    args = [needs, cuts, q, k, v, near, fara, farb]
    aliases = {}
    if not first:
        in_specs += [hbm, vmem, vmem, vmem]
        args += list(prev)
        aliases = {8: 0}
    out_shape = [
        jax.ShapeDtypeStruct(q.shape, jnp.bfloat16),
        jax.ShapeDtypeStruct((heads, batch, piece), jnp.float32),
    ]
    if not last:
        out_shape += [
            jax.ShapeDtypeStruct(q.shape[1:], jnp.bfloat16),
            jax.ShapeDtypeStruct((4, piece, head), jnp.bfloat16),
        ]
    return pl.pallas_call(
        functools.partial(attend_kernel, first, last, base, size),
        in_specs=in_specs,
        out_specs=[hbm] + [vmem] * (len(out_shape) - 1),
        scratch_shapes=[
            pltpu.SMEM(needs.shape, jnp.int32),
            pltpu.SMEM((1,), jnp.int32),
            pltpu.VMEM((DEPTH, heads, piece, head), jnp.bfloat16),
            pltpu.VMEM((DEPTH, 4 * piece, head), jnp.bfloat16),
            pltpu.VMEM((DEPTH, 4 * piece, head), jnp.bfloat16),
            pltpu.VMEM((2, heads, piece, head), jnp.bfloat16),
            pltpu.SemaphoreType.DMA,
            pltpu.SemaphoreType.DMA((DEPTH,)),
            pltpu.SemaphoreType.DMA((DEPTH, heads // GROUP)),
            pltpu.SemaphoreType.DMA((2, heads // GROUP)),
            pltpu.SemaphoreType.DMA,
        ],
        out_shape=out_shape,
        input_output_aliases=aliases,
        compiler_params=pltpu.CompilerParams(vmem_limit_bytes=32 << 20),
        cost_estimate=pl.CostEstimate(
            flops=size * heads * piece * 4 * piece * head * 4,
            bytes_accessed=size * heads * piece * head * 4,
            transcendentals=0,
        ),
    )(*args)


def swap_kernel(mine_ref, other_ref, send_sem, recv_sem):
    me = lax.axis_index("cp")
    partner = {"cp": me + 1 - 2 * lax.rem(me, 2)}
    barrier = pltpu.get_barrier_semaphore()
    pl.semaphore_signal(barrier, inc=1, device_id=partner, device_id_type=pl.DeviceIdType.MESH)
    pl.semaphore_wait(barrier, 1)
    copy = pltpu.make_async_remote_copy(
        src_ref=mine_ref,
        dst_ref=other_ref,
        send_sem=send_sem,
        recv_sem=recv_sem,
        device_id=partner,
        device_id_type=pl.DeviceIdType.MESH,
    )
    copy.start()
    copy.wait()


def swap(n, x):
    vmem = pl.BlockSpec(memory_space=pltpu.VMEM)
    return pl.pallas_call(
        swap_kernel,
        in_specs=[vmem],
        out_specs=vmem,
        out_shape=jax.ShapeDtypeStruct(x.shape, x.dtype),
        scratch_shapes=[pltpu.SemaphoreType.DMA, pltpu.SemaphoreType.DMA],
        compiler_params=pltpu.CompilerParams(
            collective_id=n, has_side_effects=True, vmem_limit_bytes=16 << 20
        ),
        cost_estimate=pl.CostEstimate(flops=1 << 20, bytes_accessed=4 * x.size, transcendentals=0),
    )(x)


def shift(x, pairs):
    return lax.ppermute(x, "cp", pairs)


def solution(mesh):
    def local(q_loc, k_loc, v_loc, seg_loc):
        batch, piece, _, _ = q_loc.shape
        me = lax.axis_index("cp")
        q = jnp.transpose(q_loc, (0, 2, 1, 3))
        ranges = tuple(zip(BOUNDS[:-1], BOUNDS[1:]))
        sends = pack(ranges[:1], (True,), seg_loc, k_loc, v_loc)
        *more, whole = pack(ranges[1:] + ((0, batch),), (False,) * len(ranges[1:]) + (True,), seg_loc, k_loc, v_loc)
        sends = list(sends) + more
        fara = [shift(x, ACROSS) for x in sends]
        near = shift(whole, BESIDE)
        farb = [swap(n, x) for n, x in enumerate(fara)]

        def zeros(packed, there):
            return jnp.where(there, packed[-batch:, 0].astype(jnp.int32), 0)

        odd, upper = me % 2 == 1, me >= 2
        cuts = zeros(whole, True) + zeros(near, odd) + zeros(fara[0], upper) + zeros(farb[0], upper)
        need = jnp.where(cuts <= me * piece, me - cuts // piece, me) + 1
        table = jnp.broadcast_to((cuts - me * piece)[:, None], (batch, piece))
        state = None
        for n in range(len(CHUNKS)):
            state = attend(n, need.astype(jnp.int32), table, q, k_loc, v_loc, near, fara[n], farb[n], state)
        out, lse = state[:2]
        return jnp.transpose(out, (0, 2, 1, 3)), jnp.transpose(lse, (1, 2, 0))

    return jax.shard_map(
        local,
        mesh=mesh,
        in_specs=(P("dp", "cp", None, None), P("dp", "cp", None), P("dp", "cp", None), P("dp", "cp")),
        out_specs=(P("dp", "cp", None, None), P("dp", "cp", None)),
        check_vma=False,
    )
```

```python
import functools

import jax
import jax.numpy as jnp
from jax import lax
from jax.experimental import pallas as pl
from jax.experimental.pallas import tpu as pltpu
from jax.sharding import PartitionSpec as P


CHUNKS = (5, 6, 6, 5, 4, 3, 3)
BOUNDS = tuple(sum(CHUNKS[:n]) for n in range(len(CHUNKS) + 1))
GROUP = 2
DEPTH = 3
LOG2E = 1.4426950408889634

ACROSS = [(0, 2), (1, 3)]
BESIDE = [(0, 1), (2, 3)]


def pack_kernel(ranges, tails, seg_ref, k_ref, v_ref, *rest):
    outs, (seg_scr, seg_sem, sem) = rest[:-3], rest[-3:]
    batch, piece, head = k_ref.shape
    segments = pltpu.make_async_copy(seg_ref, seg_scr, seg_sem)
    segments.start()

    def copies(i, out, at):
        for half, ref in enumerate((k_ref, v_ref)):
            rows = pl.ds(pl.multiple_of((2 * i + half) * piece, piece), piece)
            yield pltpu.make_async_copy(ref.at[at + i], out.at[rows], sem)

    for out, (a, b) in zip(outs, ranges):
        @pl.loop(0, b - a)
        def _(i):
            for copy in copies(i, out, a):
                copy.start()
    segments.wait()
    here = jnp.sum((seg_scr[...] == 0).astype(jnp.float32), axis=1, keepdims=True)
    rows = jnp.broadcast_to(here, (batch, head)).astype(jnp.bfloat16)
    for out, (a, b), tail in zip(outs, ranges, tails):
        if tail:
            out[(b - a) * 2 * piece:] = rows
    for out, (a, b) in zip(outs, ranges):
        @pl.loop(0, b - a)
        def _(i):
            for copy in copies(i, out, a):
                copy.wait()


def pack(ranges, tails, seg, k, v):
    batch, piece, head = k.shape
    vmem, hbm = pl.BlockSpec(memory_space=pltpu.VMEM), pl.BlockSpec(memory_space=pltpu.HBM)
    seg, k, v = (pltpu.with_memory_space_constraint(x, pltpu.HBM) for x in (seg, k, v))
    return pl.pallas_call(
        functools.partial(pack_kernel, ranges, tails),
        in_specs=[hbm] * 3,
        out_specs=[vmem] * len(ranges),
        out_shape=[
            jax.ShapeDtypeStruct(((b - a) * 2 * piece + (batch if tail else 0), head), jnp.bfloat16)
            for (a, b), tail in zip(ranges, tails)
        ],
        scratch_shapes=[pltpu.VMEM(seg.shape, jnp.int32), pltpu.SemaphoreType.DMA, pltpu.SemaphoreType.DMA],
        compiler_params=pltpu.CompilerParams(vmem_limit_bytes=16 << 20),
        cost_estimate=pl.CostEstimate(flops=1 << 20, bytes_accessed=4 * k.size, transcendentals=0),
    )(seg, k, v)


def attend_kernel(first, last, base, size, s_hbm, cut_ref, q_ref, k_ref, v_ref, near_ref, fara_ref, farb_ref, *rest):
    if not first:
        _, lse_in, q_in, kv_in, *rest = rest
    o_ref, lse_ref, *rest = rest
    if last:
        lse_out, (lse_ref, lse_sem, *rest) = lse_ref, rest
    else:
        q_out, kv_out, *rest = rest
    s_ref, n_ref, q_buf, k_buf, v_buf, o_buf, s_sem, kv_sem, q_sem, o_sem, ahead_sem = rest
    depth, heads, piece, head = q_buf.shape
    batch = lse_ref.shape[1]
    groups = heads // GROUP
    width = GROUP * piece
    scale = head ** -0.5
    me = lax.axis_index("cp")
    odd = lax.rem(me, 2)
    scalars = pltpu.make_async_copy(s_hbm, s_ref, s_sem)
    scalars.start()

    def kv_loads(step):
        slot = lax.rem(step, depth)
        seq = base + step
        there = pl.ds(pl.multiple_of(jnp.where(odd == 1, 1, 3) * piece, piece), piece)
        out = []
        for half, (ref, buf) in enumerate(((k_ref, k_buf), (v_ref, v_buf))):
            rows = pl.ds(pl.multiple_of((2 * seq + half) * piece, piece), piece)
            out.append(pltpu.make_async_copy(ref.at[seq], buf.at[slot, pl.ds(0, piece)], kv_sem.at[slot]))
            out.append(pltpu.make_async_copy(near_ref.at[rows], buf.at[slot, there], kv_sem.at[slot]))
        return out

    def aheads():
        at = base + size
        out = [pltpu.make_async_copy(q_ref.at[at], q_out, ahead_sem)]
        for half, ref in enumerate((k_ref, v_ref)):
            near_rows = pl.ds((2 * at + half) * piece, piece)
            out.append(pltpu.make_async_copy(ref.at[at], kv_out.at[2 * half], ahead_sem))
            out.append(pltpu.make_async_copy(near_ref.at[near_rows], kv_out.at[2 * half + 1], ahead_sem))
        return out

    def part(g):
        return pl.ds(g * GROUP, GROUP)

    def q_load(step, g):
        slot = lax.rem(step, depth)
        return pltpu.make_async_copy(q_ref.at[base + step, part(g)], q_buf.at[slot, part(g)], q_sem.at[slot, g])

    def o_store(step, g):
        slot = lax.rem(step, 2)
        return pltpu.make_async_copy(o_buf.at[slot, part(g)], o_ref.at[base + step, part(g)], o_sem.at[slot, g])

    def load(step):
        for copy in kv_loads(step):
            copy.start()
        for g in range(groups):
            q_load(step, g).start()

    def place(step):
        slot = lax.rem(step, depth)
        for ref, block in ((fara_ref, 2), (farb_ref, jnp.where(odd == 1, 3, 1))):
            there = pl.ds(pl.multiple_of(block * piece, piece), piece)
            for half, buf in enumerate((k_buf, v_buf)):
                buf[slot, there] = ref[pl.ds(pl.multiple_of((2 * step + half) * piece, piece), piece)]

    def run(count, step, cut):
        seq = base + step
        slot, out = lax.rem(step, depth), lax.rem(step, 2)
        keys = count * piece
        lane = lax.broadcasted_iota(jnp.int32, (piece, piece), 1)
        row = lax.broadcasted_iota(jnp.int32, (piece, piece), 0)
        low = jnp.maximum(jnp.where(row >= cut, cut, -keys), -me * piece)
        caps = [
            jnp.where((lane - n * piece <= row) & (lane - n * piece >= low), jnp.inf, -jnp.inf) for n in range(count)
        ]
        cap = jnp.concatenate([jnp.concatenate(caps, axis=1)] * GROUP, axis=0)
        logs = jnp.zeros((piece, piece), jnp.float32)

        def scores(g):
            q = q_buf[slot, g * GROUP:(g + 1) * GROUP].reshape(width, head)
            s = lax.dot_general(q, k_buf[slot, :keys], (((1,), (1,)), ((), ())), preferred_element_type=jnp.float32)
            s = jnp.minimum(s, cap)
            return s, jnp.max(s, axis=1, keepdims=True)

        def weigh(s, m):
            p = jnp.exp2((s - m) * (scale * LOG2E))
            return p.astype(jnp.bfloat16), m, jnp.sum(p, axis=1, keepdims=True)

        def finish(g, logs, p, m, l):
            o = jnp.dot(p, v_buf[slot, :keys], preferred_element_type=jnp.float32) * (1.0 / l)
            o_buf[out, g * GROUP:(g + 1) * GROUP] = o.astype(jnp.bfloat16).reshape(GROUP, piece, head)
            o_store(step, g).start()
            e = m * scale + jnp.log(l)
            for j in range(GROUP):
                logs = jnp.where(lane == g * GROUP + j, e[j * piece:(j + 1) * piece], logs)
            return logs

        now, before = scores(0), None
        for g in range(groups):
            later = scores(g + 1) if g + 1 < groups else None
            if before is not None:
                logs = finish(g - 1, logs, *before)
            before, now = weigh(*now), later
        logs = finish(groups - 1, logs, *before)
        lse_ref[:, pl.ds(seq, 1), :] = logs.T[:heads][:, None, :]

    n_ref[0] = jnp.where(me >= 2, 4, 2)
    if first:
        load(0)
    else:
        q_buf[0] = q_in[...]
        there = pl.ds(pl.multiple_of(jnp.where(odd == 1, 1, 3) * piece, piece), piece)
        for half, buf in enumerate((k_buf, v_buf)):
            buf[0, :piece] = kv_in[2 * half]
            buf[0, there] = kv_in[2 * half + 1]
        lse_ref[...] = lse_in[...]

    @pl.loop(0, size)
    def _(step):
        @pl.when((step > 0) | first)
        def _():
            for copy in kv_loads(step):
                copy.wait()
            for g in range(groups):
                q_load(step, g).wait()

        @pl.when((step == 0) & (size > 1))
        def _():
            load(1)

        @pl.when(step + 2 < size)
        def _():
            load(step + 2)

        if not last:
            @pl.when(step == max(size - 2, 0))
            def _():
                for copy in aheads():
                    copy.start()

        @pl.when(step >= 2)
        def _():
            for g in range(groups):
                o_store(step - 2, g).wait()

        place(step)
        need = n_ref[0]
        for count in (2, 3, 4):
            @pl.when((need == count) | (count == 2 and need == 1))
            def _():
                run(count, step, cut_ref[pl.ds(base + step, 1), :])

        @pl.when(step == 0)
        def _():
            scalars.wait()

        n_ref[0] = s_ref[jnp.minimum(base + step + 1, batch - 1)]

    if last:
        log_store = pltpu.make_async_copy(lse_ref, lse_out, lse_sem)
        log_store.start()
        log_store.wait()
    else:
        for copy in aheads():
            copy.wait()
    for step in range(max(size - 2, 0), size):
        for g in range(groups):
            o_store(step, g).wait()


def attend(n, needs, cuts, q, k, v, near, fara, farb, prev):
    batch, heads, piece, head = q.shape
    base, size = BOUNDS[n], CHUNKS[n]
    first, last = prev is None, n == len(CHUNKS) - 1
    hbm = pl.BlockSpec(memory_space=pltpu.HBM)
    vmem = pl.BlockSpec(memory_space=pltpu.VMEM)
    in_specs = [hbm, vmem] + [hbm] * 4 + [vmem] * 2
    needs, q, k, v, near = (pltpu.with_memory_space_constraint(x, pltpu.HBM) for x in (needs, q, k, v, near))
    args = [needs, cuts, q, k, v, near, fara, farb]
    aliases = {}
    if not first:
        in_specs += [hbm, vmem, vmem, vmem]
        args += list(prev)
        aliases = {8: 0}
    out_shape = [
        jax.ShapeDtypeStruct(q.shape, jnp.bfloat16),
        jax.ShapeDtypeStruct((heads, batch, piece), jnp.float32),
    ]
    if not last:
        out_shape += [
            jax.ShapeDtypeStruct(q.shape[1:], jnp.bfloat16),
            jax.ShapeDtypeStruct((4, piece, head), jnp.bfloat16),
        ]
    return pl.pallas_call(
        functools.partial(attend_kernel, first, last, base, size),
        in_specs=in_specs,
        out_specs=[hbm, hbm] if last else [hbm] + [vmem] * 3,
        scratch_shapes=([pltpu.VMEM(out_shape[1].shape, jnp.float32), pltpu.SemaphoreType.DMA] if last else []) + [
            pltpu.SMEM(needs.shape, jnp.int32),
            pltpu.SMEM((1,), jnp.int32),
            pltpu.VMEM((DEPTH, heads, piece, head), jnp.bfloat16),
            pltpu.VMEM((DEPTH, 4 * piece, head), jnp.bfloat16),
            pltpu.VMEM((DEPTH, 4 * piece, head), jnp.bfloat16),
            pltpu.VMEM((2, heads, piece, head), jnp.bfloat16),
            pltpu.SemaphoreType.DMA,
            pltpu.SemaphoreType.DMA((DEPTH,)),
            pltpu.SemaphoreType.DMA((DEPTH, heads // GROUP)),
            pltpu.SemaphoreType.DMA((2, heads // GROUP)),
            pltpu.SemaphoreType.DMA,
        ],
        out_shape=out_shape,
        input_output_aliases=aliases,
        compiler_params=pltpu.CompilerParams(vmem_limit_bytes=20 << 20),
        cost_estimate=pl.CostEstimate(
            flops=size * heads * piece * 4 * piece * head * 4,
            bytes_accessed=size * heads * piece * head * 4,
            transcendentals=0,
        ),
    )(*args)


def swap_kernel(mine_ref, other_ref, send_sem, recv_sem):
    me = lax.axis_index("cp")
    partner = {"cp": me + 1 - 2 * lax.rem(me, 2)}
    barrier = pltpu.get_barrier_semaphore()
    pl.semaphore_signal(barrier, inc=1, device_id=partner, device_id_type=pl.DeviceIdType.MESH)
    pl.semaphore_wait(barrier, 1)
    copy = pltpu.make_async_remote_copy(
        src_ref=mine_ref,
        dst_ref=other_ref,
        send_sem=send_sem,
        recv_sem=recv_sem,
        device_id=partner,
        device_id_type=pl.DeviceIdType.MESH,
    )
    copy.start()
    copy.wait()


def swap(n, x):
    vmem = pl.BlockSpec(memory_space=pltpu.VMEM)
    return pl.pallas_call(
        swap_kernel,
        in_specs=[vmem],
        out_specs=vmem,
        out_shape=jax.ShapeDtypeStruct(x.shape, x.dtype),
        scratch_shapes=[pltpu.SemaphoreType.DMA, pltpu.SemaphoreType.DMA],
        compiler_params=pltpu.CompilerParams(
            collective_id=n, has_side_effects=True, vmem_limit_bytes=16 << 20
        ),
        cost_estimate=pl.CostEstimate(flops=1 << 20, bytes_accessed=4 * x.size, transcendentals=0),
    )(x)


def shift(x, pairs):
    return lax.ppermute(x, "cp", pairs)


def solution(mesh):
    def local(q_loc, k_loc, v_loc, seg_loc):
        batch, piece, _, _ = q_loc.shape
        me = lax.axis_index("cp")
        q = jnp.transpose(q_loc, (0, 2, 1, 3))
        ranges = tuple(zip(BOUNDS[:-1], BOUNDS[1:]))
        sends = pack(ranges[:1], (True,), seg_loc, k_loc, v_loc)
        *more, whole = pack(ranges[1:] + ((0, batch),), (False,) * len(ranges[1:]) + (True,), seg_loc, k_loc, v_loc)
        sends = list(sends) + more
        fara = [shift(x, ACROSS) for x in sends]
        near = shift(whole, BESIDE)
        farb = [swap(n, x) for n, x in enumerate(fara)]

        def zeros(packed, there):
            return jnp.where(there, packed[-batch:, 0].astype(jnp.int32), 0)

        odd, upper = me % 2 == 1, me >= 2
        cuts = zeros(whole, True) + zeros(near, odd) + zeros(fara[0], upper) + zeros(farb[0], upper)
        need = jnp.where(cuts <= me * piece, me - cuts // piece, me) + 1
        table = jnp.broadcast_to((cuts - me * piece)[:, None], (batch, piece))
        state = None
        for n in range(len(CHUNKS)):
            state = attend(n, need.astype(jnp.int32), table, q, k_loc, v_loc, near, fara[n], farb[n], state)
        out, lse = state[:2]
        return jnp.transpose(out, (0, 2, 1, 3)), jnp.transpose(lse, (1, 2, 0))

    return jax.shard_map(
        local,
        mesh=mesh,
        in_specs=(P("dp", "cp", None, None), P("dp", "cp", None), P("dp", "cp", None), P("dp", "cp")),
        out_specs=(P("dp", "cp", None, None), P("dp", "cp", None)),
        check_vma=False,
    )
```

```python
import functools

import jax
import jax.numpy as jnp
from jax import lax
from jax.experimental import pallas as pl
from jax.experimental.pallas import tpu as pltpu
from jax.sharding import PartitionSpec as P


CHUNKS = (5, 6, 6, 5, 4, 3, 3)
BOUNDS = tuple(sum(CHUNKS[:n]) for n in range(len(CHUNKS) + 1))
GROUP = 2
DEPTH = 3
LOG2E = 1.4426950408889634

ACROSS = [(0, 2), (1, 3)]
BESIDE = [(0, 1), (2, 3)]


def pack_kernel(senders, ranges, tails, seg_ref, k_ref, v_ref, *rest):
    count = len(ranges)
    outs, (seg_scr, seg_sem, sem, *stages) = rest[:count], rest[count:]
    finals, outs = (outs, stages) if stages else ((), outs)
    batch, piece, head = k_ref.shape
    segments = pltpu.make_async_copy(seg_ref, seg_scr, seg_sem)

    def copies(i, out, at):
        for half, ref in enumerate((k_ref, v_ref)):
            rows = pl.ds(pl.multiple_of((2 * i + half) * piece, piece), piece)
            yield pltpu.make_async_copy(ref.at[at + i], out.at[rows], sem)

    def fill():
        segments.start()
        for out, (a, b) in zip(outs, ranges):
            @pl.loop(0, b - a)
            def _(i):
                for copy in copies(i, out, a):
                    copy.start()
        segments.wait()
        here = jnp.sum((seg_scr[...] == 0).astype(jnp.float32), axis=1, keepdims=True)
        rows = jnp.broadcast_to(here, (batch, head)).astype(jnp.bfloat16)
        for out, (a, b), tail in zip(outs, ranges, tails):
            if tail:
                out[(b - a) * 2 * piece:] = rows
        for out, (a, b) in zip(outs, ranges):
            @pl.loop(0, b - a)
            def _(i):
                for copy in copies(i, out, a):
                    copy.wait()
        stores = [pltpu.make_async_copy(out, final, sem) for out, final in zip(outs, finals)]
        for store in stores:
            store.start()
        for store in stores:
            store.wait()

    if senders is None:
        fill()
    else:
        pl.when(lax.axis_index("cp") < senders)(fill)


def pack(senders, ranges, tails, seg, k, v):
    batch, piece, head = k.shape
    vmem, hbm = pl.BlockSpec(memory_space=pltpu.VMEM), pl.BlockSpec(memory_space=pltpu.HBM)
    seg, k, v = (pltpu.with_memory_space_constraint(x, pltpu.HBM) for x in (seg, k, v))
    out_shape = [
        jax.ShapeDtypeStruct(((b - a) * 2 * piece + (batch if tail else 0), head), jnp.bfloat16)
        for (a, b), tail in zip(ranges, tails)
    ]
    stages = [] if senders is None else [pltpu.VMEM(x.shape, x.dtype) for x in out_shape]
    return pl.pallas_call(
        functools.partial(pack_kernel, senders, ranges, tails),
        in_specs=[hbm] * 3,
        out_specs=[hbm if stages else vmem] * len(ranges),
        out_shape=out_shape,
        scratch_shapes=[pltpu.VMEM(seg.shape, jnp.int32), pltpu.SemaphoreType.DMA, pltpu.SemaphoreType.DMA] + stages,
        compiler_params=pltpu.CompilerParams(vmem_limit_bytes=16 << 20),
        cost_estimate=pl.CostEstimate(flops=1 << 20, bytes_accessed=4 * k.size, transcendentals=0),
    )(seg, k, v)


def attend_kernel(first, last, base, size, s_hbm, cut_ref, q_ref, k_ref, v_ref, near_ref, fara_ref, farb_ref, *rest):
    if not first:
        _, lse_in, q_in, kv_in, *rest = rest
    o_ref, lse_ref, *rest = rest
    if last:
        lse_out, (lse_ref, lse_sem, *rest) = lse_ref, rest
    else:
        q_out, kv_out, *rest = rest
    s_ref, n_ref, q_buf, k_buf, v_buf, o_buf, s_sem, kv_sem, q_sem, o_sem, ahead_sem = rest
    depth, heads, piece, head = q_buf.shape
    batch = lse_ref.shape[1]
    groups = heads // GROUP
    width = GROUP * piece
    scale = head ** -0.5
    me = lax.axis_index("cp")
    odd = lax.rem(me, 2)
    scalars = pltpu.make_async_copy(s_hbm, s_ref, s_sem)
    scalars.start()

    def kv_loads(step):
        slot = lax.rem(step, depth)
        seq = base + step
        there = pl.ds(pl.multiple_of(jnp.where(odd == 1, 1, 3) * piece, piece), piece)
        out = []
        for half, (ref, buf) in enumerate(((k_ref, k_buf), (v_ref, v_buf))):
            rows = pl.ds(pl.multiple_of((2 * seq + half) * piece, piece), piece)
            out.append(pltpu.make_async_copy(ref.at[seq], buf.at[slot, pl.ds(0, piece)], kv_sem.at[slot]))
            out.append(pltpu.make_async_copy(near_ref.at[rows], buf.at[slot, there], kv_sem.at[slot]))
        return out

    def aheads():
        at = base + size
        out = [pltpu.make_async_copy(q_ref.at[at], q_out, ahead_sem)]
        for half, ref in enumerate((k_ref, v_ref)):
            near_rows = pl.ds((2 * at + half) * piece, piece)
            out.append(pltpu.make_async_copy(ref.at[at], kv_out.at[2 * half], ahead_sem))
            out.append(pltpu.make_async_copy(near_ref.at[near_rows], kv_out.at[2 * half + 1], ahead_sem))
        return out

    def part(g):
        return pl.ds(g * GROUP, GROUP)

    def q_load(step, g):
        slot = lax.rem(step, depth)
        return pltpu.make_async_copy(q_ref.at[base + step, part(g)], q_buf.at[slot, part(g)], q_sem.at[slot, g])

    def o_store(step, g):
        slot = lax.rem(step, 2)
        return pltpu.make_async_copy(o_buf.at[slot, part(g)], o_ref.at[base + step, part(g)], o_sem.at[slot, g])

    def load(step):
        for copy in kv_loads(step):
            copy.start()
        for g in range(groups):
            q_load(step, g).start()

    def place(step):
        slot = lax.rem(step, depth)
        for ref, block in ((fara_ref, 2), (farb_ref, jnp.where(odd == 1, 3, 1))):
            there = pl.ds(pl.multiple_of(block * piece, piece), piece)
            for half, buf in enumerate((k_buf, v_buf)):
                buf[slot, there] = ref[pl.ds(pl.multiple_of((2 * step + half) * piece, piece), piece)]

    def run(count, step, cut):
        seq = base + step
        slot, out = lax.rem(step, depth), lax.rem(step, 2)
        keys = count * piece
        lane = lax.broadcasted_iota(jnp.int32, (piece, piece), 1)
        row = lax.broadcasted_iota(jnp.int32, (piece, piece), 0)
        low = jnp.maximum(jnp.where(row >= cut, cut, -keys), -me * piece)
        caps = [
            jnp.where((lane - n * piece <= row) & (lane - n * piece >= low), jnp.inf, -jnp.inf) for n in range(count)
        ]
        cap = jnp.concatenate([jnp.concatenate(caps, axis=1)] * GROUP, axis=0)
        logs = jnp.zeros((piece, piece), jnp.float32)

        def scores(g):
            q = q_buf[slot, g * GROUP:(g + 1) * GROUP].reshape(width, head)
            s = lax.dot_general(q, k_buf[slot, :keys], (((1,), (1,)), ((), ())), preferred_element_type=jnp.float32)
            s = jnp.minimum(s, cap)
            return s, jnp.max(s, axis=1, keepdims=True)

        def weigh(s, m):
            p = jnp.exp2((s - m) * (scale * LOG2E))
            return p.astype(jnp.bfloat16), m, jnp.sum(p, axis=1, keepdims=True)

        def finish(g, logs, p, m, l):
            o = jnp.dot(p, v_buf[slot, :keys], preferred_element_type=jnp.float32) * (1.0 / l)
            o_buf[out, g * GROUP:(g + 1) * GROUP] = o.astype(jnp.bfloat16).reshape(GROUP, piece, head)
            o_store(step, g).start()
            e = m * scale + jnp.log(l)
            for j in range(GROUP):
                logs = jnp.where(lane == g * GROUP + j, e[j * piece:(j + 1) * piece], logs)
            return logs

        now, before = scores(0), None
        for g in range(groups):
            later = scores(g + 1) if g + 1 < groups else None
            if before is not None:
                logs = finish(g - 1, logs, *before)
            before, now = weigh(*now), later
        logs = finish(groups - 1, logs, *before)
        lse_ref[:, pl.ds(seq, 1), :] = logs.T[:heads][:, None, :]

    n_ref[0] = jnp.where(me >= 2, 4, 2)
    if first:
        load(0)
    else:
        q_buf[0] = q_in[...]
        there = pl.ds(pl.multiple_of(jnp.where(odd == 1, 1, 3) * piece, piece), piece)
        for half, buf in enumerate((k_buf, v_buf)):
            buf[0, :piece] = kv_in[2 * half]
            buf[0, there] = kv_in[2 * half + 1]
        lse_ref[...] = lse_in[...]

    @pl.loop(0, size)
    def _(step):
        @pl.when((step > 0) | first)
        def _():
            for copy in kv_loads(step):
                copy.wait()
            for g in range(groups):
                q_load(step, g).wait()

        @pl.when((step == 0) & (size > 1))
        def _():
            load(1)

        @pl.when(step + 2 < size)
        def _():
            load(step + 2)

        if not last:
            @pl.when(step == max(size - 2, 0))
            def _():
                for copy in aheads():
                    copy.start()

        @pl.when(step >= 2)
        def _():
            for g in range(groups):
                o_store(step - 2, g).wait()

        place(step)
        need = n_ref[0]
        for count in (2, 3, 4):
            @pl.when((need == count) | (count == 2 and need == 1))
            def _():
                run(count, step, cut_ref[pl.ds(base + step, 1), :])

        @pl.when(step == 0)
        def _():
            scalars.wait()

        n_ref[0] = s_ref[jnp.minimum(base + step + 1, batch - 1)]

    if last:
        log_store = pltpu.make_async_copy(lse_ref, lse_out, lse_sem)
        log_store.start()
        log_store.wait()
    else:
        for copy in aheads():
            copy.wait()
    for step in range(max(size - 2, 0), size):
        for g in range(groups):
            o_store(step, g).wait()


def attend(n, needs, cuts, q, k, v, near, fara, farb, prev):
    batch, heads, piece, head = q.shape
    base, size = BOUNDS[n], CHUNKS[n]
    first, last = prev is None, n == len(CHUNKS) - 1
    hbm = pl.BlockSpec(memory_space=pltpu.HBM)
    vmem = pl.BlockSpec(memory_space=pltpu.VMEM)
    in_specs = [hbm, vmem] + [hbm] * 4 + [vmem] * 2
    needs, q, k, v, near = (pltpu.with_memory_space_constraint(x, pltpu.HBM) for x in (needs, q, k, v, near))
    args = [needs, cuts, q, k, v, near, fara, farb]
    aliases = {}
    if not first:
        in_specs += [hbm, vmem, vmem, vmem]
        args += list(prev)
        aliases = {8: 0}
    out_shape = [
        jax.ShapeDtypeStruct(q.shape, jnp.bfloat16),
        jax.ShapeDtypeStruct((heads, batch, piece), jnp.float32),
    ]
    if not last:
        out_shape += [
            jax.ShapeDtypeStruct(q.shape[1:], jnp.bfloat16),
            jax.ShapeDtypeStruct((4, piece, head), jnp.bfloat16),
        ]
    return pl.pallas_call(
        functools.partial(attend_kernel, first, last, base, size),
        in_specs=in_specs,
        out_specs=[hbm, hbm] if last else [hbm] + [vmem] * 3,
        scratch_shapes=([pltpu.VMEM(out_shape[1].shape, jnp.float32), pltpu.SemaphoreType.DMA] if last else []) + [
            pltpu.SMEM(needs.shape, jnp.int32),
            pltpu.SMEM((1,), jnp.int32),
            pltpu.VMEM((DEPTH, heads, piece, head), jnp.bfloat16),
            pltpu.VMEM((DEPTH, 4 * piece, head), jnp.bfloat16),
            pltpu.VMEM((DEPTH, 4 * piece, head), jnp.bfloat16),
            pltpu.VMEM((2, heads, piece, head), jnp.bfloat16),
            pltpu.SemaphoreType.DMA,
            pltpu.SemaphoreType.DMA((DEPTH,)),
            pltpu.SemaphoreType.DMA((DEPTH, heads // GROUP)),
            pltpu.SemaphoreType.DMA((2, heads // GROUP)),
            pltpu.SemaphoreType.DMA,
        ],
        out_shape=out_shape,
        input_output_aliases=aliases,
        compiler_params=pltpu.CompilerParams(vmem_limit_bytes=20 << 20),
        cost_estimate=pl.CostEstimate(
            flops=size * heads * piece * 4 * piece * head * 4,
            bytes_accessed=size * heads * piece * head * 4,
            transcendentals=0,
        ),
    )(*args)


def swap_kernel(mine_ref, other_ref, send_sem, recv_sem):
    me = lax.axis_index("cp")
    partner = {"cp": me + 1 - 2 * lax.rem(me, 2)}
    barrier = pltpu.get_barrier_semaphore()
    pl.semaphore_signal(barrier, inc=1, device_id=partner, device_id_type=pl.DeviceIdType.MESH)
    pl.semaphore_wait(barrier, 1)
    copy = pltpu.make_async_remote_copy(
        src_ref=mine_ref,
        dst_ref=other_ref,
        send_sem=send_sem,
        recv_sem=recv_sem,
        device_id=partner,
        device_id_type=pl.DeviceIdType.MESH,
    )
    copy.start()
    copy.wait()


def swap(n, x):
    vmem = pl.BlockSpec(memory_space=pltpu.VMEM)
    return pl.pallas_call(
        swap_kernel,
        in_specs=[vmem],
        out_specs=vmem,
        out_shape=jax.ShapeDtypeStruct(x.shape, x.dtype),
        scratch_shapes=[pltpu.SemaphoreType.DMA, pltpu.SemaphoreType.DMA],
        compiler_params=pltpu.CompilerParams(
            collective_id=n, has_side_effects=True, vmem_limit_bytes=16 << 20
        ),
        cost_estimate=pl.CostEstimate(flops=1 << 20, bytes_accessed=4 * x.size, transcendentals=0),
    )(x)


def shift(x, pairs):
    return lax.ppermute(x, "cp", pairs)


def solution(mesh):
    def local(q_loc, k_loc, v_loc, seg_loc):
        batch, piece, _, _ = q_loc.shape
        me = lax.axis_index("cp")
        q = jnp.transpose(q_loc, (0, 2, 1, 3))
        ranges = tuple(zip(BOUNDS[:-1], BOUNDS[1:]))
        sends = pack(2, ranges[:1], (True,), seg_loc, k_loc, v_loc)
        *more, whole = pack(None, ranges[1:] + ((0, batch),), (False,) * len(ranges[1:]) + (True,), seg_loc, k_loc, v_loc)
        sends = list(sends) + more
        fara = [shift(x, ACROSS) for x in sends]
        near = shift(whole, BESIDE)
        farb = [swap(n, x) for n, x in enumerate(fara)]

        def zeros(packed, there):
            return jnp.where(there, packed[-batch:, 0].astype(jnp.int32), 0)

        odd, upper = me % 2 == 1, me >= 2
        cuts = zeros(whole, True) + zeros(near, odd) + zeros(fara[0], upper) + zeros(farb[0], upper)
        need = jnp.where(cuts <= me * piece, me - cuts // piece, me) + 1
        table = jnp.broadcast_to((cuts - me * piece)[:, None], (batch, piece))
        state = None
        for n in range(len(CHUNKS)):
            state = attend(n, need.astype(jnp.int32), table, q, k_loc, v_loc, near, fara[n], farb[n], state)
        out, lse = state[:2]
        return jnp.transpose(out, (0, 2, 1, 3)), jnp.transpose(lse, (1, 2, 0))

    return jax.shard_map(
        local,
        mesh=mesh,
        in_specs=(P("dp", "cp", None, None), P("dp", "cp", None), P("dp", "cp", None), P("dp", "cp")),
        out_specs=(P("dp", "cp", None, None), P("dp", "cp", None)),
        check_vma=False,
    )
```

```python
import functools

import jax
import jax.numpy as jnp
from jax import lax
from jax.experimental import pallas as pl
from jax.experimental.pallas import tpu as pltpu
from jax.sharding import PartitionSpec as P


CHUNKS = (4, 6, 6, 6, 4, 3, 3)
BOUNDS = tuple(sum(CHUNKS[:n]) for n in range(len(CHUNKS) + 1))
GROUP = 2
DEPTH = 3
LOG2E = 1.4426950408889634

ACROSS = [(0, 2), (1, 3)]
BESIDE = [(0, 1), (2, 3)]


def pack_kernel(senders, ranges, tails, seg_ref, k_ref, v_ref, *rest):
    outs, (seg_scr, seg_sem, sem) = rest[:-3], rest[-3:]
    batch, piece, head = k_ref.shape
    segments = pltpu.make_async_copy(seg_ref, seg_scr, seg_sem)

    def copies(i, out, at):
        for half, ref in enumerate((k_ref, v_ref)):
            rows = pl.ds(pl.multiple_of((2 * i + half) * piece, piece), piece)
            yield pltpu.make_async_copy(ref.at[at + i], out.at[rows], sem)

    def fill():
        segments.start()
        for out, (a, b) in zip(outs, ranges):
            @pl.loop(0, b - a)
            def _(i):
                for copy in copies(i, out, a):
                    copy.start()
        segments.wait()
        here = jnp.sum((seg_scr[...] == 0).astype(jnp.float32), axis=1, keepdims=True)
        rows = jnp.broadcast_to(here, (batch, head)).astype(jnp.bfloat16)
        for out, (a, b), tail in zip(outs, ranges, tails):
            if tail:
                out[(b - a) * 2 * piece:] = rows
        for out, (a, b) in zip(outs, ranges):
            @pl.loop(0, b - a)
            def _(i):
                for copy in copies(i, out, a):
                    copy.wait()

    if senders is None:
        fill()
    else:
        pl.when(lax.axis_index("cp") < senders)(fill)


def pack(senders, ranges, tails, seg, k, v):
    batch, piece, head = k.shape
    vmem, hbm = pl.BlockSpec(memory_space=pltpu.VMEM), pl.BlockSpec(memory_space=pltpu.HBM)
    seg, k, v = (pltpu.with_memory_space_constraint(x, pltpu.HBM) for x in (seg, k, v))
    out_shape = [
        jax.ShapeDtypeStruct(((b - a) * 2 * piece + (batch if tail else 0), head), jnp.bfloat16)
        for (a, b), tail in zip(ranges, tails)
    ]
    return pl.pallas_call(
        functools.partial(pack_kernel, senders, ranges, tails),
        in_specs=[hbm] * 3,
        out_specs=[vmem] * len(ranges),
        out_shape=out_shape,
        scratch_shapes=[pltpu.VMEM(seg.shape, jnp.int32), pltpu.SemaphoreType.DMA, pltpu.SemaphoreType.DMA],
        compiler_params=pltpu.CompilerParams(vmem_limit_bytes=16 << 20),
        cost_estimate=pl.CostEstimate(flops=1 << 20, bytes_accessed=4 * k.size, transcendentals=0),
    )(seg, k, v)


def attend_kernel(first, last, base, size, s_hbm, cut_ref, q_ref, k_ref, v_ref, near_ref, fara_ref, farb_ref, *rest):
    if not first:
        _, lse_in, q_in, kv_in, *rest = rest
    o_ref, lse_ref, *rest = rest
    if last:
        lse_out, (lse_ref, lse_sem, *rest) = lse_ref, rest
    else:
        q_out, kv_out, *rest = rest
    s_ref, n_ref, q_buf, k_buf, v_buf, o_buf, s_sem, kv_sem, q_sem, o_sem, ahead_sem = rest
    depth, heads, piece, head = q_buf.shape
    batch = lse_ref.shape[1]
    groups = heads // GROUP
    width = GROUP * piece
    scale = head ** -0.5
    me = lax.axis_index("cp")
    odd = lax.rem(me, 2)
    scalars = pltpu.make_async_copy(s_hbm, s_ref, s_sem)
    scalars.start()

    def kv_loads(step):
        slot = lax.rem(step, depth)
        seq = base + step
        there = pl.ds(pl.multiple_of(jnp.where(odd == 1, 1, 3) * piece, piece), piece)
        out = []
        for half, (ref, buf) in enumerate(((k_ref, k_buf), (v_ref, v_buf))):
            rows = pl.ds(pl.multiple_of((2 * seq + half) * piece, piece), piece)
            out.append(pltpu.make_async_copy(ref.at[seq], buf.at[slot, pl.ds(0, piece)], kv_sem.at[slot]))
            out.append(pltpu.make_async_copy(near_ref.at[rows], buf.at[slot, there], kv_sem.at[slot]))
        return out

    def aheads():
        at = base + size
        out = [pltpu.make_async_copy(q_ref.at[at], q_out, ahead_sem)]
        for half, ref in enumerate((k_ref, v_ref)):
            near_rows = pl.ds((2 * at + half) * piece, piece)
            out.append(pltpu.make_async_copy(ref.at[at], kv_out.at[2 * half], ahead_sem))
            out.append(pltpu.make_async_copy(near_ref.at[near_rows], kv_out.at[2 * half + 1], ahead_sem))
        return out

    def part(g):
        return pl.ds(g * GROUP, GROUP)

    def q_load(step, g):
        slot = lax.rem(step, depth)
        return pltpu.make_async_copy(q_ref.at[base + step, part(g)], q_buf.at[slot, part(g)], q_sem.at[slot, g])

    def o_store(step, g):
        slot = lax.rem(step, 2)
        return pltpu.make_async_copy(o_buf.at[slot, part(g)], o_ref.at[base + step, part(g)], o_sem.at[slot, g])

    def load(step):
        for copy in kv_loads(step):
            copy.start()
        for g in range(groups):
            q_load(step, g).start()

    def place(step):
        slot = lax.rem(step, depth)
        for ref, block in ((fara_ref, 2), (farb_ref, jnp.where(odd == 1, 3, 1))):
            there = pl.ds(pl.multiple_of(block * piece, piece), piece)
            for half, buf in enumerate((k_buf, v_buf)):
                buf[slot, there] = ref[pl.ds(pl.multiple_of((2 * step + half) * piece, piece), piece)]

    def run(count, step, cut):
        seq = base + step
        slot, out = lax.rem(step, depth), lax.rem(step, 2)
        keys = count * piece
        lane = lax.broadcasted_iota(jnp.int32, (piece, piece), 1)
        row = lax.broadcasted_iota(jnp.int32, (piece, piece), 0)
        low = jnp.maximum(jnp.where(row >= cut, cut, -keys), -me * piece)
        caps = [
            jnp.where((lane - n * piece <= row) & (lane - n * piece >= low), jnp.inf, -jnp.inf) for n in range(count)
        ]
        cap = jnp.concatenate([jnp.concatenate(caps, axis=1)] * GROUP, axis=0)
        logs = jnp.zeros((piece, piece), jnp.float32)

        def scores(g):
            q = q_buf[slot, g * GROUP:(g + 1) * GROUP].reshape(width, head)
            s = lax.dot_general(q, k_buf[slot, :keys], (((1,), (1,)), ((), ())), preferred_element_type=jnp.float32)
            s = jnp.minimum(s, cap)
            return s, jnp.max(s, axis=1, keepdims=True)

        def weigh(s, m):
            p = jnp.exp2((s - m) * (scale * LOG2E))
            return p.astype(jnp.bfloat16), m, jnp.sum(p, axis=1, keepdims=True)

        def finish(g, logs, p, m, l):
            o = jnp.dot(p, v_buf[slot, :keys], preferred_element_type=jnp.float32) * (1.0 / l)
            o_buf[out, g * GROUP:(g + 1) * GROUP] = o.astype(jnp.bfloat16).reshape(GROUP, piece, head)
            o_store(step, g).start()
            e = m * scale + jnp.log(l)
            for j in range(GROUP):
                logs = jnp.where(lane == g * GROUP + j, e[j * piece:(j + 1) * piece], logs)
            return logs

        now, before = scores(0), None
        for g in range(groups):
            later = scores(g + 1) if g + 1 < groups else None
            if before is not None:
                logs = finish(g - 1, logs, *before)
            before, now = weigh(*now), later
        logs = finish(groups - 1, logs, *before)
        lse_ref[:, pl.ds(seq, 1), :] = logs.T[:heads][:, None, :]

    n_ref[0] = jnp.where(me >= 2, 4, 2)
    if first:
        load(0)
    else:
        q_buf[0] = q_in[...]
        there = pl.ds(pl.multiple_of(jnp.where(odd == 1, 1, 3) * piece, piece), piece)
        for half, buf in enumerate((k_buf, v_buf)):
            buf[0, :piece] = kv_in[2 * half]
            buf[0, there] = kv_in[2 * half + 1]
        lse_ref[...] = lse_in[...]

    @pl.loop(0, size)
    def _(step):
        @pl.when((step > 0) | first)
        def _():
            for copy in kv_loads(step):
                copy.wait()
            for g in range(groups):
                q_load(step, g).wait()

        @pl.when((step == 0) & (size > 1))
        def _():
            load(1)

        @pl.when(step + 2 < size)
        def _():
            load(step + 2)

        if not last:
            @pl.when(step == max(size - 2, 0))
            def _():
                for copy in aheads():
                    copy.start()

        @pl.when(step >= 2)
        def _():
            for g in range(groups):
                o_store(step - 2, g).wait()

        place(step)
        need = n_ref[0]
        for count in (2, 3, 4):
            @pl.when((need == count) | (count == 2 and need == 1))
            def _():
                run(count, step, cut_ref[pl.ds(base + step, 1), :])

        @pl.when(step == 0)
        def _():
            scalars.wait()

        n_ref[0] = s_ref[jnp.minimum(base + step + 1, batch - 1)]

    if last:
        log_store = pltpu.make_async_copy(lse_ref, lse_out, lse_sem)
        log_store.start()
        log_store.wait()
    else:
        for copy in aheads():
            copy.wait()
    for step in range(max(size - 2, 0), size):
        for g in range(groups):
            o_store(step, g).wait()


def attend(n, needs, cuts, q, k, v, near, fara, farb, prev):
    batch, heads, piece, head = q.shape
    base, size = BOUNDS[n], CHUNKS[n]
    first, last = prev is None, n == len(CHUNKS) - 1
    hbm = pl.BlockSpec(memory_space=pltpu.HBM)
    vmem = pl.BlockSpec(memory_space=pltpu.VMEM)
    in_specs = [hbm, vmem] + [hbm] * 4 + [vmem] * 2
    needs, q, k, v, near = (pltpu.with_memory_space_constraint(x, pltpu.HBM) for x in (needs, q, k, v, near))
    args = [needs, cuts, q, k, v, near, fara, farb]
    aliases = {}
    if not first:
        in_specs += [hbm, vmem, vmem, vmem]
        args += list(prev)
        aliases = {8: 0}
    out_shape = [
        jax.ShapeDtypeStruct(q.shape, jnp.bfloat16),
        jax.ShapeDtypeStruct((heads, batch, piece), jnp.float32),
    ]
    if not last:
        out_shape += [
            jax.ShapeDtypeStruct(q.shape[1:], jnp.bfloat16),
            jax.ShapeDtypeStruct((4, piece, head), jnp.bfloat16),
        ]
    return pl.pallas_call(
        functools.partial(attend_kernel, first, last, base, size),
        in_specs=in_specs,
        out_specs=[hbm, hbm] if last else [hbm] + [vmem] * 3,
        scratch_shapes=([pltpu.VMEM(out_shape[1].shape, jnp.float32), pltpu.SemaphoreType.DMA] if last else []) + [
            pltpu.SMEM(needs.shape, jnp.int32),
            pltpu.SMEM((1,), jnp.int32),
            pltpu.VMEM((DEPTH, heads, piece, head), jnp.bfloat16),
            pltpu.VMEM((DEPTH, 4 * piece, head), jnp.bfloat16),
            pltpu.VMEM((DEPTH, 4 * piece, head), jnp.bfloat16),
            pltpu.VMEM((2, heads, piece, head), jnp.bfloat16),
            pltpu.SemaphoreType.DMA,
            pltpu.SemaphoreType.DMA((DEPTH,)),
            pltpu.SemaphoreType.DMA((DEPTH, heads // GROUP)),
            pltpu.SemaphoreType.DMA((2, heads // GROUP)),
            pltpu.SemaphoreType.DMA,
        ],
        out_shape=out_shape,
        input_output_aliases=aliases,
        compiler_params=pltpu.CompilerParams(vmem_limit_bytes=20 << 20),
        cost_estimate=pl.CostEstimate(
            flops=size * heads * piece * 4 * piece * head * 4,
            bytes_accessed=size * heads * piece * head * 4,
            transcendentals=0,
        ),
    )(*args)


def swap_kernel(mine_ref, other_ref, send_sem, recv_sem):
    me = lax.axis_index("cp")
    partner = {"cp": me + 1 - 2 * lax.rem(me, 2)}
    barrier = pltpu.get_barrier_semaphore()
    pl.semaphore_signal(barrier, inc=1, device_id=partner, device_id_type=pl.DeviceIdType.MESH)
    pl.semaphore_wait(barrier, 1)
    copy = pltpu.make_async_remote_copy(
        src_ref=mine_ref,
        dst_ref=other_ref,
        send_sem=send_sem,
        recv_sem=recv_sem,
        device_id=partner,
        device_id_type=pl.DeviceIdType.MESH,
    )
    copy.start()
    copy.wait()


def swap(n, x):
    vmem = pl.BlockSpec(memory_space=pltpu.VMEM)
    return pl.pallas_call(
        swap_kernel,
        in_specs=[vmem],
        out_specs=vmem,
        out_shape=jax.ShapeDtypeStruct(x.shape, x.dtype),
        scratch_shapes=[pltpu.SemaphoreType.DMA, pltpu.SemaphoreType.DMA],
        compiler_params=pltpu.CompilerParams(
            collective_id=n, has_side_effects=True, vmem_limit_bytes=16 << 20
        ),
        cost_estimate=pl.CostEstimate(flops=1 << 20, bytes_accessed=4 * x.size, transcendentals=0),
    )(x)


def shift(x, pairs):
    return lax.ppermute(x, "cp", pairs)


def solution(mesh):
    def local(q_loc, k_loc, v_loc, seg_loc):
        batch, piece, _, _ = q_loc.shape
        me = lax.axis_index("cp")
        q = jnp.transpose(q_loc, (0, 2, 1, 3))
        ranges = tuple(zip(BOUNDS[:-1], BOUNDS[1:]))
        sends = pack(2, ranges[:1], (True,), seg_loc, k_loc, v_loc)
        *more, whole = pack(None, ranges[1:] + ((0, batch),), (False,) * len(ranges[1:]) + (True,), seg_loc, k_loc, v_loc)
        sends = list(sends) + more
        fara = [shift(x, ACROSS) for x in sends]
        near = shift(whole, BESIDE)
        farb = [swap(n, x) for n, x in enumerate(fara)]

        def zeros(packed, there):
            return jnp.where(there, packed[-batch:, 0].astype(jnp.int32), 0)

        odd, upper = me % 2 == 1, me >= 2
        cuts = zeros(whole, True) + zeros(near, odd) + zeros(fara[0], upper) + zeros(farb[0], upper)
        need = jnp.where(cuts <= me * piece, me - cuts // piece, me) + 1
        table = jnp.broadcast_to((cuts - me * piece)[:, None], (batch, piece))
        state = None
        for n in range(len(CHUNKS)):
            state = attend(n, need.astype(jnp.int32), table, q, k_loc, v_loc, near, fara[n], farb[n], state)
        out, lse = state[:2]
        return jnp.transpose(out, (0, 2, 1, 3)), jnp.transpose(lse, (1, 2, 0))

    return jax.shard_map(
        local,
        mesh=mesh,
        in_specs=(P("dp", "cp", None, None), P("dp", "cp", None), P("dp", "cp", None), P("dp", "cp")),
        out_specs=(P("dp", "cp", None, None), P("dp", "cp", None)),
        check_vma=False,
    )
```

```python
import functools

import jax
import jax.numpy as jnp
from jax import lax
from jax.experimental import pallas as pl
from jax.experimental.pallas import tpu as pltpu
from jax.sharding import PartitionSpec as P


CHUNKS = (4, 6, 6, 6, 4, 3, 3)
BOUNDS = tuple(sum(CHUNKS[:n]) for n in range(len(CHUNKS) + 1))
GROUP = 2
DEPTH = 3
LOG2E = 1.4426950408889634

ACROSS = [(0, 2), (1, 3)]
BESIDE = [(0, 1), (2, 3)]


def pack_kernel(senders, ranges, tails, seg_ref, k_ref, v_ref, *rest):
    outs, (seg_scr, seg_sem, sem) = rest[:-3], rest[-3:]
    batch, piece, head = k_ref.shape
    segments = pltpu.make_async_copy(seg_ref, seg_scr, seg_sem)

    def copies(i, out, at):
        for half, ref in enumerate((k_ref, v_ref)):
            rows = pl.ds(pl.multiple_of((2 * i + half) * piece, piece), piece)
            yield pltpu.make_async_copy(ref.at[at + i], out.at[rows], sem)

    def fill():
        segments.start()
        for out, (a, b) in zip(outs, ranges):
            @pl.loop(0, b - a)
            def _(i):
                for copy in copies(i, out, a):
                    copy.start()
        segments.wait()
        here = jnp.sum((seg_scr[...] == 0).astype(jnp.float32), axis=1, keepdims=True)
        rows = jnp.broadcast_to(here, (batch, head)).astype(jnp.bfloat16)
        for out, (a, b), tail in zip(outs, ranges, tails):
            if tail:
                out[(b - a) * 2 * piece:] = rows
        for out, (a, b) in zip(outs, ranges):
            @pl.loop(0, b - a)
            def _(i):
                for copy in copies(i, out, a):
                    copy.wait()

    if senders is None:
        fill()
    else:
        pl.when(lax.axis_index("cp") < senders)(fill)


def pack(senders, ranges, tails, seg, k, v):
    batch, piece, head = k.shape
    vmem, hbm = pl.BlockSpec(memory_space=pltpu.VMEM), pl.BlockSpec(memory_space=pltpu.HBM)
    seg, k, v = (pltpu.with_memory_space_constraint(x, pltpu.HBM) for x in (seg, k, v))
    out_shape = [
        jax.ShapeDtypeStruct(((b - a) * 2 * piece + (batch if tail else 0), head), jnp.bfloat16)
        for (a, b), tail in zip(ranges, tails)
    ]
    return pl.pallas_call(
        functools.partial(pack_kernel, senders, ranges, tails),
        in_specs=[hbm] * 3,
        out_specs=[vmem] * len(ranges),
        out_shape=out_shape,
        scratch_shapes=[pltpu.VMEM(seg.shape, jnp.int32), pltpu.SemaphoreType.DMA, pltpu.SemaphoreType.DMA],
        compiler_params=pltpu.CompilerParams(vmem_limit_bytes=16 << 20),
        cost_estimate=pl.CostEstimate(flops=1 << 20, bytes_accessed=4 * k.size, transcendentals=0),
    )(seg, k, v)


def attend_kernel(first, last, base, size, s_hbm, cut_ref, q_ref, k_ref, v_ref, near_ref, fara_ref, farb_ref, *rest):
    if not first:
        _, lse_in, q_in, kv_in, *rest = rest
    o_ref, lse_ref, *rest = rest
    if last:
        lse_out, (lse_ref, lse_sem, *rest) = lse_ref, rest
    else:
        q_out, kv_out, *rest = rest
    s_ref, n_ref, q_buf, k_buf, v_buf, o_buf, s_sem, kv_sem, q_sem, o_sem, ahead_sem = rest
    depth, heads, piece, head = q_buf.shape
    batch = lse_ref.shape[1]
    groups = heads // GROUP
    width = GROUP * piece
    scale = head ** -0.5
    me = lax.axis_index("cp")
    odd = lax.rem(me, 2)
    scalars = pltpu.make_async_copy(s_hbm, s_ref, s_sem)
    scalars.start()

    def kv_loads(step):
        slot = lax.rem(step, depth)
        seq = base + step
        there = pl.ds(pl.multiple_of(jnp.where(odd == 1, 1, 3) * piece, piece), piece)
        out = []
        for half, (ref, buf) in enumerate(((k_ref, k_buf), (v_ref, v_buf))):
            rows = pl.ds(pl.multiple_of((2 * seq + half) * piece, piece), piece)
            out.append(pltpu.make_async_copy(ref.at[seq], buf.at[slot, pl.ds(0, piece)], kv_sem.at[slot]))
            out.append(pltpu.make_async_copy(near_ref.at[rows], buf.at[slot, there], kv_sem.at[slot]))
        return out

    def aheads():
        at = base + size
        out = [pltpu.make_async_copy(q_ref.at[at], q_out, ahead_sem)]
        for half, ref in enumerate((k_ref, v_ref)):
            near_rows = pl.ds((2 * at + half) * piece, piece)
            out.append(pltpu.make_async_copy(ref.at[at], kv_out.at[2 * half], ahead_sem))
            out.append(pltpu.make_async_copy(near_ref.at[near_rows], kv_out.at[2 * half + 1], ahead_sem))
        return out

    def part(g):
        return pl.ds(g * GROUP, GROUP)

    def q_load(step, g):
        slot = lax.rem(step, depth)
        return pltpu.make_async_copy(q_ref.at[base + step, part(g)], q_buf.at[slot, part(g)], q_sem.at[slot, g])

    def o_store(step, g):
        slot = lax.rem(step, 2)
        return pltpu.make_async_copy(o_buf.at[slot, part(g)], o_ref.at[base + step, part(g)], o_sem.at[slot, g])

    def load(step):
        for copy in kv_loads(step):
            copy.start()
        for g in range(groups):
            q_load(step, g).start()

    def place(step):
        slot = lax.rem(step, depth)
        for ref, block in ((fara_ref, 2), (farb_ref, jnp.where(odd == 1, 3, 1))):
            there = pl.ds(pl.multiple_of(block * piece, piece), piece)
            for half, buf in enumerate((k_buf, v_buf)):
                buf[slot, there] = ref[pl.ds(pl.multiple_of((2 * step + half) * piece, piece), piece)]

    def run(count, step, cut):
        seq = base + step
        slot, out = lax.rem(step, depth), lax.rem(step, 2)
        keys = count * piece
        lane = lax.broadcasted_iota(jnp.int32, (piece, piece), 1)
        row = lax.broadcasted_iota(jnp.int32, (piece, piece), 0)
        low = jnp.maximum(jnp.where(row >= cut, cut, -keys), -me * piece)
        caps = [
            jnp.where((lane - n * piece <= row) & (lane - n * piece >= low), jnp.inf, -jnp.inf) for n in range(count)
        ]
        cap = jnp.concatenate([jnp.concatenate(caps, axis=1)] * GROUP, axis=0)
        logs = jnp.zeros((piece, piece), jnp.float32)

        def scores(g):
            q = q_buf[slot, g * GROUP:(g + 1) * GROUP].reshape(width, head)
            s = lax.dot_general(q, k_buf[slot, :keys], (((1,), (1,)), ((), ())), preferred_element_type=jnp.float32)
            s = jnp.minimum(s, cap)
            return s, jnp.max(s, axis=1, keepdims=True)

        def weigh(s, m):
            p = jnp.exp2((s - m) * (scale * LOG2E))
            return p.astype(jnp.bfloat16), m, jnp.sum(p, axis=1, keepdims=True)

        def finish(g, logs, p, m, l):
            o = jnp.dot(p, v_buf[slot, :keys], preferred_element_type=jnp.float32) * (1.0 / l)
            o_buf[out, g * GROUP:(g + 1) * GROUP] = o.astype(jnp.bfloat16).reshape(GROUP, piece, head)
            o_store(step, g).start()
            e = m * scale + jnp.log(l)
            for j in range(GROUP):
                logs = jnp.where(lane == g * GROUP + j, e[j * piece:(j + 1) * piece], logs)
            return logs

        now, before = scores(0), None
        for g in range(groups):
            later = scores(g + 1) if g + 1 < groups else None
            if before is not None:
                logs = finish(g - 1, logs, *before)
            before, now = weigh(*now), later
        logs = finish(groups - 1, logs, *before)
        lse_ref[:, pl.ds(seq, 1), :] = logs.T[:heads][:, None, :]

    n_ref[0] = jnp.maximum(me + 1, 2)
    if first:
        load(0)
    else:
        for step in range(1, min(3, size)):
            load(step)
        q_buf[0] = q_in[...]
        there = pl.ds(pl.multiple_of(jnp.where(odd == 1, 1, 3) * piece, piece), piece)
        for half, buf in enumerate((k_buf, v_buf)):
            buf[0, :piece] = kv_in[2 * half]
            buf[0, there] = kv_in[2 * half + 1]
        lse_ref[...] = lse_in[...]

    @pl.loop(0, size)
    def _(step):
        @pl.when((step > 0) | first)
        def _():
            for copy in kv_loads(step):
                copy.wait()
            for g in range(groups):
                q_load(step, g).wait()

        @pl.when((step == 0) & first)
        def _():
            for at in range(1, min(3, size)):
                load(at)

        @pl.when((step > 0) & (step + 2 < size))
        def _():
            load(step + 2)

        if not last:
            @pl.when(step == max(size - 2, 0))
            def _():
                for copy in aheads():
                    copy.start()

        @pl.when(step >= 2)
        def _():
            for g in range(groups):
                o_store(step - 2, g).wait()

        place(step)
        need = n_ref[0]
        for count in (2, 3, 4):
            @pl.when((need == count) | (count == 2 and need == 1))
            def _():
                run(count, step, cut_ref[pl.ds(base + step, 1), :])

        @pl.when(step == 0)
        def _():
            scalars.wait()

        n_ref[0] = s_ref[jnp.minimum(base + step + 1, batch - 1)]

    if last:
        log_store = pltpu.make_async_copy(lse_ref, lse_out, lse_sem)
        log_store.start()
        log_store.wait()
    else:
        for copy in aheads():
            copy.wait()
    for step in range(max(size - 2, 0), size):
        for g in range(groups):
            o_store(step, g).wait()


def attend(n, needs, cuts, q, k, v, near, fara, farb, prev):
    batch, heads, piece, head = q.shape
    base, size = BOUNDS[n], CHUNKS[n]
    first, last = prev is None, n == len(CHUNKS) - 1
    hbm = pl.BlockSpec(memory_space=pltpu.HBM)
    vmem = pl.BlockSpec(memory_space=pltpu.VMEM)
    in_specs = [hbm, vmem] + [hbm] * 4 + [vmem] * 2
    needs, q, k, v, near = (pltpu.with_memory_space_constraint(x, pltpu.HBM) for x in (needs, q, k, v, near))
    args = [needs, cuts, q, k, v, near, fara, farb]
    aliases = {}
    if not first:
        in_specs += [hbm, vmem, vmem, vmem]
        args += list(prev)
        aliases = {8: 0}
    out_shape = [
        jax.ShapeDtypeStruct(q.shape, jnp.bfloat16),
        jax.ShapeDtypeStruct((heads, batch, piece), jnp.float32),
    ]
    if not last:
        out_shape += [
            jax.ShapeDtypeStruct(q.shape[1:], jnp.bfloat16),
            jax.ShapeDtypeStruct((4, piece, head), jnp.bfloat16),
        ]
    return pl.pallas_call(
        functools.partial(attend_kernel, first, last, base, size),
        in_specs=in_specs,
        out_specs=[hbm, hbm] if last else [hbm] + [vmem] * 3,
        scratch_shapes=([pltpu.VMEM(out_shape[1].shape, jnp.float32), pltpu.SemaphoreType.DMA] if last else []) + [
            pltpu.SMEM(needs.shape, jnp.int32),
            pltpu.SMEM((1,), jnp.int32),
            pltpu.VMEM((DEPTH, heads, piece, head), jnp.bfloat16),
            pltpu.VMEM((DEPTH, 4 * piece, head), jnp.bfloat16),
            pltpu.VMEM((DEPTH, 4 * piece, head), jnp.bfloat16),
            pltpu.VMEM((2, heads, piece, head), jnp.bfloat16),
            pltpu.SemaphoreType.DMA,
            pltpu.SemaphoreType.DMA((DEPTH,)),
            pltpu.SemaphoreType.DMA((DEPTH, heads // GROUP)),
            pltpu.SemaphoreType.DMA((2, heads // GROUP)),
            pltpu.SemaphoreType.DMA,
        ],
        out_shape=out_shape,
        input_output_aliases=aliases,
        compiler_params=pltpu.CompilerParams(vmem_limit_bytes=20 << 20),
        cost_estimate=pl.CostEstimate(
            flops=size * heads * piece * 4 * piece * head * 4,
            bytes_accessed=size * heads * piece * head * 4,
            transcendentals=0,
        ),
    )(*args)


def swap_kernel(mine_ref, other_ref, send_sem, recv_sem):
    me = lax.axis_index("cp")
    partner = {"cp": me + 1 - 2 * lax.rem(me, 2)}
    barrier = pltpu.get_barrier_semaphore()
    pl.semaphore_signal(barrier, inc=1, device_id=partner, device_id_type=pl.DeviceIdType.MESH)
    pl.semaphore_wait(barrier, 1)
    copy = pltpu.make_async_remote_copy(
        src_ref=mine_ref,
        dst_ref=other_ref,
        send_sem=send_sem,
        recv_sem=recv_sem,
        device_id=partner,
        device_id_type=pl.DeviceIdType.MESH,
    )
    copy.start()
    copy.wait()


def swap(n, x):
    vmem = pl.BlockSpec(memory_space=pltpu.VMEM)
    return pl.pallas_call(
        swap_kernel,
        in_specs=[vmem],
        out_specs=vmem,
        out_shape=jax.ShapeDtypeStruct(x.shape, x.dtype),
        scratch_shapes=[pltpu.SemaphoreType.DMA, pltpu.SemaphoreType.DMA],
        compiler_params=pltpu.CompilerParams(
            collective_id=n, has_side_effects=True, vmem_limit_bytes=16 << 20
        ),
        cost_estimate=pl.CostEstimate(flops=1 << 20, bytes_accessed=4 * x.size, transcendentals=0),
    )(x)


def shift(x, pairs):
    return lax.ppermute(x, "cp", pairs)


def solution(mesh):
    def local(q_loc, k_loc, v_loc, seg_loc):
        batch, piece, _, _ = q_loc.shape
        me = lax.axis_index("cp")
        q = jnp.transpose(q_loc, (0, 2, 1, 3))
        ranges = tuple(zip(BOUNDS[:-1], BOUNDS[1:]))
        sends = pack(2, ranges[:1], (True,), seg_loc, k_loc, v_loc)
        *more, whole = pack(None, ranges[1:] + ((0, batch),), (False,) * len(ranges[1:]) + (True,), seg_loc, k_loc, v_loc)
        sends = list(sends) + more
        fara = [shift(x, ACROSS) for x in sends]
        near = shift(whole, BESIDE)
        farb = [swap(n, x) for n, x in enumerate(fara)]

        def zeros(packed, there):
            return jnp.where(there, packed[-batch:, 0].astype(jnp.int32), 0)

        odd, upper = me % 2 == 1, me >= 2
        cuts = zeros(whole, True) + zeros(near, odd) + zeros(fara[0], upper) + zeros(farb[0], upper)
        need = jnp.where(cuts <= me * piece, me - cuts // piece, me) + 1
        table = jnp.broadcast_to((cuts - me * piece)[:, None], (batch, piece))
        state = None
        for n in range(len(CHUNKS)):
            state = attend(n, need.astype(jnp.int32), table, q, k_loc, v_loc, near, fara[n], farb[n], state)
        out, lse = state[:2]
        return jnp.transpose(out, (0, 2, 1, 3)), jnp.transpose(lse, (1, 2, 0))

    return jax.shard_map(
        local,
        mesh=mesh,
        in_specs=(P("dp", "cp", None, None), P("dp", "cp", None), P("dp", "cp", None), P("dp", "cp")),
        out_specs=(P("dp", "cp", None, None), P("dp", "cp", None)),
        check_vma=False,
    )
```

```python
import functools

import jax
import jax.numpy as jnp
from jax import lax
from jax.experimental import pallas as pl
from jax.experimental.pallas import tpu as pltpu
from jax.sharding import PartitionSpec as P


CHUNKS = (4, 6, 6, 7, 4, 3, 2)
BOUNDS = tuple(sum(CHUNKS[:n]) for n in range(len(CHUNKS) + 1))
GROUP = 2
DEPTH = 3
LOG2E = 1.4426950408889634

ACROSS = [(0, 2), (1, 3)]
BESIDE = [(0, 1), (2, 3)]


def pack_kernel(senders, ranges, tails, seg_ref, k_ref, v_ref, *rest):
    outs, (seg_scr, seg_sem, sem) = rest[:-3], rest[-3:]
    batch, piece, head = k_ref.shape
    segments = pltpu.make_async_copy(seg_ref, seg_scr, seg_sem)

    def copies(i, out, at):
        for half, ref in enumerate((k_ref, v_ref)):
            rows = pl.ds(pl.multiple_of((2 * i + half) * piece, piece), piece)
            yield pltpu.make_async_copy(ref.at[at + i], out.at[rows], sem)

    def fill():
        segments.start()
        for out, (a, b) in zip(outs, ranges):
            @pl.loop(0, b - a)
            def _(i):
                for copy in copies(i, out, a):
                    copy.start()
        segments.wait()
        here = jnp.sum((seg_scr[...] == 0).astype(jnp.float32), axis=1, keepdims=True)
        half = (batch // 2, head // 2)
        rows = [jnp.broadcast_to(x, half) for x in (here[:half[0]], here[half[0]:])]
        rows = jnp.concatenate(rows, axis=1).astype(jnp.bfloat16)
        for out, (a, b), tail in zip(outs, ranges, tails):
            if tail:
                out[(b - a) * 2 * piece:] = rows
        for out, (a, b) in zip(outs, ranges):
            @pl.loop(0, b - a)
            def _(i):
                for copy in copies(i, out, a):
                    copy.wait()

    if senders is None:
        fill()
    else:
        pl.when(lax.axis_index("cp") < senders)(fill)


def pack(senders, ranges, tails, seg, k, v):
    batch, piece, head = k.shape
    vmem, hbm = pl.BlockSpec(memory_space=pltpu.VMEM), pl.BlockSpec(memory_space=pltpu.HBM)
    seg, k, v = (pltpu.with_memory_space_constraint(x, pltpu.HBM) for x in (seg, k, v))
    out_shape = [
        jax.ShapeDtypeStruct(((b - a) * 2 * piece + (batch // 2 if tail else 0), head), jnp.bfloat16)
        for (a, b), tail in zip(ranges, tails)
    ]
    return pl.pallas_call(
        functools.partial(pack_kernel, senders, ranges, tails),
        in_specs=[hbm] * 3,
        out_specs=[vmem] * len(ranges),
        out_shape=out_shape,
        scratch_shapes=[pltpu.VMEM(seg.shape, jnp.int32), pltpu.SemaphoreType.DMA, pltpu.SemaphoreType.DMA],
        compiler_params=pltpu.CompilerParams(vmem_limit_bytes=16 << 20),
        cost_estimate=pl.CostEstimate(flops=1 << 20, bytes_accessed=4 * k.size, transcendentals=0),
    )(seg, k, v)


def attend_kernel(first, last, base, size, s_hbm, cut_ref, q_ref, k_ref, v_ref, near_ref, fara_ref, farb_ref, *rest):
    if not first:
        _, lse_in, q_in, kv_in, *rest = rest
    o_ref, lse_ref, *rest = rest
    if last:
        lse_out, (lse_ref, lse_sem, *rest) = lse_ref, rest
    else:
        q_out, kv_out, *rest = rest
    s_ref, n_ref, q_buf, k_buf, v_buf, o_buf, s_sem, kv_sem, q_sem, o_sem, ahead_sem = rest
    depth, heads, piece, head = q_buf.shape
    batch = lse_ref.shape[1]
    groups = heads // GROUP
    width = GROUP * piece
    scale = head ** -0.5
    me = lax.axis_index("cp")
    odd = lax.rem(me, 2)
    scalars = pltpu.make_async_copy(s_hbm, s_ref, s_sem)
    scalars.start()

    def kv_loads(step):
        slot = lax.rem(step, depth)
        seq = base + step
        there = pl.ds(pl.multiple_of(jnp.where(odd == 1, 1, 3) * piece, piece), piece)
        out = []
        for half, (ref, buf) in enumerate(((k_ref, k_buf), (v_ref, v_buf))):
            rows = pl.ds(pl.multiple_of((2 * seq + half) * piece, piece), piece)
            out.append(pltpu.make_async_copy(ref.at[seq], buf.at[slot, pl.ds(0, piece)], kv_sem.at[slot]))
            out.append(pltpu.make_async_copy(near_ref.at[rows], buf.at[slot, there], kv_sem.at[slot]))
        return out

    def aheads():
        at = base + size
        out = [pltpu.make_async_copy(q_ref.at[at], q_out, ahead_sem)]
        for half, ref in enumerate((k_ref, v_ref)):
            near_rows = pl.ds((2 * at + half) * piece, piece)
            out.append(pltpu.make_async_copy(ref.at[at], kv_out.at[2 * half], ahead_sem))
            out.append(pltpu.make_async_copy(near_ref.at[near_rows], kv_out.at[2 * half + 1], ahead_sem))
        return out

    def part(g):
        return pl.ds(g * GROUP, GROUP)

    def q_load(step, g):
        slot = lax.rem(step, depth)
        return pltpu.make_async_copy(q_ref.at[base + step, part(g)], q_buf.at[slot, part(g)], q_sem.at[slot, g])

    def o_store(step, g):
        slot = lax.rem(step, 2)
        return pltpu.make_async_copy(o_buf.at[slot, part(g)], o_ref.at[base + step, part(g)], o_sem.at[slot, g])

    def load(step):
        for copy in kv_loads(step):
            copy.start()
        for g in range(groups):
            q_load(step, g).start()

    def place(step):
        slot = lax.rem(step, depth)
        for ref, block in ((fara_ref, 2), (farb_ref, jnp.where(odd == 1, 3, 1))):
            there = pl.ds(pl.multiple_of(block * piece, piece), piece)
            for half, buf in enumerate((k_buf, v_buf)):
                buf[slot, there] = ref[pl.ds(pl.multiple_of((2 * step + half) * piece, piece), piece)]

    def run(count, step, cut):
        seq = base + step
        slot, out = lax.rem(step, depth), lax.rem(step, 2)
        keys = count * piece
        lane = lax.broadcasted_iota(jnp.int32, (piece, piece), 1)
        row = lax.broadcasted_iota(jnp.int32, (piece, piece), 0)
        low = jnp.maximum(jnp.where(row >= cut, cut, -keys), -me * piece)
        caps = [
            jnp.where((lane - n * piece <= row) & (lane - n * piece >= low), jnp.inf, -jnp.inf) for n in range(count)
        ]
        cap = jnp.concatenate([jnp.concatenate(caps, axis=1)] * GROUP, axis=0)
        logs = jnp.zeros((piece, piece), jnp.float32)

        def scores(g):
            q = q_buf[slot, g * GROUP:(g + 1) * GROUP].reshape(width, head)
            s = lax.dot_general(q, k_buf[slot, :keys], (((1,), (1,)), ((), ())), preferred_element_type=jnp.float32)
            s = jnp.minimum(s, cap)
            return s, jnp.max(s, axis=1, keepdims=True)

        def weigh(s, m):
            p = jnp.exp2((s - m) * (scale * LOG2E))
            return p.astype(jnp.bfloat16), m, jnp.sum(p, axis=1, keepdims=True)

        def finish(g, logs, p, m, l):
            o = jnp.dot(p, v_buf[slot, :keys], preferred_element_type=jnp.float32) * (1.0 / l)
            o_buf[out, g * GROUP:(g + 1) * GROUP] = o.astype(jnp.bfloat16).reshape(GROUP, piece, head)
            o_store(step, g).start()
            e = m * scale + jnp.log(l)
            for j in range(GROUP):
                logs = jnp.where(lane == g * GROUP + j, e[j * piece:(j + 1) * piece], logs)
            return logs

        now, before = scores(0), None
        for g in range(groups):
            later = scores(g + 1) if g + 1 < groups else None
            if before is not None:
                logs = finish(g - 1, logs, *before)
            before, now = weigh(*now), later
        logs = finish(groups - 1, logs, *before)
        lse_ref[:, pl.ds(seq, 1), :] = logs.T[:heads][:, None, :]

    n_ref[0] = jnp.maximum(me + 1, 2)
    if first:
        load(0)
    else:
        for step in range(1, min(3, size)):
            load(step)
        q_buf[0] = q_in[...]
        there = pl.ds(pl.multiple_of(jnp.where(odd == 1, 1, 3) * piece, piece), piece)
        for half, buf in enumerate((k_buf, v_buf)):
            buf[0, :piece] = kv_in[2 * half]
            buf[0, there] = kv_in[2 * half + 1]
        lse_ref[...] = lse_in[...]

    @pl.loop(0, size)
    def _(step):
        @pl.when((step > 0) | first)
        def _():
            for copy in kv_loads(step):
                copy.wait()
            for g in range(groups):
                q_load(step, g).wait()

        @pl.when((step == 0) & first)
        def _():
            for at in range(1, min(3, size)):
                load(at)

        @pl.when((step > 0) & (step + 2 < size))
        def _():
            load(step + 2)

        if not last:
            @pl.when(step == max(size - 2, 0))
            def _():
                for copy in aheads():
                    copy.start()

        @pl.when(step >= 2)
        def _():
            for g in range(groups):
                o_store(step - 2, g).wait()

        place(step)
        need = n_ref[0]
        for count in (2, 3, 4):
            @pl.when((need == count) | (count == 2 and need == 1))
            def _():
                run(count, step, cut_ref[pl.ds(base + step, 1), :])

        @pl.when(step == 0)
        def _():
            scalars.wait()

        n_ref[0] = s_ref[jnp.minimum(base + step + 1, batch - 1)]

    if last:
        log_store = pltpu.make_async_copy(lse_ref, lse_out, lse_sem)
        log_store.start()
        log_store.wait()
    else:
        for copy in aheads():
            copy.wait()
    for step in range(max(size - 2, 0), size):
        for g in range(groups):
            o_store(step, g).wait()


def attend(n, needs, cuts, q, k, v, near, fara, farb, prev):
    batch, heads, piece, head = q.shape
    base, size = BOUNDS[n], CHUNKS[n]
    first, last = prev is None, n == len(CHUNKS) - 1
    hbm = pl.BlockSpec(memory_space=pltpu.HBM)
    vmem = pl.BlockSpec(memory_space=pltpu.VMEM)
    in_specs = [hbm, vmem] + [hbm] * 4 + [vmem] * 2
    needs, q, k, v, near = (pltpu.with_memory_space_constraint(x, pltpu.HBM) for x in (needs, q, k, v, near))
    args = [needs, cuts, q, k, v, near, fara, farb]
    aliases = {}
    if not first:
        in_specs += [hbm, vmem, vmem, vmem]
        args += list(prev)
        aliases = {8: 0}
    out_shape = [
        jax.ShapeDtypeStruct(q.shape, jnp.bfloat16),
        jax.ShapeDtypeStruct((heads, batch, piece), jnp.float32),
    ]
    if not last:
        out_shape += [
            jax.ShapeDtypeStruct(q.shape[1:], jnp.bfloat16),
            jax.ShapeDtypeStruct((4, piece, head), jnp.bfloat16),
        ]
    return pl.pallas_call(
        functools.partial(attend_kernel, first, last, base, size),
        in_specs=in_specs,
        out_specs=[hbm, hbm] if last else [hbm] + [vmem] * 3,
        scratch_shapes=([pltpu.VMEM(out_shape[1].shape, jnp.float32), pltpu.SemaphoreType.DMA] if last else []) + [
            pltpu.SMEM(needs.shape, jnp.int32),
            pltpu.SMEM((1,), jnp.int32),
            pltpu.VMEM((DEPTH, heads, piece, head), jnp.bfloat16),
            pltpu.VMEM((DEPTH, 4 * piece, head), jnp.bfloat16),
            pltpu.VMEM((DEPTH, 4 * piece, head), jnp.bfloat16),
            pltpu.VMEM((2, heads, piece, head), jnp.bfloat16),
            pltpu.SemaphoreType.DMA,
            pltpu.SemaphoreType.DMA((DEPTH,)),
            pltpu.SemaphoreType.DMA((DEPTH, heads // GROUP)),
            pltpu.SemaphoreType.DMA((2, heads // GROUP)),
            pltpu.SemaphoreType.DMA,
        ],
        out_shape=out_shape,
        input_output_aliases=aliases,
        compiler_params=pltpu.CompilerParams(vmem_limit_bytes=20 << 20),
        cost_estimate=pl.CostEstimate(
            flops=size * heads * piece * 4 * piece * head * 4,
            bytes_accessed=size * heads * piece * head * 4,
            transcendentals=0,
        ),
    )(*args)


def swap_kernel(mine_ref, other_ref, send_sem, recv_sem):
    me = lax.axis_index("cp")
    partner = {"cp": me + 1 - 2 * lax.rem(me, 2)}
    barrier = pltpu.get_barrier_semaphore()
    pl.semaphore_signal(barrier, inc=1, device_id=partner, device_id_type=pl.DeviceIdType.MESH)
    pl.semaphore_wait(barrier, 1)
    copy = pltpu.make_async_remote_copy(
        src_ref=mine_ref,
        dst_ref=other_ref,
        send_sem=send_sem,
        recv_sem=recv_sem,
        device_id=partner,
        device_id_type=pl.DeviceIdType.MESH,
    )
    copy.start()
    copy.wait()


def swap(n, x):
    vmem = pl.BlockSpec(memory_space=pltpu.VMEM)
    return pl.pallas_call(
        swap_kernel,
        in_specs=[vmem],
        out_specs=vmem,
        out_shape=jax.ShapeDtypeStruct(x.shape, x.dtype),
        scratch_shapes=[pltpu.SemaphoreType.DMA, pltpu.SemaphoreType.DMA],
        compiler_params=pltpu.CompilerParams(
            collective_id=n, has_side_effects=True, vmem_limit_bytes=16 << 20
        ),
        cost_estimate=pl.CostEstimate(flops=1 << 20, bytes_accessed=4 * x.size, transcendentals=0),
    )(x)


def shift(x, pairs):
    return lax.ppermute(x, "cp", pairs)


def solution(mesh):
    def local(q_loc, k_loc, v_loc, seg_loc):
        batch, piece, _, head = q_loc.shape
        me = lax.axis_index("cp")
        q = jnp.transpose(q_loc, (0, 2, 1, 3))
        ranges = tuple(zip(BOUNDS[:-1], BOUNDS[1:]))
        sends = pack(2, ranges[:1], (True,), seg_loc, k_loc, v_loc)
        *more, whole = pack(None, ranges[1:] + ((0, batch),), (False,) * len(ranges[1:]) + (True,), seg_loc, k_loc, v_loc)
        sends = list(sends) + more
        fara = [shift(x, ACROSS) for x in sends]
        near = shift(whole, BESIDE)
        farb = [swap(n, x) for n, x in enumerate(fara)]

        def zeros(packed, there):
            halves = jnp.concatenate([packed[-batch // 2:, at] for at in (0, head // 2)])
            return jnp.where(there, halves.astype(jnp.int32), 0)

        odd, upper = me % 2 == 1, me >= 2
        cuts = zeros(whole, True) + zeros(near, odd) + zeros(fara[0], upper) + zeros(farb[0], upper)
        need = jnp.where(cuts <= me * piece, me - cuts // piece, me) + 1
        table = jnp.broadcast_to((cuts - me * piece)[:, None], (batch, piece))
        state = None
        for n in range(len(CHUNKS)):
            state = attend(n, need.astype(jnp.int32), table, q, k_loc, v_loc, near, fara[n], farb[n], state)
        out, lse = state[:2]
        return jnp.transpose(out, (0, 2, 1, 3)), jnp.transpose(lse, (1, 2, 0))

    return jax.shard_map(
        local,
        mesh=mesh,
        in_specs=(P("dp", "cp", None, None), P("dp", "cp", None), P("dp", "cp", None), P("dp", "cp")),
        out_specs=(P("dp", "cp", None, None), P("dp", "cp", None)),
        check_vma=False,
    )
```

```python
import functools

import jax
import jax.numpy as jnp
from jax import lax
from jax.experimental import pallas as pl
from jax.experimental.pallas import tpu as pltpu
from jax.sharding import PartitionSpec as P


CHUNKS = (4, 6, 6, 5, 4, 4, 3)
BOUNDS = tuple(sum(CHUNKS[:n]) for n in range(len(CHUNKS) + 1))
GROUP = 2
DEPTH = 3
LOG2E = 1.4426950408889634

ACROSS = [(0, 2), (1, 3)]
BESIDE = [(0, 1), (2, 3)]


def pack_kernel(senders, ranges, tails, seg_ref, k_ref, v_ref, *rest):
    outs, (seg_scr, seg_sem, sem) = rest[:-3], rest[-3:]
    batch, piece, head = k_ref.shape
    segments = pltpu.make_async_copy(seg_ref, seg_scr, seg_sem)

    def copies(i, out, at):
        for half, ref in enumerate((k_ref, v_ref)):
            rows = pl.ds(pl.multiple_of((2 * i + half) * piece, piece), piece)
            yield pltpu.make_async_copy(ref.at[at + i], out.at[rows], sem)

    def fill():
        segments.start()
        for out, (a, b) in zip(outs, ranges):
            @pl.loop(0, b - a)
            def _(i):
                for copy in copies(i, out, a):
                    copy.start()
        segments.wait()
        here = jnp.sum((seg_scr[...] == 0).astype(jnp.float32), axis=1, keepdims=True)
        half = (batch // 2, head // 2)
        rows = [jnp.broadcast_to(x, half) for x in (here[:half[0]], here[half[0]:])]
        rows = jnp.concatenate(rows, axis=1).astype(jnp.bfloat16)
        for out, (a, b), tail in zip(outs, ranges, tails):
            if tail:
                out[(b - a) * 2 * piece:] = rows
        for out, (a, b) in zip(outs, ranges):
            @pl.loop(0, b - a)
            def _(i):
                for copy in copies(i, out, a):
                    copy.wait()

    if senders is None:
        fill()
    else:
        pl.when(lax.axis_index("cp") < senders)(fill)


def pack(senders, ranges, tails, seg, k, v):
    batch, piece, head = k.shape
    vmem, hbm = pl.BlockSpec(memory_space=pltpu.VMEM), pl.BlockSpec(memory_space=pltpu.HBM)
    seg, k, v = (pltpu.with_memory_space_constraint(x, pltpu.HBM) for x in (seg, k, v))
    out_shape = [
        jax.ShapeDtypeStruct(((b - a) * 2 * piece + (batch // 2 if tail else 0), head), jnp.bfloat16)
        for (a, b), tail in zip(ranges, tails)
    ]
    return pl.pallas_call(
        functools.partial(pack_kernel, senders, ranges, tails),
        in_specs=[hbm] * 3,
        out_specs=[vmem] * len(ranges),
        out_shape=out_shape,
        scratch_shapes=[pltpu.VMEM(seg.shape, jnp.int32), pltpu.SemaphoreType.DMA, pltpu.SemaphoreType.DMA],
        compiler_params=pltpu.CompilerParams(vmem_limit_bytes=16 << 20),
        cost_estimate=pl.CostEstimate(flops=1 << 20, bytes_accessed=4 * k.size, transcendentals=0),
    )(seg, k, v)


def attend_kernel(first, last, base, size, s_hbm, cut_ref, q_ref, k_ref, v_ref, near_ref, fara_ref, farb_ref, *rest):
    if not first:
        _, lse_in, q_in, kv_in, *rest = rest
    o_ref, lse_ref, *rest = rest
    if last:
        lse_out, (lse_ref, lse_sem, early_sem, *rest) = lse_ref, rest
    else:
        q_out, kv_out, *rest = rest
    s_ref, n_ref, q_buf, k_buf, v_buf, o_buf, s_sem, kv_sem, q_sem, o_sem, ahead_sem = rest
    depth, heads, piece, head = q_buf.shape
    batch = lse_ref.shape[1]
    groups = heads // GROUP
    width = GROUP * piece
    scale = head ** -0.5
    me = lax.axis_index("cp")
    odd = lax.rem(me, 2)
    scalars = pltpu.make_async_copy(s_hbm, s_ref, s_sem)
    scalars.start()

    def kv_loads(step):
        slot = lax.rem(step, depth)
        seq = base + step
        there = pl.ds(pl.multiple_of(jnp.where(odd == 1, 1, 3) * piece, piece), piece)
        out = []
        for half, (ref, buf) in enumerate(((k_ref, k_buf), (v_ref, v_buf))):
            rows = pl.ds(pl.multiple_of((2 * seq + half) * piece, piece), piece)
            out.append(pltpu.make_async_copy(ref.at[seq], buf.at[slot, pl.ds(0, piece)], kv_sem.at[slot]))
            out.append(pltpu.make_async_copy(near_ref.at[rows], buf.at[slot, there], kv_sem.at[slot]))
        return out

    def aheads():
        at = base + size
        out = [pltpu.make_async_copy(q_ref.at[at], q_out, ahead_sem)]
        for half, ref in enumerate((k_ref, v_ref)):
            near_rows = pl.ds((2 * at + half) * piece, piece)
            out.append(pltpu.make_async_copy(ref.at[at], kv_out.at[2 * half], ahead_sem))
            out.append(pltpu.make_async_copy(near_ref.at[near_rows], kv_out.at[2 * half + 1], ahead_sem))
        return out

    def part(g):
        return pl.ds(g * GROUP, GROUP)

    def q_load(step, g):
        slot = lax.rem(step, depth)
        return pltpu.make_async_copy(q_ref.at[base + step, part(g)], q_buf.at[slot, part(g)], q_sem.at[slot, g])

    def o_store(step, g):
        slot = lax.rem(step, 2)
        return pltpu.make_async_copy(o_buf.at[slot, part(g)], o_ref.at[base + step, part(g)], o_sem.at[slot, g])

    def load(step):
        for copy in kv_loads(step):
            copy.start()
        for g in range(groups):
            q_load(step, g).start()

    def place(step):
        slot = lax.rem(step, depth)
        for ref, block in ((fara_ref, 2), (farb_ref, jnp.where(odd == 1, 3, 1))):
            there = pl.ds(pl.multiple_of(block * piece, piece), piece)
            for half, buf in enumerate((k_buf, v_buf)):
                buf[slot, there] = ref[pl.ds(pl.multiple_of((2 * step + half) * piece, piece), piece)]

    def run(count, step, cut):
        seq = base + step
        slot, out = lax.rem(step, depth), lax.rem(step, 2)
        keys = count * piece
        lane = lax.broadcasted_iota(jnp.int32, (piece, piece), 1)
        row = lax.broadcasted_iota(jnp.int32, (piece, piece), 0)
        low = jnp.maximum(jnp.where(row >= cut, cut, -keys), -me * piece)
        caps = [
            jnp.where((lane - n * piece <= row) & (lane - n * piece >= low), jnp.inf, -jnp.inf) for n in range(count)
        ]
        cap = jnp.concatenate([jnp.concatenate(caps, axis=1)] * GROUP, axis=0)
        logs = jnp.zeros((piece, piece), jnp.float32)

        def scores(g):
            q = q_buf[slot, g * GROUP:(g + 1) * GROUP].reshape(width, head)
            s = lax.dot_general(q, k_buf[slot, :keys], (((1,), (1,)), ((), ())), preferred_element_type=jnp.float32)
            s = jnp.minimum(s, cap)
            return s, jnp.max(s, axis=1, keepdims=True)

        def weigh(s, m):
            p = jnp.exp2((s - m) * (scale * LOG2E))
            return p.astype(jnp.bfloat16), m, jnp.sum(p, axis=1, keepdims=True)

        def finish(g, logs, p, m, l):
            o = jnp.dot(p, v_buf[slot, :keys], preferred_element_type=jnp.float32) * (1.0 / l)
            o_buf[out, g * GROUP:(g + 1) * GROUP] = o.astype(jnp.bfloat16).reshape(GROUP, piece, head)
            o_store(step, g).start()
            e = m * scale + jnp.log(l)
            for j in range(GROUP):
                logs = jnp.where(lane == g * GROUP + j, e[j * piece:(j + 1) * piece], logs)
            return logs

        now, before = scores(0), None
        for g in range(groups):
            later = scores(g + 1) if g + 1 < groups else None
            if before is not None:
                logs = finish(g - 1, logs, *before)
            before, now = weigh(*now), later
        logs = finish(groups - 1, logs, *before)
        lse_ref[:, pl.ds(seq, 1), :] = logs.T[:heads][:, None, :]

    n_ref[0] = jnp.maximum(me + 1, 2)
    if first:
        load(0)
    else:
        for step in range(1, min(3, size)):
            load(step)
        q_buf[0] = q_in[...]
        there = pl.ds(pl.multiple_of(jnp.where(odd == 1, 1, 3) * piece, piece), piece)
        for half, buf in enumerate((k_buf, v_buf)):
            buf[0, :piece] = kv_in[2 * half]
            buf[0, there] = kv_in[2 * half + 1]
        lse_ref[...] = lse_in[...]

    if last:
        ready = base // 8 * 8
        early = pltpu.make_async_copy(lse_in.at[:, pl.ds(0, ready)], lse_out.at[:, pl.ds(0, ready)], early_sem)
        early.start()

    @pl.loop(0, size)
    def _(step):
        @pl.when((step > 0) | first)
        def _():
            for copy in kv_loads(step):
                copy.wait()
            for g in range(groups):
                q_load(step, g).wait()

        @pl.when((step == 0) & first)
        def _():
            for at in range(1, min(3, size)):
                load(at)

        @pl.when((step > 0) & (step + 2 < size))
        def _():
            load(step + 2)

        if not last:
            @pl.when(step == max(size - 2, 0))
            def _():
                for copy in aheads():
                    copy.start()

        @pl.when(step >= 2)
        def _():
            for g in range(groups):
                o_store(step - 2, g).wait()

        place(step)
        need = n_ref[0]
        for count in (2, 3, 4):
            @pl.when((need == count) | (count == 2 and need == 1))
            def _():
                run(count, step, cut_ref[pl.ds(base + step, 1), :])

        @pl.when(step == 0)
        def _():
            scalars.wait()

        n_ref[0] = s_ref[jnp.minimum(base + step + 1, batch - 1)]

    if last:
        late = pl.ds(ready, batch - ready)
        log_store = pltpu.make_async_copy(lse_ref.at[:, late], lse_out.at[:, late], lse_sem)
        log_store.start()
        early.wait()
        log_store.wait()
    else:
        for copy in aheads():
            copy.wait()
    for step in range(max(size - 2, 0), size):
        for g in range(groups):
            o_store(step, g).wait()


def attend(n, needs, cuts, q, k, v, near, fara, farb, prev):
    batch, heads, piece, head = q.shape
    base, size = BOUNDS[n], CHUNKS[n]
    first, last = prev is None, n == len(CHUNKS) - 1
    hbm = pl.BlockSpec(memory_space=pltpu.HBM)
    vmem = pl.BlockSpec(memory_space=pltpu.VMEM)
    in_specs = [hbm, vmem] + [hbm] * 4 + [vmem] * 2
    needs, q, k, v, near = (pltpu.with_memory_space_constraint(x, pltpu.HBM) for x in (needs, q, k, v, near))
    args = [needs, cuts, q, k, v, near, fara, farb]
    aliases = {}
    if not first:
        in_specs += [hbm, vmem, vmem, vmem]
        args += list(prev)
        aliases = {8: 0}
    out_shape = [
        jax.ShapeDtypeStruct(q.shape, jnp.bfloat16),
        jax.ShapeDtypeStruct((heads, batch, piece), jnp.float32),
    ]
    if not last:
        out_shape += [
            jax.ShapeDtypeStruct(q.shape[1:], jnp.bfloat16),
            jax.ShapeDtypeStruct((4, piece, head), jnp.bfloat16),
        ]
    return pl.pallas_call(
        functools.partial(attend_kernel, first, last, base, size),
        in_specs=in_specs,
        out_specs=[hbm, hbm] if last else [hbm] + [vmem] * 3,
        scratch_shapes=([pltpu.VMEM(out_shape[1].shape, jnp.float32)] + [pltpu.SemaphoreType.DMA] * 2 if last else []) + [
            pltpu.SMEM(needs.shape, jnp.int32),
            pltpu.SMEM((1,), jnp.int32),
            pltpu.VMEM((DEPTH, heads, piece, head), jnp.bfloat16),
            pltpu.VMEM((DEPTH, 4 * piece, head), jnp.bfloat16),
            pltpu.VMEM((DEPTH, 4 * piece, head), jnp.bfloat16),
            pltpu.VMEM((2, heads, piece, head), jnp.bfloat16),
            pltpu.SemaphoreType.DMA,
            pltpu.SemaphoreType.DMA((DEPTH,)),
            pltpu.SemaphoreType.DMA((DEPTH, heads // GROUP)),
            pltpu.SemaphoreType.DMA((2, heads // GROUP)),
            pltpu.SemaphoreType.DMA,
        ],
        out_shape=out_shape,
        input_output_aliases=aliases,
        compiler_params=pltpu.CompilerParams(vmem_limit_bytes=20 << 20),
        cost_estimate=pl.CostEstimate(
            flops=size * heads * piece * 4 * piece * head * 4,
            bytes_accessed=size * heads * piece * head * 4,
            transcendentals=0,
        ),
    )(*args)


def swap_kernel(mine_ref, other_ref, send_sem, recv_sem):
    me = lax.axis_index("cp")
    partner = {"cp": me + 1 - 2 * lax.rem(me, 2)}
    barrier = pltpu.get_barrier_semaphore()
    pl.semaphore_signal(barrier, inc=1, device_id=partner, device_id_type=pl.DeviceIdType.MESH)
    pl.semaphore_wait(barrier, 1)
    copy = pltpu.make_async_remote_copy(
        src_ref=mine_ref,
        dst_ref=other_ref,
        send_sem=send_sem,
        recv_sem=recv_sem,
        device_id=partner,
        device_id_type=pl.DeviceIdType.MESH,
    )
    copy.start()
    copy.wait()


def swap(n, x):
    vmem = pl.BlockSpec(memory_space=pltpu.VMEM)
    return pl.pallas_call(
        swap_kernel,
        in_specs=[vmem],
        out_specs=vmem,
        out_shape=jax.ShapeDtypeStruct(x.shape, x.dtype),
        scratch_shapes=[pltpu.SemaphoreType.DMA, pltpu.SemaphoreType.DMA],
        compiler_params=pltpu.CompilerParams(
            collective_id=n, has_side_effects=True, vmem_limit_bytes=16 << 20
        ),
        cost_estimate=pl.CostEstimate(flops=1 << 20, bytes_accessed=4 * x.size, transcendentals=0),
    )(x)


def shift(x, pairs):
    return lax.ppermute(x, "cp", pairs)


def solution(mesh):
    def local(q_loc, k_loc, v_loc, seg_loc):
        batch, piece, _, head = q_loc.shape
        me = lax.axis_index("cp")
        q = jnp.transpose(q_loc, (0, 2, 1, 3))
        ranges = tuple(zip(BOUNDS[:-1], BOUNDS[1:]))
        sends = pack(2, ranges[:1], (True,), seg_loc, k_loc, v_loc)
        *more, whole = pack(None, ranges[1:] + ((0, batch),), (False,) * len(ranges[1:]) + (True,), seg_loc, k_loc, v_loc)
        sends = list(sends) + more
        fara = [shift(x, ACROSS) for x in sends]
        near = shift(whole, BESIDE)
        farb = [swap(n, x) for n, x in enumerate(fara)]

        def zeros(packed, there):
            halves = jnp.concatenate([packed[-batch // 2:, at] for at in (0, head // 2)])
            return jnp.where(there, halves.astype(jnp.int32), 0)

        odd, upper = me % 2 == 1, me >= 2
        cuts = zeros(whole, True) + zeros(near, odd) + zeros(fara[0], upper) + zeros(farb[0], upper)
        need = jnp.where(cuts <= me * piece, me - cuts // piece, me) + 1
        table = jnp.broadcast_to((cuts - me * piece)[:, None], (batch, piece))
        state = None
        for n in range(len(CHUNKS)):
            state = attend(n, need.astype(jnp.int32), table, q, k_loc, v_loc, near, fara[n], farb[n], state)
        out, lse = state[:2]
        return jnp.transpose(out, (0, 2, 1, 3)), jnp.transpose(lse, (1, 2, 0))

    return jax.shard_map(
        local,
        mesh=mesh,
        in_specs=(P("dp", "cp", None, None), P("dp", "cp", None), P("dp", "cp", None), P("dp", "cp")),
        out_specs=(P("dp", "cp", None, None), P("dp", "cp", None)),
        check_vma=False,
    )
```
